8 devices in a mesh: dp: 1 (over z), tp: 2 (over y), cp: 4 (over x, core).
Axes of the slice: x: 2, y: 2, z: 1, core: 2. Of those that a mesh axis runs over, the one named last changes fastest.
Arguments:
- hidden: bfloat16 [24, 64, 2048], P('dp')
- attn_gain: bfloat16 [2048], replicated
- w_query: bfloat16 [2048, 2048], P(None, 'tp')
- w_key: bfloat16 [2048, 512], P(None, 'tp')
- w_value: bfloat16 [2048, 512], P(None, 'tp')
- w_out: bfloat16 [2048, 2048], P('tp')
- cache_k: bfloat16 [24, 4, 4, 8, 256, 64], P('dp', None, 'cp', 'tp')
- cache_v: bfloat16 [24, 4, 4, 8, 256, 64], P('dp', None, 'cp', 'tp')
- ctx_len: int32 [24], P('dp')
- positions: int32 [24, 64], P('dp')
- tree_mask: int32 [24, 64, 64], P('dp')
Outputs:
- output 1: bfloat16 [24, 64, 2048], P('dp')
- output 2: bfloat16 [24, 4, 4, 8, 256, 64], P('dp', None, 'cp', 'tp')
- output 3: bfloat16 [24, 4, 4, 8, 256, 64], P('dp', None, 'cp', 'tp')
All inputs are finite; a program needn't handle non-finite values.
Results may differ from the reference program's by a relative error of at most 0.00876036.
Values sent between devices are 32-bit elements.
A program may use at most 1 GiB of HBM per device.

```python
import math
import jax
import jax.numpy as jnp
from jax import lax

D = 2048
HEADS = 32
KV_HEADS = 8
HEAD = 64
REQ = 24
TREE = 64
BLOCKS_DEV = 4
CP = 4
TP = 2
BLOCK = 256
ROPE_THETA = 500000.0
NORM_EPS = 1e-5
MASKED = -1e30


def rope_tables(positions, head_dim):
    freq_idx = jnp.arange(head_dim // 2, dtype=jnp.float32)
    inv_freq = 1.0 / (ROPE_THETA ** (2.0 * freq_idx / head_dim))
    wavelen = 2.0 * math.pi / inv_freq
    smooth = (8192.0 / wavelen - 1.0) / 3.0
    blended = (1.0 - smooth) * inv_freq / 8.0 + smooth * inv_freq
    inv_freq = jnp.where(wavelen < 2048.0, inv_freq, jnp.where(wavelen > 8192.0, inv_freq / 8.0, blended))
    angle = positions.astype(jnp.float32)[..., None] * inv_freq
    return jnp.cos(angle)[..., None, :], jnp.sin(angle)[..., None, :]


def apply_rope(values, cos_tab, sin_tab):
    half = values.shape[-1] // 2
    first = values[..., :half]
    second = values[..., half:]
    return jnp.concatenate([first * cos_tab - second * sin_tab, second * cos_tab + first * sin_tab], axis=-1)


def rms_norm(hidden, attn_gain):
    wide = hidden.astype(jnp.float32)
    inv_rms = lax.rsqrt(jnp.mean(wide * wide, axis=-1, keepdims=True) + NORM_EPS)
    return wide, (wide * inv_rms * attn_gain.astype(jnp.float32)).astype(jnp.bfloat16)


def draw_structure(key):
    ctx_key, tree_key = jax.random.split(key)
    max_len = BLOCKS_DEV * CP * BLOCK
    ctx_len = jax.random.randint(ctx_key, (REQ,), max_len // 2, max_len - TREE + 1, dtype=jnp.int32)
    ctx_len = ctx_len.at[0].set(max_len - TREE).at[1].set(max_len // 2)
    raw = jax.random.randint(tree_key, (REQ, TREE), 0, 1 << 30, dtype=jnp.int32)
    node_ids = jnp.arange(TREE, dtype=jnp.int32)
    parents = raw % jnp.maximum(node_ids, 1)[None, :]
    ancestry = jnp.broadcast_to(jnp.eye(TREE, dtype=jnp.int32), (REQ, TREE, TREE))
    for node in range(1, TREE):
        above = jnp.take_along_axis(ancestry, parents[:, node][:, None, None], axis=1)[:, 0, :]
        ancestry = ancestry.at[:, node, :].add(above)
    depth = ancestry.sum(axis=-1) - 1
    positions = ctx_len[:, None] + depth
    return ctx_len, positions.astype(jnp.int32), ancestry


def setup_inputs(seed: int = 0, part: int = 0) -> dict:
    base = jax.random.key(seed)
    part_key = jax.random.fold_in(base, part)
    wkeys = jax.random.split(base, 5)
    pkeys = jax.random.split(part_key, 4)
    max_len = BLOCKS_DEV * CP * BLOCK
    key_scale = math.sqrt(math.log(max_len / 64.0))
    new_scale = math.log(max_len) - 1.4
    ctx_len, positions, tree_mask = draw_structure(pkeys[0])
    hidden = (0.5 * jax.random.normal(pkeys[1], (REQ, TREE, D), jnp.float32)).astype(jnp.bfloat16)
    attn_gain = (1.0 + 0.3 * jax.random.normal(wkeys[0], (D,), jnp.float32)).astype(jnp.bfloat16)
    w_query = (jax.random.normal(wkeys[1], (D, HEADS * HEAD), jnp.float32) * D ** -0.5).astype(jnp.bfloat16)
    w_key = (jax.random.normal(wkeys[2], (D, KV_HEADS * HEAD), jnp.float32) * (new_scale * D ** -0.5)).astype(jnp.bfloat16)
    w_value = (jax.random.normal(wkeys[3], (D, KV_HEADS * HEAD), jnp.float32) * (2.0 * D ** -0.5)).astype(jnp.bfloat16)
    w_out = (jax.random.normal(wkeys[4], (HEADS * HEAD, D), jnp.float32) * (HEADS * HEAD) ** -0.5).astype(jnp.bfloat16)
    cache_shape = (REQ, BLOCKS_DEV, CP, KV_HEADS, BLOCK, HEAD)
    cache_k = (key_scale * jax.random.normal(pkeys[2], cache_shape, jnp.float32)).astype(jnp.bfloat16)
    cache_v = (4.0 * jax.random.normal(pkeys[3], cache_shape, jnp.float32)).astype(jnp.bfloat16)
    return {'hidden': hidden, 'attn_gain': attn_gain, 'w_query': w_query, 'w_key': w_key, 'w_value': w_value, 'w_out': w_out, 'cache_k': cache_k, 'cache_v': cache_v, 'ctx_len': ctx_len, 'positions': positions, 'tree_mask': tree_mask}


def reference(hidden, attn_gain, w_query, w_key, w_value, w_out, cache_k, cache_v, ctx_len, positions, tree_mask):
    group = HEADS // KV_HEADS
    max_len = BLOCKS_DEV * CP * BLOCK
    scale = HEAD ** -0.5
    wide, normed = rms_norm(hidden, attn_gain)
    flat_rows = normed.reshape(REQ * TREE, D)
    query = jnp.dot(flat_rows, w_query, preferred_element_type=jnp.float32).reshape(REQ, TREE, HEADS, HEAD)
    key_new = jnp.dot(flat_rows, w_key, preferred_element_type=jnp.float32).reshape(REQ, TREE, KV_HEADS, HEAD)
    val_new = jnp.dot(flat_rows, w_value, preferred_element_type=jnp.float32).astype(jnp.bfloat16).reshape(REQ, TREE, KV_HEADS, HEAD)
    cos_tab, sin_tab = rope_tables(positions, HEAD)
    query = apply_rope(query, cos_tab, sin_tab).astype(jnp.bfloat16)
    key_new = apply_rope(key_new, cos_tab, sin_tab).astype(jnp.bfloat16)

    def attend_one(item):
        q_one, key_one, val_one, cache_k_one, cache_v_one, ctx_one, mask_one = item
        keys_all = jnp.transpose(cache_k_one, (0, 1, 3, 2, 4)).reshape(max_len, KV_HEADS, HEAD).astype(jnp.float32)
        vals_all = jnp.transpose(cache_v_one, (0, 1, 3, 2, 4)).reshape(max_len, KV_HEADS, HEAD).astype(jnp.float32)
        q_wide = q_one.reshape(TREE, KV_HEADS, group, HEAD).astype(jnp.float32)
        score_cache = jnp.einsum('tkgd,lkd->tkgl', q_wide, keys_all) * scale
        valid = jnp.arange(max_len) < ctx_one
        score_cache = jnp.where(valid, score_cache, MASKED)
        score_tree = jnp.einsum('tkgd,skd->tkgs', q_wide, key_one.astype(jnp.float32)) * scale
        tree_ok = (mask_one > 0)[:, None, None, :]
        score_tree = jnp.where(tree_ok, score_tree, MASKED)
        row_max = jnp.maximum(score_cache.max(axis=-1), score_tree.max(axis=-1))
        prob_cache = jnp.exp(score_cache - row_max[..., None])
        prob_tree = jnp.exp(score_tree - row_max[..., None])
        row_sum = prob_cache.sum(axis=-1) + prob_tree.sum(axis=-1)
        mixed = jnp.einsum('tkgl,lkd->tkgd', prob_cache, vals_all) + jnp.einsum('tkgs,skd->tkgd', prob_tree, val_one.astype(jnp.float32))
        return (mixed / row_sum[..., None]).reshape(TREE, HEADS * HEAD).astype(jnp.bfloat16)

    attn = lax.map(attend_one, (query, key_new, val_new, cache_k, cache_v, ctx_len, tree_mask))
    head_part = HEADS * HEAD // TP
    grouped = attn.reshape(REQ, TREE, TP, head_part).astype(jnp.float32)
    proj = jnp.einsum('rtgf,gfe->rtge', grouped, w_out.reshape(TP, head_part, D).astype(jnp.float32)).astype(jnp.bfloat16)
    out_hidden = (wide + proj.astype(jnp.float32).sum(axis=2)).astype(jnp.bfloat16)
    slot_ids = ctx_len[:, None] + jnp.arange(TREE)[None, :]
    block_ids = slot_ids // BLOCK
    req_ids = jnp.broadcast_to(jnp.arange(REQ)[:, None], (REQ, TREE))
    new_cache_k = cache_k.at[req_ids, block_ids // CP, block_ids % CP, :, slot_ids % BLOCK, :].set(key_new)
    new_cache_v = cache_v.at[req_ids, block_ids // CP, block_ids % CP, :, slot_ids % BLOCK, :].set(val_new)
    return (out_hidden, new_cache_k, new_cache_v)
```

```python
import functools
import math
import jax
import jax.numpy as jnp
from jax import lax
from jax.experimental import pallas as pl
from jax.experimental.pallas import tpu as pltpu
from jax.sharding import PartitionSpec as P

ROPE_THETA = 500000.0
NORM_EPS = 1e-5
MASKED = -1e30
LOG2E = math.log2(math.e)
MESH = pl.DeviceIdType.MESH
F32 = jnp.float32
BF16 = jnp.bfloat16
CHUNK = 4


def mm(a, b):
    return jnp.dot(a, b, preferred_element_type=F32)


def mm_tn(a, b):
    return lax.dot_general(a, b, (((0,), (0,)), ((), ())), preferred_element_type=F32)


def rope_tables(positions, head_dim):
    freq_idx = jnp.arange(head_dim // 2, dtype=F32)
    inv_freq = 1.0 / (ROPE_THETA ** (2.0 * freq_idx / head_dim))
    wavelen = 2.0 * math.pi / inv_freq
    smooth = (8192.0 / wavelen - 1.0) / 3.0
    blended = (1.0 - smooth) * inv_freq / 8.0 + smooth * inv_freq
    inv_freq = jnp.where(wavelen < 2048.0, inv_freq, jnp.where(wavelen > 8192.0, inv_freq / 8.0, blended))
    angle = positions.astype(F32)[:, None, :] * inv_freq[None, :, None]
    return jnp.cos(angle), jnp.sin(angle)


def qkv_kernel(ctx_ref, x_ref, gain_ref, wq_ref, wk_ref, wv_ref, cos_ref, sin_ref, kc_hbm, vc_hbm,
               q_ref, ko_hbm, vo_hbm, buf, new_ref, in_sem, out_sem):
    step, steps = pl.program_id(0), pl.num_programs(0)
    cp_rank, cp_size = lax.axis_index('cp'), lax.axis_size('cp')
    slot = lax.rem(step, 2)
    num_blocks, kv_heads, hd, blk = buf.shape[3:]
    half = hd // 2
    tree = x_ref.shape[0] // CHUNK
    heads = q_ref.shape[1]
    group = q_ref.shape[3] // tree

    def fetch(idx, to):
        rows = pl.ds(idx * CHUNK, CHUNK)
        return [pltpu.make_async_copy(src.at[rows], buf.at[to, n], in_sem.at[to, n]) for n, src in enumerate((kc_hbm, vc_hbm))]

    def flush(idx, frm):
        rows = pl.ds(idx * CHUNK, CHUNK)
        return [pltpu.make_async_copy(buf.at[frm, n], dst.at[rows], out_sem.at[frm, n]) for n, dst in enumerate((ko_hbm, vo_hbm))]

    @pl.when(step == 0)
    def _():
        for c in fetch(0, 0):
            c.start()

    @pl.when(step >= 1)
    def _():
        for c in flush(step - 1, 1 - slot):
            c.wait()

    @pl.when(step + 1 < steps)
    def _():
        for c in fetch(step + 1, 1 - slot):
            c.start()

    wide = x_ref[...].astype(F32)
    inv_rms = lax.rsqrt(jnp.mean(wide * wide, axis=-1, keepdims=True) + NORM_EPS)
    h = (wide * inv_rms * gain_ref[...].astype(F32)).astype(BF16)
    cos, sin = cos_ref[0], sin_ref[0]

    def rotate(rows):
        first, second = rows[:half], rows[half:]
        return jnp.concatenate([first * cos - second * sin, second * cos + first * sin], axis=0)

    key_t = mm(h, wk_ref[...]).T
    for n in range(kv_heads):
        new_ref[0, n * hd:(n + 1) * hd, :] = rotate(key_t[n * hd:(n + 1) * hd]).astype(BF16)
    new_ref[1] = mm(h, wv_ref[...]).T.astype(BF16)

    for c in fetch(step, slot):
        c.wait()
    cols = CHUNK * tree
    for i in range(CHUNK):
        ctx = ctx_ref[step * CHUNK + i]
        for j in range(num_blocks // 2, num_blocks):
            first_pos = (j * cp_size + cp_rank) * blk

            @pl.when((first_pos < ctx + tree) & (first_pos + blk > ctx))
            def _():
                tok = first_pos - ctx + lax.broadcasted_iota(jnp.int32, (cols, blk), 1)
                row = lax.broadcasted_iota(jnp.int32, (cols, blk), 0) - i * tree
                pick = jnp.where((row == tok) & (row >= 0) & (row < tree), 1.0, 0.0).astype(BF16)
                tok_h = first_pos - ctx + lax.broadcasted_iota(jnp.int32, (hd, blk), 1)
                fresh = (tok_h >= 0) & (tok_h < tree)
                for n in range(2):
                    put = mm(new_ref[n], pick)
                    for head in range(kv_heads):
                        old = buf[slot, n, i, j, head].astype(F32)
                        buf[slot, n, i, j, head] = jnp.where(fresh, put[head * hd:(head + 1) * hd], old).astype(BF16)

    for c in flush(step, slot):
        c.start()
    for head in range(heads):
        cols_h = pl.ds(head * group * hd, group * hd)
        q_t = mm(h, wq_ref[:, cols_h]).T
        parts = [rotate(q_t[g * hd:(g + 1) * hd]) for g in range(group)]
        for i in range(CHUNK):
            q_ref[i, head] = jnp.concatenate([p[:, i * tree:(i + 1) * tree] for p in parts], axis=1).astype(BF16)

    @pl.when(step == steps - 1)
    def _():
        for c in flush(step, slot):
            c.wait()


def attend_kernel(ctx_ref, q_ref, bias_ref, kc_hbm, vc_hbm, hid_hbm, wo_hbm, y_ref,
                  kbuf, vbuf, kext, qext, scores, msg, rpart, xsend, xrecv, psend, precv, wout, resid,
                  kv_sem, w_sem, hid_sem, snd, rcv):
    cp, tp = lax.axis_index('cp'), lax.axis_index('tp')
    chip, core = cp // 2, cp % 2
    partner = {'cp': chip * 2 + 1 - core}
    across_x = {'cp': (1 - chip) * 2 + core}
    across_y = {'tp': 1 - tp}
    heads, hd, qcols = q_ref.shape[1:]
    tree = bias_ref.shape[1]
    group = qcols // tree
    num_blocks, blk = kbuf.shape[1], kbuf.shape[4]
    nreq = q_ref.shape[0]
    chunks = nreq // CHUNK
    width = wo_hbm.shape[1]
    wcols = width // 2
    coef = hd ** -0.5 * LOG2E
    own_cols = pl.ds(pl.multiple_of(tp * wcols, wcols), wcols)
    other_cols = pl.ds(pl.multiple_of((1 - tp) * wcols, wcols), wcols)

    def remote(src, dst, k, n, to):
        return pltpu.make_async_remote_copy(src_ref=src, dst_ref=dst, send_sem=snd.at[k, n], recv_sem=rcv.at[k, n], device_id=to, device_id_type=MESH)

    barrier = pltpu.get_barrier_semaphore()
    for to in (partner, across_x, across_y):
        pl.semaphore_signal(barrier, inc=1, device_id=to, device_id_type=MESH)

    def request_of(n):
        return (n // CHUNK) * CHUNK + (2 * (1 - chip) + n % CHUNK) % CHUNK

    def fetch(n):
        r, to = request_of(n), n % 2
        return [pltpu.make_async_copy(kc_hbm.at[r], kbuf.at[to], kv_sem.at[to, 0]),
                pltpu.make_async_copy(vc_hbm.at[r], vbuf.at[to, :, :, pl.ds(0, hd), :], kv_sem.at[to, 1])]

    def weight_copies():
        out = []
        for g in range(group):
            for h in range(heads):
                out.append(pltpu.make_async_copy(wo_hbm.at[pl.ds((h * group + g) * hd, hd)], wout.at[g, pl.ds(h * hd, hd)], w_sem.at[g, h]))
        return out

    def resid_copies():
        return [pltpu.make_async_copy(hid_hbm.at[k * CHUNK + cp, :, own_cols], resid.at[k], hid_sem.at[k]) for k in range(chunks)]

    for c in fetch(0):
        c.start()
    for c in weight_copies() + resid_copies():
        c.start()
    ones = jnp.ones((vbuf.shape[3] - hd, blk), BF16)
    for s in range(2):
        for j in range(num_blocks):
            for h in range(heads):
                vbuf[s, j, h, hd:, :] = ones
    pad = qext.shape[1] - hd - tree
    hide = jnp.where(lax.broadcasted_iota(jnp.int32, (pad, qcols), 0) == 0, MASKED, 0.0).astype(BF16)
    for h in range(heads):
        qext[h, hd + tree:, :] = hide
    pl.semaphore_wait(barrier, 3)
    for c in weight_copies() + resid_copies():
        c.wait()

    def attend(n):
        k, r, slot = n // CHUNK, request_of(n), n % 2
        i = r - k * CHUNK

        @pl.when(n + 1 < nreq)
        def _():
            for c in fetch(n + 1):
                c.start()

        ctx = ctx_ref[r]
        bias = bias_ref[r]
        for h in range(heads):
            qext[h, :hd, :] = q_ref[r, h]
            qext[h, hd:hd + tree, :] = bias
        for c in fetch(n):
            c.wait()
        late = num_blocks // 2
        for j in range(late, num_blocks):
            off = (j * 4 + cp) * blk - ctx
            tok = off + lax.broadcasted_iota(jnp.int32, (tree, blk), 1)
            pick = jnp.where(tok == lax.broadcasted_iota(jnp.int32, (tree, blk), 0), 1.0, 0.0).astype(BF16)
            tok_p = off + lax.broadcasted_iota(jnp.int32, (pad, blk), 1)
            tail = jnp.where((tok_p >= tree) & (lax.broadcasted_iota(jnp.int32, (pad, blk), 0) == 0), 1.0, 0.0).astype(BF16)
            tok_h = off + lax.broadcasted_iota(jnp.int32, (hd, blk), 1)
            for h in range(heads):
                kext[j - late, h, :hd, :] = jnp.where(tok_h < tree, kbuf[slot, j, h].astype(F32), 0.0).astype(BF16)
                kext[j - late, h, hd:hd + tree, :] = pick
                kext[j - late, h, hd + tree:, :] = tail

        def score(h, j):
            if j < late:
                s = mm_tn(kbuf[slot, j, h], qext[h, :hd, :])
            else:
                s = mm_tn(kext[j - late, h], qext[h])
            scores[h % 2, j * blk:(j + 1) * blk, :] = s
            return jnp.max(s.reshape(blk // 8, 8, qcols), axis=0)

        tops = [None] * heads
        tops[0] = functools.reduce(jnp.maximum, [score(0, j) for j in range(num_blocks)])
        for h in range(heads):
            top = jnp.max(tops[h], axis=0, keepdims=True)
            shift = top * coef
            total, nxt = None, []
            for j in range(num_blocks):
                if h + 1 < heads:
                    nxt.append(score(h + 1, j))
                p = jnp.exp2(scores[h % 2, j * blk:(j + 1) * blk, :] * coef - shift).astype(BF16)
                o = mm(vbuf[slot, j, h], p)
                total = o if total is None else total + o
            if h + 1 < heads:
                tops[h + 1] = functools.reduce(jnp.maximum, nxt)
            msg[k, i, h * hd:(h + 1) * hd, :] = total[:hd]
            msg[k, i, heads * hd + h:heads * hd + h + 1, :] = top
            msg[k, i, heads * hd + heads + h:heads * hd + heads + h + 1, :] = total[hd:hd + 1]

        which = (n % CHUNK) // 2

        @pl.when(i % 2 != core)
        def _():
            remote(msg.at[k, i], rpart.at[k, which], k, which, partner).start()

    stat = heads * hd

    def scales(parts, h):
        tops = [p[stat + h:stat + h + 1, :] for p in parts]
        top = functools.reduce(jnp.maximum, tops)
        return top, [jnp.exp2((t - top) * coef) for t in tops]

    def merge_chip(k):
        remote(msg.at[k, 0], rpart.at[k, 0], k, 0, partner).wait_recv()
        parts = [msg.at[k, 2 * (1 - chip) + core], rpart.at[k, 0]]
        for h in range(heads):
            top, fac = scales(parts, h)
            rows = slice(h * hd, (h + 1) * hd)
            xsend[k, rows, :] = sum(p[rows, :] * f for p, f in zip(parts, fac))
            xsend[k, stat + h:stat + h + 1, :] = top
            srow = slice(stat + heads + h, stat + heads + h + 1)
            xsend[k, srow, :] = sum(p[srow, :] * f for p, f in zip(parts, fac))
        remote(xsend.at[k], xrecv.at[k], k, 2, across_x).start()

    def project(k):
        remote(msg.at[k, 0], rpart.at[k, 1], k, 1, partner).wait_recv()
        remote(xsend.at[k], xrecv.at[k], k, 2, across_x).wait_recv()
        parts = [msg.at[k, cp], rpart.at[k, 1], xrecv.at[k]]
        outs = []
        for h in range(heads):
            _, fac = scales(parts, h)
            rows = slice(h * hd, (h + 1) * hd)
            srow = slice(stat + heads + h, stat + heads + h + 1)
            inv = 1.0 / sum(p[srow, :] * f for p, f in zip(parts, fac))
            outs.append(sum(p[rows, :] * (f * inv) for p, f in zip(parts, fac)))
        attn = jnp.concatenate(outs, axis=0).T.astype(BF16)

        def part(cols):
            acc = None
            for g in range(group):
                d = mm(attn[g * tree:(g + 1) * tree], wout[g, :, cols])
                acc = d if acc is None else acc + d
            return acc.astype(BF16).astype(F32)

        psend[k] = part(other_cols)
        remote(psend.at[k], precv.at[k], k, 3, across_y).start()
        y_ref[k * CHUNK + cp, :, own_cols] = resid[k].astype(F32) + part(own_cols)

    def piece(k, owner_cp, owner_tp, lo=0, n=None):
        rows = pl.ds(lo, tree if n is None else n)
        return y_ref.at[k * CHUNK + owner_cp, rows, pl.ds(pl.multiple_of(owner_tp * wcols, wcols), wcols)]

    hf = tree // 2
    pcp, xcp, dcp = chip * 2 + 1 - core, (1 - chip) * 2 + core, (1 - chip) * 2 + 1 - core

    def gather_copy(k, n):
        if n == 4:
            return remote(piece(k, cp, tp), piece(k, cp, tp), k, n, across_x)
        if n == 5:
            return remote(piece(k, cp, tp), piece(k, cp, tp), k, n, across_y)
        if n == 6:
            return remote(piece(k, cp, tp), piece(k, cp, tp), k, n, partner)
        if n == 7:
            return remote(piece(k, xcp, tp, 0, hf), piece(k, xcp, tp, 0, hf), k, n, across_y)
        if n == 8:
            return remote(piece(k, xcp, tp), piece(k, xcp, tp), k, n, partner)
        if n == 9:
            return remote(piece(k, cp, 1 - tp, hf, hf), piece(k, cp, 1 - tp, hf, hf), k, n, across_x)
        if n == 10:
            return remote(piece(k, cp, 1 - tp), piece(k, cp, 1 - tp), k, n, partner)
        if n == 11:
            return remote(piece(k, xcp, 1 - tp, 0, hf), piece(k, xcp, 1 - tp, 0, hf), k, n, partner)
        return remote(piece(k, xcp, 1 - tp, hf, hf), piece(k, xcp, 1 - tp, hf, hf), k, n, partner)

    def landed(k, n):
        src = {4: (xcp, tp, 0, tree), 5: (cp, 1 - tp, 0, tree), 6: (pcp, tp, 0, tree), 7: (xcp, 1 - tp, 0, hf), 8: (dcp, tp, 0, tree),
               9: (xcp, 1 - tp, hf, hf), 10: (pcp, 1 - tp, 0, tree), 11: (dcp, 1 - tp, 0, hf), 12: (dcp, 1 - tp, hf, hf)}[n]
        ref = piece(k, *src)
        remote(ref, ref, k, n, partner).wait_recv()

    def finish(k):
        remote(psend.at[k], precv.at[k], k, 3, across_y).wait_recv()
        total = y_ref[k * CHUNK + cp, :, own_cols] + precv[k]
        y_ref[k * CHUNK + cp, :, own_cols] = total.astype(BF16).astype(F32)
        for n in (4, 5, 6):
            gather_copy(k, n).start()

    def forward(k):
        landed(k, 4)
        gather_copy(k, 7).start()
        gather_copy(k, 8).start()
        landed(k, 5)
        gather_copy(k, 9).start()
        gather_copy(k, 10).start()

    def forward_diagonal(k):
        landed(k, 7)
        gather_copy(k, 11).start()
        landed(k, 9)
        gather_copy(k, 12).start()

    @pl.loop(0, chunks + 4)
    def _(k):
        @pl.when(k < chunks)
        def _():
            @pl.loop(0, CHUNK)
            def _(ii):
                attend(k * CHUNK + ii)

            merge_chip(k)

        @pl.when((k >= 1) & (k < chunks + 1))
        def _():
            project(k - 1)

        @pl.when((k >= 2) & (k < chunks + 2))
        def _():
            finish(k - 2)

        @pl.when((k >= 3) & (k < chunks + 3))
        def _():
            forward(k - 3)

        @pl.when(k >= 4)
        def _():
            forward_diagonal(k - 4)

    @pl.loop(0, chunks)
    def _(k):
        for n in (6, 8, 10, 11, 12):
            landed(k, n)
        remote(msg.at[k, 0], rpart.at[k, 0], k, 0, partner).wait_send()
        remote(msg.at[k, 0], rpart.at[k, 1], k, 1, partner).wait_send()
        remote(xsend.at[k], xrecv.at[k], k, 2, across_x).wait_send()
        remote(psend.at[k], precv.at[k], k, 3, across_y).wait_send()
        for n in range(4, 13):
            gather_copy(k, n).wait_send()


def solution(mesh):
    cache_spec = P('dp', None, 'cp', 'tp')
    row_spec = P('dp')

    def local_step(hidden, attn_gain, w_query, w_key, w_value, w_out, cache_k, cache_v, ctx_len, positions, tree_mask):
        nreq, tree, width = hidden.shape
        num_blocks, kv_heads, blk, hd = cache_k.shape[1], cache_k.shape[3], cache_k.shape[4], cache_k.shape[5]
        qdim, kvdim = w_query.shape[1], w_key.shape[1]
        group = qdim // kvdim
        chunks = nreq // CHUNK
        rows = CHUNK * tree
        keys = jnp.swapaxes(cache_k[:, :, 0], -1, -2)
        values = jnp.swapaxes(cache_v[:, :, 0], -1, -2)
        cos, sin = rope_tables(positions.reshape(chunks, rows), hd)
        hbm = pl.BlockSpec(memory_space=pl.ANY)
        vmem = pl.BlockSpec(memory_space=pltpu.VMEM)
        smem = pl.BlockSpec(memory_space=pltpu.SMEM)
        cache_shape = jax.ShapeDtypeStruct(keys.shape, BF16)
        query, new_keys, new_vals = pl.pallas_call(
            qkv_kernel,
            grid=(chunks,),
            in_specs=[smem, pl.BlockSpec((rows, width), lambda s: (s, 0)), pl.BlockSpec((1, width), lambda s: (0, 0)),
                      pl.BlockSpec((width, qdim), lambda s: (0, 0)), pl.BlockSpec((width, kvdim), lambda s: (0, 0)), pl.BlockSpec((width, kvdim), lambda s: (0, 0)),
                      pl.BlockSpec((1, hd // 2, rows), lambda s: (s, 0, 0)), pl.BlockSpec((1, hd // 2, rows), lambda s: (s, 0, 0)), hbm, hbm],
            out_specs=[pl.BlockSpec((CHUNK, kv_heads, hd, group * tree), lambda s: (s, 0, 0, 0)), hbm, hbm],
            out_shape=[jax.ShapeDtypeStruct((nreq, kv_heads, hd, group * tree), BF16), cache_shape, cache_shape],
            scratch_shapes=[pltpu.VMEM((2, 2, CHUNK, num_blocks, kv_heads, hd, blk), BF16), pltpu.VMEM((2, kvdim, rows), BF16),
                            pltpu.SemaphoreType.DMA((2, 2)), pltpu.SemaphoreType.DMA((2, 2))],
            compiler_params=pltpu.CompilerParams(vmem_limit_bytes=58 * 2**20),
            name='qkv_and_cache',
        )(ctx_len, hidden.reshape(nreq * tree, width), attn_gain.reshape(1, width), w_query, w_key, w_value, cos, sin, keys, values)
        bias = jnp.where(jnp.swapaxes(tree_mask, 1, 2) > 0, 0.0, MASKED).astype(BF16)
        bias = jnp.tile(bias, (1, 1, group))
        qcols = group * tree
        rows_msg = kv_heads * hd + 2 * kv_heads
        ext = hd + tree + 16
        wide_y = pl.pallas_call(
            attend_kernel,
            in_specs=[smem, vmem, vmem, hbm, hbm, hbm, hbm],
            out_specs=vmem,
            out_shape=jax.ShapeDtypeStruct((nreq, tree, width), F32),
            scratch_shapes=[
                pltpu.VMEM((2, num_blocks, kv_heads, hd, blk), BF16),
                pltpu.VMEM((2, num_blocks, kv_heads, hd + 16, blk), BF16),
                pltpu.VMEM((num_blocks - num_blocks // 2, kv_heads, ext, blk), BF16),
                pltpu.VMEM((kv_heads, ext, qcols), BF16),
                pltpu.VMEM((2, num_blocks * blk, qcols), F32),
                pltpu.VMEM((chunks, CHUNK, rows_msg, qcols), F32),
                pltpu.VMEM((chunks, 2, rows_msg, qcols), F32),
                pltpu.VMEM((chunks, rows_msg, qcols), F32),
                pltpu.VMEM((chunks, rows_msg, qcols), F32),
                pltpu.VMEM((chunks, tree, width // 2), F32),
                pltpu.VMEM((chunks, tree, width // 2), F32),
                pltpu.VMEM((group, kv_heads * hd, width), BF16),
                pltpu.VMEM((chunks, tree, width // 2), BF16),
                pltpu.SemaphoreType.DMA((2, 2)),
                pltpu.SemaphoreType.DMA((group, kv_heads)),
                pltpu.SemaphoreType.DMA((chunks,)),
                pltpu.SemaphoreType.DMA((chunks, 13)),
                pltpu.SemaphoreType.DMA((chunks, 13)),
            ],
            compiler_params=pltpu.CompilerParams(collective_id=0, has_side_effects=True, vmem_limit_bytes=62 * 2**20),
            name='attend_and_combine',
        )(ctx_len, query, bias, new_keys, new_vals, hidden, w_out)
        return (wide_y.astype(BF16), jnp.swapaxes(new_keys, -1, -2)[:, :, None], jnp.swapaxes(new_vals, -1, -2)[:, :, None])

    return jax.shard_map(local_step, mesh=mesh, in_specs=(row_spec, P(), P(None, 'tp'), P(None, 'tp'), P(None, 'tp'), P('tp', None), cache_spec, cache_spec, row_spec, row_spec, row_spec), out_specs=(row_spec, cache_spec, cache_spec), check_vma=False)
```

```python
import functools
import math
import jax
import jax.numpy as jnp
import numpy as np
from jax import lax
from jax.experimental import pallas as pl
from jax.experimental.pallas import tpu as pltpu
from jax.sharding import PartitionSpec as P

ROPE_THETA = 500000.0
NORM_EPS = 1e-5
MASKED = -1e30
LOG2E = math.log2(math.e)
MESH = pl.DeviceIdType.MESH
F32 = jnp.float32
BF16 = jnp.bfloat16
CHUNK = 4


def mm(a, b):
    return jnp.dot(a, b, preferred_element_type=F32)


def mm_tn(a, b):
    return lax.dot_general(a, b, (((0,), (0,)), ((), ())), preferred_element_type=F32)


def rope_frequencies(head_dim):
    freq_idx = np.arange(head_dim // 2, dtype=np.float32)
    inv_freq = np.float32(1.0) / (np.float32(ROPE_THETA) ** (np.float32(2.0) * freq_idx / np.float32(head_dim)))
    wavelen = np.float32(2.0 * math.pi) / inv_freq
    smooth = (np.float32(8192.0) / wavelen - np.float32(1.0)) / np.float32(3.0)
    blended = (np.float32(1.0) - smooth) * inv_freq / np.float32(8.0) + smooth * inv_freq
    inv_freq = np.where(wavelen < 2048.0, inv_freq, np.where(wavelen > 8192.0, inv_freq / np.float32(8.0), blended))
    return np.broadcast_to(inv_freq.astype(np.float32)[:, None], (head_dim // 2, 128))


def qkv_kernel(ctx_ref, x_ref, gain_ref, wq_ref, wk_ref, wv_ref, pos_ref, freq_ref, kc_hbm, vc_hbm,
               q_ref, ko_hbm, vo_hbm, buf, new_ref, in_sem, out_sem):
    step, steps = pl.program_id(0), pl.num_programs(0)
    cp_rank, cp_size = lax.axis_index('cp'), lax.axis_size('cp')
    slot = lax.rem(step, 2)
    num_blocks, kv_heads, hd, blk = buf.shape[3:]
    half = hd // 2
    tree = x_ref.shape[0] // CHUNK
    heads = q_ref.shape[1]
    group = q_ref.shape[3] // tree

    def fetch(idx, to):
        rows = pl.ds(idx * CHUNK, CHUNK)
        return [pltpu.make_async_copy(src.at[rows], buf.at[to, n], in_sem.at[to, n]) for n, src in enumerate((kc_hbm, vc_hbm))]

    def flush(idx, frm):
        rows = pl.ds(idx * CHUNK, CHUNK)
        return [pltpu.make_async_copy(buf.at[frm, n], dst.at[rows], out_sem.at[frm, n]) for n, dst in enumerate((ko_hbm, vo_hbm))]

    @pl.when(step == 0)
    def _():
        for c in fetch(0, 0):
            c.start()

    @pl.when(step >= 1)
    def _():
        for c in flush(step - 1, 1 - slot):
            c.wait()

    @pl.when(step + 1 < steps)
    def _():
        for c in fetch(step + 1, 1 - slot):
            c.start()

    wide = x_ref[...].astype(F32)
    inv_rms = lax.rsqrt(jnp.mean(wide * wide, axis=-1, keepdims=True) + NORM_EPS)
    h = (wide * inv_rms * gain_ref[...].astype(F32)[None, :]).astype(BF16)
    pos = jnp.concatenate([pos_ref[pl.ds(step * CHUNK + i, 1), :] for i in range(CHUNK)], axis=1).astype(F32)
    angle = pos * freq_ref[:, 0:1]
    cos, sin = jnp.cos(angle), jnp.sin(angle)

    def rotate(rows):
        first, second = rows[:half], rows[half:]
        return jnp.concatenate([first * cos - second * sin, second * cos + first * sin], axis=0)

    key_t = mm(h, wk_ref[...]).T
    for n in range(kv_heads):
        new_ref[0, n * hd:(n + 1) * hd, :] = rotate(key_t[n * hd:(n + 1) * hd]).astype(BF16)
    new_ref[1] = mm(h, wv_ref[...]).T.astype(BF16)

    for c in fetch(step, slot):
        c.wait()
    cols = CHUNK * tree
    for i in range(CHUNK):
        ctx = ctx_ref[step * CHUNK + i]
        for j in range(num_blocks // 2, num_blocks):
            first_pos = (j * cp_size + cp_rank) * blk

            @pl.when((first_pos < ctx + tree) & (first_pos + blk > ctx))
            def _():
                tok = first_pos - ctx + lax.broadcasted_iota(jnp.int32, (cols, blk), 1)
                row = lax.broadcasted_iota(jnp.int32, (cols, blk), 0) - i * tree
                pick = jnp.where((row == tok) & (row >= 0) & (row < tree), 1.0, 0.0).astype(BF16)
                tok_h = first_pos - ctx + lax.broadcasted_iota(jnp.int32, (hd, blk), 1)
                fresh = (tok_h >= 0) & (tok_h < tree)
                for n in range(2):
                    put = mm(new_ref[n], pick)
                    for head in range(kv_heads):
                        old = buf[slot, n, i, j, head].astype(F32)
                        buf[slot, n, i, j, head] = jnp.where(fresh, put[head * hd:(head + 1) * hd], old).astype(BF16)

    for c in flush(step, slot):
        c.start()
    for head in range(heads):
        cols_h = pl.ds(head * group * hd, group * hd)
        q_t = mm(h, wq_ref[:, cols_h]).T
        parts = [rotate(q_t[g * hd:(g + 1) * hd]) for g in range(group)]
        for i in range(CHUNK):
            q_ref[i, head] = jnp.concatenate([p[:, i * tree:(i + 1) * tree] for p in parts], axis=1).astype(BF16)

    @pl.when(step == steps - 1)
    def _():
        for c in flush(step, slot):
            c.wait()


def attend_kernel(ctx_ref, q_hbm, mask_hbm, kc_hbm, vc_hbm, hid_hbm, wo_hbm, out_hbm,
                  y_ref, kbuf, vbuf, kext, qext, mbuf, scores, msg, rpart, xsend, xrecv, psend, precv, wout, resid, stage,
                  kv_sem, w_sem, hid_sem, out_sem, snd, rcv):
    cp, tp = lax.axis_index('cp'), lax.axis_index('tp')
    chip, core = cp // 2, cp % 2
    partner = {'cp': chip * 2 + 1 - core}
    across_x = {'cp': (1 - chip) * 2 + core}
    across_y = {'tp': 1 - tp}
    nreq, heads, hd, qcols = q_hbm.shape
    tree = mask_hbm.shape[1]
    group = qcols // tree
    num_blocks, blk = kbuf.shape[1], kbuf.shape[4]
    chunks = nreq // CHUNK
    width = wo_hbm.shape[1]
    wcols = width // 2
    coef = hd ** -0.5 * LOG2E
    own_cols = pl.ds(pl.multiple_of(tp * wcols, wcols), wcols)
    other_cols = pl.ds(pl.multiple_of((1 - tp) * wcols, wcols), wcols)

    def remote(src, dst, k, n, to):
        return pltpu.make_async_remote_copy(src_ref=src, dst_ref=dst, send_sem=snd.at[k, n], recv_sem=rcv.at[k, n], device_id=to, device_id_type=MESH)

    barrier = pltpu.get_barrier_semaphore()
    for to in (partner, across_x, across_y):
        pl.semaphore_signal(barrier, inc=1, device_id=to, device_id_type=MESH)

    def request_of(n):
        return (n // CHUNK) * CHUNK + (2 * (1 - chip) + n % CHUNK) % CHUNK

    def fetch(n):
        r, to = request_of(n), n % 2
        return [pltpu.make_async_copy(kc_hbm.at[r], kbuf.at[to], kv_sem.at[to, 0]),
                pltpu.make_async_copy(vc_hbm.at[r], vbuf.at[to, :, :, pl.ds(0, hd), :], kv_sem.at[to, 1]),
                pltpu.make_async_copy(q_hbm.at[r], qext.at[to, :, pl.ds(0, hd), :], kv_sem.at[to, 2]),
                pltpu.make_async_copy(mask_hbm.at[r], mbuf.at[to], kv_sem.at[to, 3])]

    def weight_copies():
        out = []
        for g in range(group):
            for h in range(heads):
                out.append(pltpu.make_async_copy(wo_hbm.at[pl.ds((h * group + g) * hd, hd)], wout.at[g, pl.ds(h * hd, hd)], w_sem.at[g, h]))
        return out

    def resid_copies():
        return [pltpu.make_async_copy(hid_hbm.at[k * CHUNK + cp, :, own_cols], resid.at[k], hid_sem.at[k]) for k in range(chunks)]

    for c in fetch(0):
        c.start()
    for c in weight_copies() + resid_copies():
        c.start()
    ones = jnp.ones((vbuf.shape[3] - hd, blk), BF16)
    for s in range(2):
        for j in range(num_blocks):
            for h in range(heads):
                vbuf[s, j, h, hd:, :] = ones
    pad = qext.shape[2] - hd - tree
    hide = jnp.where(lax.broadcasted_iota(jnp.int32, (pad, qcols), 0) == 0, MASKED, 0.0).astype(BF16)
    for s in range(2):
        for h in range(heads):
            qext[s, h, hd + tree:, :] = hide
    pl.semaphore_wait(barrier, 3)

    def attend(n):
        k, r, slot = n // CHUNK, request_of(n), n % 2
        i = r - k * CHUNK

        @pl.when(n + 1 < nreq)
        def _():
            for c in fetch(n + 1):
                c.start()

        ctx = ctx_ref[r]
        for c in fetch(n):
            c.wait()
        seen = jnp.concatenate([mbuf[slot].astype(F32)] * group, axis=0).T
        bias = jnp.where(seen > 0.0, 0.0, MASKED).astype(BF16)
        for h in range(heads):
            qext[slot, h, hd:hd + tree, :] = bias
        late = num_blocks // 2
        for j in range(late, num_blocks):
            off = (j * 4 + cp) * blk - ctx
            tok = off + lax.broadcasted_iota(jnp.int32, (tree, blk), 1)
            pick = jnp.where(tok == lax.broadcasted_iota(jnp.int32, (tree, blk), 0), 1.0, 0.0).astype(BF16)
            tok_p = off + lax.broadcasted_iota(jnp.int32, (pad, blk), 1)
            tail = jnp.where((tok_p >= tree) & (lax.broadcasted_iota(jnp.int32, (pad, blk), 0) == 0), 1.0, 0.0).astype(BF16)
            tok_h = off + lax.broadcasted_iota(jnp.int32, (hd, blk), 1)
            for h in range(heads):
                kext[j - late, h, :hd, :] = jnp.where(tok_h < tree, kbuf[slot, j, h].astype(F32), 0.0).astype(BF16)
                kext[j - late, h, hd:hd + tree, :] = pick
                kext[j - late, h, hd + tree:, :] = tail

        def score(h, j):
            if j < late:
                s = mm_tn(kbuf[slot, j, h], qext[slot, h, :hd, :])
            else:
                s = mm_tn(kext[j - late, h], qext[slot, h])
            scores[h % 2, j * blk:(j + 1) * blk, :] = s
            return jnp.max(s.reshape(blk // 8, 8, qcols), axis=0)

        tops = [None] * heads
        tops[0] = functools.reduce(jnp.maximum, [score(0, j) for j in range(num_blocks)])
        for h in range(heads):
            top = jnp.max(tops[h], axis=0, keepdims=True)
            shift = top * coef
            total, nxt = None, []
            for j in range(num_blocks):
                if h + 1 < heads:
                    nxt.append(score(h + 1, j))
                p = jnp.exp2(scores[h % 2, j * blk:(j + 1) * blk, :] * coef - shift).astype(BF16)
                o = mm(vbuf[slot, j, h], p)
                total = o if total is None else total + o
            if h + 1 < heads:
                tops[h + 1] = functools.reduce(jnp.maximum, nxt)
            msg[k, i, h * hd:(h + 1) * hd, :] = total[:hd]
            msg[k, i, heads * hd + h:heads * hd + h + 1, :] = top
            msg[k, i, heads * hd + heads + h:heads * hd + heads + h + 1, :] = total[hd:hd + 1]

        which = (n % CHUNK) // 2

        @pl.when(i % 2 != core)
        def _():
            remote(msg.at[k, i], rpart.at[k, which], k, which, partner).start()

    stat = heads * hd

    def scales(parts, h):
        tops = [p[stat + h:stat + h + 1, :] for p in parts]
        top = functools.reduce(jnp.maximum, tops)
        return top, [jnp.exp2((t - top) * coef) for t in tops]

    def merge_chip(k):
        remote(msg.at[k, 0], rpart.at[k, 0], k, 0, partner).wait_recv()
        parts = [msg.at[k, 2 * (1 - chip) + core], rpart.at[k, 0]]
        for h in range(heads):
            top, fac = scales(parts, h)
            rows = slice(h * hd, (h + 1) * hd)
            xsend[k, rows, :] = sum(p[rows, :] * f for p, f in zip(parts, fac))
            xsend[k, stat + h:stat + h + 1, :] = top
            srow = slice(stat + heads + h, stat + heads + h + 1)
            xsend[k, srow, :] = sum(p[srow, :] * f for p, f in zip(parts, fac))
        remote(xsend.at[k], xrecv.at[k], k, 2, across_x).start()

    def project(k):
        remote(msg.at[k, 0], rpart.at[k, 1], k, 1, partner).wait_recv()
        remote(xsend.at[k], xrecv.at[k], k, 2, across_x).wait_recv()
        parts = [msg.at[k, cp], rpart.at[k, 1], xrecv.at[k]]
        outs = []
        for h in range(heads):
            _, fac = scales(parts, h)
            rows = slice(h * hd, (h + 1) * hd)
            srow = slice(stat + heads + h, stat + heads + h + 1)
            inv = 1.0 / sum(p[srow, :] * f for p, f in zip(parts, fac))
            outs.append(sum(p[rows, :] * (f * inv) for p, f in zip(parts, fac)))
        attn = jnp.concatenate(outs, axis=0).T.astype(BF16)

        @pl.when(k == 0)
        def _():
            for c in weight_copies() + resid_copies():
                c.wait()

        def part(cols):
            acc = None
            for g in range(group):
                d = mm(attn[g * tree:(g + 1) * tree], wout[g, :, cols])
                acc = d if acc is None else acc + d
            return acc.astype(BF16).astype(F32)

        psend[k] = part(other_cols)
        remote(psend.at[k], precv.at[k], k, 3, across_y).start()
        y_ref[k * CHUNK + cp, :, own_cols] = resid[k].astype(F32) + part(own_cols)

    def piece(k, owner_cp, owner_tp, lo=0, n=None):
        rows = pl.ds(lo, tree if n is None else n)
        return y_ref.at[k * CHUNK + owner_cp, rows, pl.ds(pl.multiple_of(owner_tp * wcols, wcols), wcols)]

    hf = (tree * 3 // 8) // 8 * 8
    hb = tree - hf
    pcp, xcp, dcp = chip * 2 + 1 - core, (1 - chip) * 2 + core, (1 - chip) * 2 + 1 - core

    def gather_copy(k, n):
        if n == 4:
            return remote(piece(k, cp, tp), piece(k, cp, tp), k, n, across_x)
        if n == 5:
            return remote(piece(k, cp, tp), piece(k, cp, tp), k, n, across_y)
        if n == 6:
            return remote(piece(k, cp, tp), piece(k, cp, tp), k, n, partner)
        if n == 7:
            return remote(piece(k, xcp, tp, 0, hf), piece(k, xcp, tp, 0, hf), k, n, across_y)
        if n == 8:
            return remote(piece(k, xcp, tp), piece(k, xcp, tp), k, n, partner)
        if n == 9:
            return remote(piece(k, cp, 1 - tp, hf, hb), piece(k, cp, 1 - tp, hf, hb), k, n, across_x)
        if n == 10:
            return remote(piece(k, cp, 1 - tp), piece(k, cp, 1 - tp), k, n, partner)
        if n == 11:
            return remote(piece(k, xcp, 1 - tp, 0, hf), piece(k, xcp, 1 - tp, 0, hf), k, n, partner)
        return remote(piece(k, xcp, 1 - tp, hf, hb), piece(k, xcp, 1 - tp, hf, hb), k, n, partner)

    def landed(k, n):
        src = {4: (xcp, tp, 0, tree), 5: (cp, 1 - tp, 0, tree), 6: (pcp, tp, 0, tree), 7: (xcp, 1 - tp, 0, hf), 8: (dcp, tp, 0, tree),
               9: (xcp, 1 - tp, hf, hb), 10: (pcp, 1 - tp, 0, tree), 11: (dcp, 1 - tp, 0, hf), 12: (dcp, 1 - tp, hf, hb)}[n]
        ref = piece(k, *src)
        remote(ref, ref, k, n, partner).wait_recv()

    def finish(k):
        remote(psend.at[k], precv.at[k], k, 3, across_y).wait_recv()
        total = y_ref[k * CHUNK + cp, :, own_cols] + precv[k]
        y_ref[k * CHUNK + cp, :, own_cols] = total.astype(BF16).astype(F32)
        for n in (4, 5, 6):
            gather_copy(k, n).start()

    def forward(k):
        landed(k, 4)
        gather_copy(k, 7).start()
        gather_copy(k, 8).start()
        landed(k, 5)
        gather_copy(k, 9).start()
        gather_copy(k, 10).start()

    def forward_diagonal(k):
        landed(k, 7)
        gather_copy(k, 11).start()
        landed(k, 9)
        gather_copy(k, 12).start()

    def out_copy(k):
        return pltpu.make_async_copy(stage.at[k % 2], out_hbm.at[pl.ds(k * CHUNK, CHUNK)], out_sem.at[k % 2])

    def emit(k):
        for n in (6, 8, 10, 11, 12):
            landed(k, n)

        @pl.when(k >= 2)
        def _():
            out_copy(k - 2).wait()

        for i in range(CHUNK):
            stage[k % 2, i] = y_ref[k * CHUNK + i].astype(BF16)
        out_copy(k).start()

    steps = ((merge_chip, 3), (project, 7), (finish, 11), (forward, 15), (forward_diagonal, 19), (emit, 23))

    @pl.loop(0, nreq + steps[-1][1])
    def _(n):
        @pl.when(n < nreq)
        def _():
            attend(n)

        for work, after in steps:
            since = n + 1 - after

            @pl.when((since >= 0) & (since < nreq) & (since % CHUNK == 0))
            def _():
                work(since // CHUNK)

    for k in range(chunks - 2, chunks):
        out_copy(k).wait()

    @pl.loop(0, chunks)
    def _(k):
        remote(msg.at[k, 0], rpart.at[k, 0], k, 0, partner).wait_send()
        remote(msg.at[k, 0], rpart.at[k, 1], k, 1, partner).wait_send()
        remote(xsend.at[k], xrecv.at[k], k, 2, across_x).wait_send()
        remote(psend.at[k], precv.at[k], k, 3, across_y).wait_send()
        for n in range(4, 13):
            gather_copy(k, n).wait_send()


def solution(mesh):
    cache_spec = P('dp', None, 'cp', 'tp')
    row_spec = P('dp')

    def local_step(hidden, attn_gain, w_query, w_key, w_value, w_out, cache_k, cache_v, ctx_len, positions, tree_mask):
        nreq, tree, width = hidden.shape
        num_blocks, kv_heads, blk, hd = cache_k.shape[1], cache_k.shape[3], cache_k.shape[4], cache_k.shape[5]
        qdim, kvdim = w_query.shape[1], w_key.shape[1]
        group = qdim // kvdim
        chunks = nreq // CHUNK
        rows = CHUNK * tree
        keys = jnp.swapaxes(cache_k[:, :, 0], -1, -2)
        values = jnp.swapaxes(cache_v[:, :, 0], -1, -2)
        hbm = pl.BlockSpec(memory_space=pl.ANY)
        smem = pl.BlockSpec(memory_space=pltpu.SMEM)
        cache_shape = jax.ShapeDtypeStruct(keys.shape, BF16)
        query, new_keys, new_vals = pl.pallas_call(
            qkv_kernel,
            grid=(chunks,),
            in_specs=[smem, pl.BlockSpec((rows, width), lambda s: (s, 0)), pl.BlockSpec((width,), lambda s: (0,)),
                      pl.BlockSpec((width, qdim), lambda s: (0, 0)), pl.BlockSpec((width, kvdim), lambda s: (0, 0)), pl.BlockSpec((width, kvdim), lambda s: (0, 0)),
                      pl.BlockSpec((nreq, tree), lambda s: (0, 0)), pl.BlockSpec((hd // 2, 128), lambda s: (0, 0)), hbm, hbm],
            out_specs=[pl.BlockSpec((CHUNK, kv_heads, hd, group * tree), lambda s: (s, 0, 0, 0)), hbm, hbm],
            out_shape=[jax.ShapeDtypeStruct((nreq, kv_heads, hd, group * tree), BF16), cache_shape, cache_shape],
            scratch_shapes=[pltpu.VMEM((2, 2, CHUNK, num_blocks, kv_heads, hd, blk), BF16), pltpu.VMEM((2, kvdim, rows), BF16),
                            pltpu.SemaphoreType.DMA((2, 2)), pltpu.SemaphoreType.DMA((2, 2))],
            compiler_params=pltpu.CompilerParams(vmem_limit_bytes=58 * 2**20),
            name='qkv_and_cache',
        )(ctx_len, hidden.reshape(nreq * tree, width), attn_gain, w_query, w_key, w_value, positions, jnp.asarray(rope_frequencies(hd)), keys, values)
        qcols = group * tree
        rows_msg = kv_heads * hd + 2 * kv_heads
        ext = hd + tree + 16
        out_hidden = pl.pallas_call(
            attend_kernel,
            in_specs=[smem, hbm, hbm, hbm, hbm, hbm, hbm],
            out_specs=hbm,
            out_shape=jax.ShapeDtypeStruct((nreq, tree, width), BF16),
            scratch_shapes=[
                pltpu.VMEM((nreq, tree, width), F32),
                pltpu.VMEM((2, num_blocks, kv_heads, hd, blk), BF16),
                pltpu.VMEM((2, num_blocks, kv_heads, hd + 16, blk), BF16),
                pltpu.VMEM((num_blocks - num_blocks // 2, kv_heads, ext, blk), BF16),
                pltpu.VMEM((2, kv_heads, ext, qcols), BF16),
                pltpu.VMEM((2, tree, tree), jnp.int32),
                pltpu.VMEM((2, num_blocks * blk, qcols), F32),
                pltpu.VMEM((chunks, CHUNK, rows_msg, qcols), F32),
                pltpu.VMEM((chunks, 2, rows_msg, qcols), F32),
                pltpu.VMEM((chunks, rows_msg, qcols), F32),
                pltpu.VMEM((chunks, rows_msg, qcols), F32),
                pltpu.VMEM((chunks, tree, width // 2), F32),
                pltpu.VMEM((chunks, tree, width // 2), F32),
                pltpu.VMEM((group, kv_heads * hd, width), BF16),
                pltpu.VMEM((chunks, tree, width // 2), BF16),
                pltpu.VMEM((2, CHUNK, tree, width), BF16),
                pltpu.SemaphoreType.DMA((2, 4)),
                pltpu.SemaphoreType.DMA((group, kv_heads)),
                pltpu.SemaphoreType.DMA((chunks,)),
                pltpu.SemaphoreType.DMA((2,)),
                pltpu.SemaphoreType.DMA((chunks, 13)),
                pltpu.SemaphoreType.DMA((chunks, 13)),
            ],
            compiler_params=pltpu.CompilerParams(collective_id=0, has_side_effects=True, vmem_limit_bytes=62 * 2**20),
            name='attend_and_combine',
        )(ctx_len, query, tree_mask, new_keys, new_vals, hidden, w_out)
        return (out_hidden, jnp.swapaxes(new_keys, -1, -2)[:, :, None], jnp.swapaxes(new_vals, -1, -2)[:, :, None])

    return jax.shard_map(local_step, mesh=mesh, in_specs=(row_spec, P(), P(None, 'tp'), P(None, 'tp'), P(None, 'tp'), P('tp', None), cache_spec, cache_spec, row_spec, row_spec, row_spec), out_specs=(row_spec, cache_spec, cache_spec), check_vma=False)
```

```python
import functools
import math
import jax
import jax.numpy as jnp
import numpy as np
from jax import lax
from jax.experimental import pallas as pl
from jax.experimental.pallas import tpu as pltpu
from jax.sharding import PartitionSpec as P

ROPE_THETA = 500000.0
NORM_EPS = 1e-5
MASKED = -1e30
LOG2E = math.log2(math.e)
MESH = pl.DeviceIdType.MESH
F32 = jnp.float32
BF16 = jnp.bfloat16
CHUNK = 4


def mm(a, b):
    return jnp.dot(a, b, preferred_element_type=F32)


def mm_tn(a, b):
    return lax.dot_general(a, b, (((0,), (0,)), ((), ())), preferred_element_type=F32)


def rope_frequencies(head_dim):
    freq_idx = np.arange(head_dim // 2, dtype=np.float32)
    inv_freq = np.float32(1.0) / (np.float32(ROPE_THETA) ** (np.float32(2.0) * freq_idx / np.float32(head_dim)))
    wavelen = np.float32(2.0 * math.pi) / inv_freq
    smooth = (np.float32(8192.0) / wavelen - np.float32(1.0)) / np.float32(3.0)
    blended = (np.float32(1.0) - smooth) * inv_freq / np.float32(8.0) + smooth * inv_freq
    return np.where(wavelen < 2048.0, inv_freq, np.where(wavelen > 8192.0, inv_freq / np.float32(8.0), blended)).astype(np.float32)


def normed_rows(x, gain):
    wide = x.astype(F32)
    inv_rms = lax.rsqrt(jnp.mean(wide * wide, axis=-1, keepdims=True) + NORM_EPS)
    return (wide * inv_rms * gain.astype(F32)[None, :]).astype(BF16)


def rotate(rows, cos, sin):
    half = rows.shape[0] // 2
    first, second = rows[:half], rows[half:]
    return jnp.concatenate([first * cos - second * sin, second * cos + first * sin], axis=0)


def project_queries(h, wq_ref, cos, sin, out, hd, group, tree):
    reqs = h.shape[0] // tree
    for head in range(wq_ref.shape[1] // (group * hd)):
        q_t = mm(h, wq_ref[:, head * group * hd:(head + 1) * group * hd]).T
        parts = [rotate(q_t[g * hd:(g + 1) * hd], cos, sin) for g in range(group)]
        for i in range(reqs):
            out(i, head, jnp.concatenate([p[:, i * tree:(i + 1) * tree] for p in parts], axis=1).astype(BF16))


def cache_kernel(ctx_ref, x_ref, gain_ref, wk_ref, wv_ref, pos_ref, freq_ref, wq_hbm, kc_hbm, vc_hbm,
                 q_ref, tab_ref, ko_hbm, vo_hbm, buf, new_ref, wq_ref, in_sem, out_sem, w_sem):
    step, steps = pl.program_id(0), pl.num_programs(0)
    cp_rank, cp_size = lax.axis_index('cp'), lax.axis_size('cp')
    slots, _, per, num_blocks, kv_heads, hd, blk = buf.shape
    slot = lax.rem(step, slots)
    tree = pos_ref.shape[1]
    group = q_ref.shape[3] // tree
    first_req = (steps - 1 - step) * per

    def fetch(idx):
        rows, to = pl.ds((steps - 1 - idx) * per, per), lax.rem(idx, slots)
        return [pltpu.make_async_copy(src.at[rows], buf.at[to, n], in_sem.at[to, n]) for n, src in enumerate((kc_hbm, vc_hbm))]

    def flush(idx):
        rows, frm = pl.ds((steps - 1 - idx) * per, per), lax.rem(idx, slots)
        return [pltpu.make_async_copy(buf.at[frm, n], dst.at[rows], out_sem.at[frm, n]) for n, dst in enumerate((ko_hbm, vo_hbm))]

    wq_copy = pltpu.make_async_copy(wq_hbm, wq_ref, w_sem)

    @pl.when(step == 0)
    def _():
        for c in fetch(0) + fetch(1):
            c.start()

    @pl.when(step == 1)
    def _():
        wq_copy.start()

    @pl.when(step + 2 < steps)
    def _():
        @pl.when(step + 2 >= slots)
        def _():
            for c in flush(step + 2 - slots):
                c.wait()

        for c in fetch(step + 2):
            c.start()

    h = normed_rows(x_ref[...], gain_ref[...])
    half = hd // 2
    diag = lax.broadcasted_iota(jnp.int32, (half, half), 0) == lax.broadcasted_iota(jnp.int32, (half, half), 1)
    freq = jnp.sum(jnp.where(diag, freq_ref[...][None, :], 0.0), axis=1, keepdims=True)
    pos = jnp.concatenate([pos_ref[pl.ds(first_req + i, 1), :] for i in range(per)], axis=1).astype(F32)
    angle = pos * freq
    cos, sin = jnp.cos(angle), jnp.sin(angle)
    tab_ref[0, 0] = cos
    tab_ref[0, 1] = sin
    key_t = mm(h, wk_ref[...]).T
    for n in range(kv_heads):
        new_ref[0, n * hd:(n + 1) * hd, :] = rotate(key_t[n * hd:(n + 1) * hd], cos, sin).astype(BF16)
    new_ref[1] = mm(h, wv_ref[...]).T.astype(BF16)

    for c in fetch(step):
        c.wait()
    cols = per * tree
    for i in range(per):
        ctx = ctx_ref[first_req + i]
        for j in range(num_blocks // 2, num_blocks):
            first_pos = (j * cp_size + cp_rank) * blk

            @pl.when((first_pos < ctx + tree) & (first_pos + blk > ctx))
            def _():
                tok = first_pos - ctx + lax.broadcasted_iota(jnp.int32, (cols, blk), 1)
                row = lax.broadcasted_iota(jnp.int32, (cols, blk), 0) - i * tree
                pick = jnp.where((row == tok) & (row >= 0) & (row < tree), 1.0, 0.0).astype(BF16)
                tok_h = first_pos - ctx + lax.broadcasted_iota(jnp.int32, (hd, blk), 1)
                fresh = (tok_h >= 0) & (tok_h < tree)
                for n in range(2):
                    put = mm(new_ref[n], pick)
                    for head in range(kv_heads):
                        old = buf[slot, n, i, j, head].astype(F32)
                        buf[slot, n, i, j, head] = jnp.where(fresh, put[head * hd:(head + 1) * hd], old).astype(BF16)

    for c in flush(step):
        c.start()

    early = CHUNK // per

    @pl.when(step == steps - early)
    def _():
        wq_copy.wait()

    @pl.when(step >= steps - early)
    def _():
        def out(i, head, value):
            q_ref[i, head] = value

        project_queries(h, wq_ref, cos, sin, out, hd, group, tree)

    @pl.when(step == steps - 1)
    def _():
        for back in range(slots):
            for c in flush(steps - 1 - back):
                c.wait()


def attend_kernel(ctx_ref, gain_ref, q_hbm, tab_hbm, mask_hbm, kc_hbm, vc_hbm, hid_hbm, wq_hbm, wo_hbm, out_ref,
                  y_ref, kbuf, vbuf, kext, qext, mbuf, scores, msg, rpart, xsend, xrecv, psend, precv, wout, resid, wq_ref, xbuf, tbuf, qbuf,
                  kv_sem, w_sem, hid_sem, q_sem, snd, rcv):
    cp, tp = lax.axis_index('cp'), lax.axis_index('tp')
    chip, core = cp // 2, cp % 2
    partner = {'cp': chip * 2 + 1 - core}
    across_x = {'cp': (1 - chip) * 2 + core}
    across_y = {'tp': 1 - tp}
    _, heads, hd, qcols = q_hbm.shape
    nreq = mask_hbm.shape[0]
    tree = mask_hbm.shape[1]
    group = qcols // tree
    num_blocks, blk = kbuf.shape[1], kbuf.shape[4]
    chunks = nreq // CHUNK
    width = wo_hbm.shape[1]
    wcols = width // 2
    coef = hd ** -0.5 * LOG2E
    own_cols = pl.ds(pl.multiple_of(tp * wcols, wcols), wcols)
    other_cols = pl.ds(pl.multiple_of((1 - tp) * wcols, wcols), wcols)

    def remote(src, dst, k, n, to):
        return pltpu.make_async_remote_copy(src_ref=src, dst_ref=dst, send_sem=snd.at[k, n], recv_sem=rcv.at[k, n], device_id=to, device_id_type=MESH)

    barrier = pltpu.get_barrier_semaphore()
    for to in (partner, across_x, across_y):
        pl.semaphore_signal(barrier, inc=1, device_id=to, device_id_type=MESH)

    def request_of(n):
        return (n // CHUNK) * CHUNK + (2 * (1 - chip) + n % CHUNK) % CHUNK

    def fetch(n):
        r, to = request_of(n), n % 2
        return [pltpu.make_async_copy(kc_hbm.at[r], kbuf.at[to], kv_sem.at[to, 0]),
                pltpu.make_async_copy(vc_hbm.at[r], vbuf.at[to, :, :, pl.ds(0, hd), :], kv_sem.at[to, 1]),
                pltpu.make_async_copy(mask_hbm.at[r], mbuf.at[to], kv_sem.at[to, 2])]

    def weight_copies():
        out = []
        for g in range(group):
            for h in range(heads):
                out.append(pltpu.make_async_copy(wo_hbm.at[pl.ds((h * group + g) * hd, hd)], wout.at[g, pl.ds(h * hd, hd)], w_sem.at[g, h]))
        return out

    def resid_copies():
        return [pltpu.make_async_copy(hid_hbm.at[k * CHUNK + cp, :, own_cols], resid.at[k], hid_sem.at[k]) for k in range(chunks)]

    first_queries = pltpu.make_async_copy(q_hbm, qbuf.at[0], q_sem.at[0])
    query_weight = pltpu.make_async_copy(wq_hbm, wq_ref, q_sem.at[1])

    def chunk_copies(k):
        pairs = tbuf.shape[0]
        return [pltpu.make_async_copy(hid_hbm.at[pl.ds(k * CHUNK, CHUNK)], xbuf, q_sem.at[2]),
                pltpu.make_async_copy(tab_hbm.at[pl.ds(k * pairs, pairs)], tbuf, q_sem.at[3])]

    for c in fetch(0) + [first_queries] + chunk_copies(1) + [query_weight] + weight_copies() + resid_copies():
        c.start()
    ones = jnp.ones((vbuf.shape[3] - hd, blk), BF16)
    for s in range(2):
        for j in range(num_blocks):
            for h in range(heads):
                vbuf[s, j, h, hd:, :] = ones
    pad = qext.shape[1] - hd - tree
    hide = jnp.where(lax.broadcasted_iota(jnp.int32, (pad, qcols), 0) == 0, MASKED, 0.0).astype(BF16)
    for h in range(heads):
        qext[h, hd + tree:, :] = hide
    pl.semaphore_wait(barrier, 3)
    first_queries.wait()

    def queries(k):
        for c in chunk_copies(k):
            c.wait()

        @pl.when(k == 1)
        def _():
            query_weight.wait()

        h = normed_rows(xbuf[...].reshape(CHUNK * tree, width), gain_ref[...])
        cos = jnp.concatenate([tbuf[p, 0] for p in range(tbuf.shape[0])], axis=1)
        sin = jnp.concatenate([tbuf[p, 1] for p in range(tbuf.shape[0])], axis=1)

        def out(i, head, value):
            qbuf[k % 2, i, head] = value

        project_queries(h, wq_ref, cos, sin, out, hd, group, tree)

        @pl.when(k + 1 < chunks)
        def _():
            for c in chunk_copies(k + 1):
                c.start()

    def attend(n):
        k, r, slot = n // CHUNK, request_of(n), n % 2
        i = r - k * CHUNK

        @pl.when(n + 1 < nreq)
        def _():
            for c in fetch(n + 1):
                c.start()

        ctx = ctx_ref[r]
        for c in fetch(n):
            c.wait()
        seen = jnp.concatenate([mbuf[slot].astype(F32)] * group, axis=0).T
        bias = jnp.where(seen > 0.0, 0.0, MASKED).astype(BF16)
        for h in range(heads):
            qext[h, :hd, :] = qbuf[k % 2, i, h]
            qext[h, hd:hd + tree, :] = bias
        late = num_blocks // 2
        for j in range(late, num_blocks):
            off = (j * 4 + cp) * blk - ctx
            tok = off + lax.broadcasted_iota(jnp.int32, (tree, blk), 1)
            pick = jnp.where(tok == lax.broadcasted_iota(jnp.int32, (tree, blk), 0), 1.0, 0.0).astype(BF16)
            tok_p = off + lax.broadcasted_iota(jnp.int32, (pad, blk), 1)
            tail = jnp.where((tok_p >= tree) & (lax.broadcasted_iota(jnp.int32, (pad, blk), 0) == 0), 1.0, 0.0).astype(BF16)
            tok_h = off + lax.broadcasted_iota(jnp.int32, (hd, blk), 1)
            for h in range(heads):
                kext[j - late, h, :hd, :] = jnp.where(tok_h < tree, kbuf[slot, j, h].astype(F32), 0.0).astype(BF16)
                kext[j - late, h, hd:hd + tree, :] = pick
                kext[j - late, h, hd + tree:, :] = tail

        def score(h, j):
            if j < late:
                s = mm_tn(kbuf[slot, j, h], qext[h, :hd, :])
            else:
                s = mm_tn(kext[j - late, h], qext[h])
            scores[h % 2, j * blk:(j + 1) * blk, :] = s
            return jnp.max(s.reshape(blk // 8, 8, qcols), axis=0)

        tops = [None] * heads
        tops[0] = functools.reduce(jnp.maximum, [score(0, j) for j in range(num_blocks)])
        for h in range(heads):
            top = jnp.max(tops[h], axis=0, keepdims=True)
            shift = top * coef
            total, nxt = None, []
            for j in range(num_blocks):
                if h + 1 < heads:
                    nxt.append(score(h + 1, j))
                p = jnp.exp2(scores[h % 2, j * blk:(j + 1) * blk, :] * coef - shift).astype(BF16)
                o = mm(vbuf[slot, j, h], p)
                total = o if total is None else total + o
            if h + 1 < heads:
                tops[h + 1] = functools.reduce(jnp.maximum, nxt)
            msg[k, i, h * hd:(h + 1) * hd, :] = total[:hd]
            msg[k, i, heads * hd + h:heads * hd + h + 1, :] = top
            msg[k, i, heads * hd + heads + h:heads * hd + heads + h + 1, :] = total[hd:hd + 1]

        which = (n % CHUNK) // 2

        @pl.when(i % 2 != core)
        def _():
            remote(msg.at[k, i], rpart.at[k, which], k, which, partner).start()

    stat = heads * hd

    def scales(parts, h):
        tops = [p[stat + h:stat + h + 1, :] for p in parts]
        top = functools.reduce(jnp.maximum, tops)
        return top, [jnp.exp2((t - top) * coef) for t in tops]

    def merge_chip(k):
        remote(msg.at[k, 0], rpart.at[k, 0], k, 0, partner).wait_recv()
        parts = [msg.at[k, 2 * (1 - chip) + core], rpart.at[k, 0]]
        for h in range(heads):
            top, fac = scales(parts, h)
            rows = slice(h * hd, (h + 1) * hd)
            xsend[k, rows, :] = sum(p[rows, :] * f for p, f in zip(parts, fac))
            xsend[k, stat + h:stat + h + 1, :] = top
            srow = slice(stat + heads + h, stat + heads + h + 1)
            xsend[k, srow, :] = sum(p[srow, :] * f for p, f in zip(parts, fac))
        remote(xsend.at[k], xrecv.at[k], k, 2, across_x).start()

    def project(k):
        remote(msg.at[k, 0], rpart.at[k, 1], k, 1, partner).wait_recv()
        remote(xsend.at[k], xrecv.at[k], k, 2, across_x).wait_recv()
        parts = [msg.at[k, cp], rpart.at[k, 1], xrecv.at[k]]
        outs = []
        for h in range(heads):
            _, fac = scales(parts, h)
            rows = slice(h * hd, (h + 1) * hd)
            srow = slice(stat + heads + h, stat + heads + h + 1)
            inv = 1.0 / sum(p[srow, :] * f for p, f in zip(parts, fac))
            outs.append(sum(p[rows, :] * (f * inv) for p, f in zip(parts, fac)))
        attn = jnp.concatenate(outs, axis=0).T.astype(BF16)

        @pl.when(k == 0)
        def _():
            for c in weight_copies() + resid_copies():
                c.wait()

        def part(cols):
            acc = None
            for g in range(group):
                d = mm(attn[g * tree:(g + 1) * tree], wout[g, :, cols])
                acc = d if acc is None else acc + d
            return acc.astype(BF16).astype(F32)

        psend[k] = part(other_cols)
        remote(psend.at[k], precv.at[k], k, 3, across_y).start()
        y_ref[k * CHUNK + cp, :, own_cols] = resid[k].astype(F32) + part(own_cols)

    def piece(k, owner_cp, owner_tp, lo=0, n=None):
        rows = pl.ds(lo, tree if n is None else n)
        return y_ref.at[k * CHUNK + owner_cp, rows, pl.ds(pl.multiple_of(owner_tp * wcols, wcols), wcols)]

    hf = (tree * 3 // 8) // 8 * 8
    hb = tree - hf
    pcp, xcp, dcp = chip * 2 + 1 - core, (1 - chip) * 2 + core, (1 - chip) * 2 + 1 - core

    def gather_copy(k, n):
        if n == 4:
            return remote(piece(k, cp, tp), piece(k, cp, tp), k, n, across_x)
        if n == 5:
            return remote(piece(k, cp, tp), piece(k, cp, tp), k, n, across_y)
        if n == 6:
            return remote(piece(k, cp, tp), piece(k, cp, tp), k, n, partner)
        if n == 7:
            return remote(piece(k, xcp, tp, 0, hf), piece(k, xcp, tp, 0, hf), k, n, across_y)
        if n == 8:
            return remote(piece(k, xcp, tp), piece(k, xcp, tp), k, n, partner)
        if n == 9:
            return remote(piece(k, cp, 1 - tp, hf, hb), piece(k, cp, 1 - tp, hf, hb), k, n, across_x)
        if n == 10:
            return remote(piece(k, cp, 1 - tp), piece(k, cp, 1 - tp), k, n, partner)
        if n == 11:
            return remote(piece(k, xcp, 1 - tp, 0, hf), piece(k, xcp, 1 - tp, 0, hf), k, n, partner)
        return remote(piece(k, xcp, 1 - tp, hf, hb), piece(k, xcp, 1 - tp, hf, hb), k, n, partner)

    def landed(k, n):
        src = {4: (xcp, tp, 0, tree), 5: (cp, 1 - tp, 0, tree), 6: (pcp, tp, 0, tree), 7: (xcp, 1 - tp, 0, hf), 8: (dcp, tp, 0, tree),
               9: (xcp, 1 - tp, hf, hb), 10: (pcp, 1 - tp, 0, tree), 11: (dcp, 1 - tp, 0, hf), 12: (dcp, 1 - tp, hf, hb)}[n]
        ref = piece(k, *src)
        remote(ref, ref, k, n, partner).wait_recv()

    def finish(k):
        remote(psend.at[k], precv.at[k], k, 3, across_y).wait_recv()
        total = y_ref[k * CHUNK + cp, :, own_cols] + precv[k]
        y_ref[k * CHUNK + cp, :, own_cols] = total.astype(BF16).astype(F32)
        for n in (4, 5, 6):
            gather_copy(k, n).start()

    def forward(k):
        landed(k, 4)
        gather_copy(k, 7).start()
        gather_copy(k, 8).start()
        landed(k, 5)
        gather_copy(k, 9).start()
        gather_copy(k, 10).start()

    def forward_diagonal(k):
        landed(k, 7)
        gather_copy(k, 11).start()
        landed(k, 9)
        gather_copy(k, 12).start()

    def emit(k):
        for n in (6, 8, 10, 11, 12):
            landed(k, n)
        for i in range(CHUNK):
            out_ref[k * CHUNK + i] = y_ref[k * CHUNK + i].astype(BF16)

    steps = ((merge_chip, 0, 2 + core), (queries, 1, -1), (project, 0, 7), (finish, 0, 11), (forward, 0, 15), (forward_diagonal, 0, 19), (emit, 0, 23))

    @pl.loop(0, nreq + steps[-1][2])
    def _(n):
        @pl.when(n < nreq)
        def _():
            attend(n)

        for work, lowest, after in steps:
            since = n + 1 - after

            @pl.when((since >= lowest * CHUNK) & (since < nreq) & (since % CHUNK == 0))
            def _():
                work(since // CHUNK)

    @pl.loop(0, chunks)
    def _(k):
        remote(msg.at[k, 0], rpart.at[k, 0], k, 0, partner).wait_send()
        remote(msg.at[k, 0], rpart.at[k, 1], k, 1, partner).wait_send()
        remote(xsend.at[k], xrecv.at[k], k, 2, across_x).wait_send()
        remote(psend.at[k], precv.at[k], k, 3, across_y).wait_send()
        for n in range(4, 13):
            gather_copy(k, n).wait_send()


def solution(mesh):
    cache_spec = P('dp', None, 'cp', 'tp')
    row_spec = P('dp')

    def local_step(hidden, attn_gain, w_query, w_key, w_value, w_out, cache_k, cache_v, ctx_len, positions, tree_mask):
        nreq, tree, width = hidden.shape
        num_blocks, kv_heads, blk, hd = cache_k.shape[1], cache_k.shape[3], cache_k.shape[4], cache_k.shape[5]
        qdim, kvdim = w_query.shape[1], w_key.shape[1]
        group = qdim // kvdim
        chunks = nreq // CHUNK
        keys = jnp.swapaxes(cache_k[:, :, 0], -1, -2)
        values = jnp.swapaxes(cache_v[:, :, 0], -1, -2)
        hbm = pl.BlockSpec(memory_space=pl.ANY)
        vmem = pl.BlockSpec(memory_space=pltpu.VMEM)
        smem = pl.BlockSpec(memory_space=pltpu.SMEM)
        cache_shape = jax.ShapeDtypeStruct(keys.shape, BF16)
        per, slots = CHUNK // 2, 4
        steps, early, rows = nreq // per, CHUNK // per, per * tree
        qcols = group * tree
        query, tables, new_keys, new_vals = pl.pallas_call(
            cache_kernel,
            grid=(steps,),
            in_specs=[smem, pl.BlockSpec((rows, width), lambda s: (steps - 1 - s, 0)), pl.BlockSpec((width,), lambda s: (0,)),
                      pl.BlockSpec((width, kvdim), lambda s: (0, 0)), pl.BlockSpec((width, kvdim), lambda s: (0, 0)),
                      pl.BlockSpec((nreq, tree), lambda s: (0, 0)), pl.BlockSpec((hd // 2,), lambda s: (0,)), hbm, hbm, hbm],
            out_specs=[pl.BlockSpec((per, kv_heads, hd, qcols), lambda s: (jnp.minimum(steps - 1 - s, early - 1), 0, 0, 0)),
                       pl.BlockSpec((1, 2, hd // 2, rows), lambda s: (steps - 1 - s, 0, 0, 0)), hbm, hbm],
            out_shape=[jax.ShapeDtypeStruct((CHUNK, kv_heads, hd, qcols), BF16), jax.ShapeDtypeStruct((steps, 2, hd // 2, rows), F32), cache_shape, cache_shape],
            scratch_shapes=[pltpu.VMEM((slots, 2, per, num_blocks, kv_heads, hd, blk), BF16), pltpu.VMEM((2, kvdim, rows), BF16), pltpu.VMEM((width, qdim), BF16),
                            pltpu.SemaphoreType.DMA((slots, 2)), pltpu.SemaphoreType.DMA((slots, 2)), pltpu.SemaphoreType.DMA],
            compiler_params=pltpu.CompilerParams(vmem_limit_bytes=62 * 2**20),
            name='fill_caches',
        )(ctx_len, hidden.reshape(nreq * tree, width), attn_gain, w_key, w_value, positions, jnp.asarray(rope_frequencies(hd)), w_query, keys, values)
        rows_msg = kv_heads * hd + 2 * kv_heads
        ext = hd + tree + 16
        wide_rows = (chunks, tree, width // 2)
        out_hidden = pl.pallas_call(
            attend_kernel,
            in_specs=[smem, vmem] + [hbm] * 8,
            out_specs=vmem,
            out_shape=pltpu.VMEM((nreq, tree, width), BF16),
            scratch_shapes=[
                pltpu.VMEM((nreq, tree, width), F32),
                pltpu.VMEM((2, num_blocks, kv_heads, hd, blk), BF16),
                pltpu.VMEM((2, num_blocks, kv_heads, hd + 16, blk), BF16),
                pltpu.VMEM((num_blocks - num_blocks // 2, kv_heads, ext, blk), BF16),
                pltpu.VMEM((kv_heads, ext, qcols), BF16),
                pltpu.VMEM((2, tree, tree), jnp.int32),
                pltpu.VMEM((2, num_blocks * blk, qcols), F32),
                pltpu.VMEM((chunks, CHUNK, rows_msg, qcols), F32),
                pltpu.VMEM((chunks, 2, rows_msg, qcols), F32),
                pltpu.VMEM((chunks, rows_msg, qcols), F32),
                pltpu.VMEM((chunks, rows_msg, qcols), F32),
                pltpu.VMEM(wide_rows, F32),
                pltpu.VMEM(wide_rows, F32),
                pltpu.VMEM((group, kv_heads * hd, width), BF16),
                pltpu.VMEM(wide_rows, BF16),
                pltpu.VMEM((width, qdim), BF16),
                pltpu.VMEM((CHUNK, tree, width), BF16),
                pltpu.VMEM((CHUNK // per, 2, hd // 2, rows), F32),
                pltpu.VMEM((2, CHUNK, kv_heads, hd, qcols), BF16),
                pltpu.SemaphoreType.DMA((2, 3)),
                pltpu.SemaphoreType.DMA((group, kv_heads)),
                pltpu.SemaphoreType.DMA((chunks,)),
                pltpu.SemaphoreType.DMA((4,)),
                pltpu.SemaphoreType.DMA((chunks, 13)),
                pltpu.SemaphoreType.DMA((chunks, 13)),
            ],
            compiler_params=pltpu.CompilerParams(collective_id=0, has_side_effects=True, vmem_limit_bytes=56 * 2**20),
            name='attend_and_combine',
        )(ctx_len, attn_gain, query, tables, tree_mask, new_keys, new_vals, hidden, w_query, w_out)
        return (out_hidden, jnp.swapaxes(new_keys, -1, -2)[:, :, None], jnp.swapaxes(new_vals, -1, -2)[:, :, None])

    return jax.shard_map(local_step, mesh=mesh, in_specs=(row_spec, P(), P(None, 'tp'), P(None, 'tp'), P(None, 'tp'), P('tp', None), cache_spec, cache_spec, row_spec, row_spec, row_spec), out_specs=(row_spec, cache_spec, cache_spec), check_vma=False)
```

```python
import functools
import math
import jax
import jax.numpy as jnp
import numpy as np
from jax import lax
from jax.experimental import pallas as pl
from jax.experimental.pallas import tpu as pltpu
from jax.sharding import PartitionSpec as P

ROPE_THETA = 500000.0
NORM_EPS = 1e-5
MASKED = -1e30
LOG2E = math.log2(math.e)
MESH = pl.DeviceIdType.MESH
F32 = jnp.float32
BF16 = jnp.bfloat16
CHUNK = 4
EARLY_CHUNKS = 3

SCHEDULE = (
    ('forward', 0, (16, 17, 28, 30, 35, 36)),
    ('merge', 0, (2, 6, 9, 15, 19, 21)),
    ('emit', 0, (29, 30, 34, 38, 40, 41)),
    ('project', 0, (7, 9, 15, 19, 26, 27)),
    ('query', EARLY_CHUNKS, (9, 14, 18)),
    ('finish', 0, (9, 13, 21, 25, 31, 33)),
    ('diagonal', 0, (21, 24, 32, 37, 39, 40)),
)

def mm(a, b):
    return jnp.dot(a, b, preferred_element_type=F32)


def mm_tn(a, b):
    return lax.dot_general(a, b, (((0,), (0,)), ((), ())), preferred_element_type=F32)


def rope_frequencies(head_dim):
    freq_idx = np.arange(head_dim // 2, dtype=np.float32)
    inv_freq = np.float32(1.0) / (np.float32(ROPE_THETA) ** (np.float32(2.0) * freq_idx / np.float32(head_dim)))
    wavelen = np.float32(2.0 * math.pi) / inv_freq
    smooth = (np.float32(8192.0) / wavelen - np.float32(1.0)) / np.float32(3.0)
    blended = (np.float32(1.0) - smooth) * inv_freq / np.float32(8.0) + smooth * inv_freq
    return np.where(wavelen < 2048.0, inv_freq, np.where(wavelen > 8192.0, inv_freq / np.float32(8.0), blended)).astype(np.float32)


def normed_rows(x, gain):
    wide = x.astype(F32)
    inv_rms = lax.rsqrt(jnp.mean(wide * wide, axis=-1, keepdims=True) + NORM_EPS)
    return (wide * inv_rms * gain.astype(F32)[None, :]).astype(BF16)


def rotate(rows, cos, sin):
    half = rows.shape[0] // 2
    first, second = rows[:half], rows[half:]
    return jnp.concatenate([first * cos - second * sin, second * cos + first * sin], axis=0)


def project_queries(h, wq_ref, cos, sin, out, hd, group, tree):
    reqs = h.shape[0] // tree
    for head in range(wq_ref.shape[1] // (group * hd)):
        q_t = mm(h, wq_ref[:, head * group * hd:(head + 1) * group * hd]).T
        parts = [rotate(q_t[g * hd:(g + 1) * hd], cos, sin) for g in range(group)]
        for i in range(reqs):
            out(i, head, jnp.concatenate([p[:, i * tree:(i + 1) * tree] for p in parts], axis=1).astype(BF16))


def cache_kernel(ctx_ref, x_ref, gain_ref, wk_ref, wv_ref, pos_ref, freq_ref, wq_hbm, kc_hbm, vc_hbm,
                 q_ref, tab_ref, ko_hbm, vo_hbm, buf, new_ref, wq_ref, in_sem, out_sem, w_sem):
    step, steps = pl.program_id(0), pl.num_programs(0)
    cp_rank, cp_size = lax.axis_index('cp'), lax.axis_size('cp')
    slots, _, per, num_blocks, kv_heads, hd, blk = buf.shape
    slot = lax.rem(step, slots)
    tree = pos_ref.shape[1]
    group = q_ref.shape[3] // tree
    first_req = (steps - 1 - step) * per

    def fetch(idx):
        rows, to = pl.ds((steps - 1 - idx) * per, per), lax.rem(idx, slots)
        return [pltpu.make_async_copy(src.at[rows], buf.at[to, n], in_sem.at[to, n]) for n, src in enumerate((kc_hbm, vc_hbm))]

    def flush(idx):
        rows, frm = pl.ds((steps - 1 - idx) * per, per), lax.rem(idx, slots)
        return [pltpu.make_async_copy(buf.at[frm, n], dst.at[rows], out_sem.at[frm, n]) for n, dst in enumerate((ko_hbm, vo_hbm))]

    wq_copy = pltpu.make_async_copy(wq_hbm, wq_ref, w_sem)

    @pl.when(step == 0)
    def _():
        for ahead in range(slots // 2):
            for c in fetch(ahead):
                c.start()

        wq_copy.start()

    later = step + slots // 2

    @pl.when(later < steps)
    def _():
        @pl.when(later >= slots)
        def _():
            for c in flush(later - slots):
                c.wait()

        for c in fetch(later):
            c.start()

    h = normed_rows(x_ref[...], gain_ref[...])
    half = hd // 2
    diag = lax.broadcasted_iota(jnp.int32, (half, half), 0) == lax.broadcasted_iota(jnp.int32, (half, half), 1)
    freq = jnp.sum(jnp.where(diag, freq_ref[...][None, :], 0.0), axis=1, keepdims=True)
    pos = jnp.concatenate([pos_ref[pl.ds(first_req + i, 1), :] for i in range(per)], axis=1).astype(F32)
    angle = pos * freq
    cos, sin = jnp.cos(angle), jnp.sin(angle)
    tab_ref[0, 0] = cos
    tab_ref[0, 1] = sin
    key_t = mm(h, wk_ref[...]).T
    for n in range(kv_heads):
        new_ref[0, n * hd:(n + 1) * hd, :] = rotate(key_t[n * hd:(n + 1) * hd], cos, sin).astype(BF16)
    new_ref[1] = mm(h, wv_ref[...]).T.astype(BF16)

    for c in fetch(step):
        c.wait()
    cols = per * tree
    for i in range(per):
        ctx = ctx_ref[first_req + i]
        for j in range(num_blocks // 2, num_blocks):
            first_pos = (j * cp_size + cp_rank) * blk

            @pl.when((first_pos < ctx + tree) & (first_pos + blk > ctx))
            def _():
                tok = first_pos - ctx + lax.broadcasted_iota(jnp.int32, (cols, blk), 1)
                row = lax.broadcasted_iota(jnp.int32, (cols, blk), 0) - i * tree
                pick = jnp.where((row == tok) & (row >= 0) & (row < tree), 1.0, 0.0).astype(BF16)
                tok_h = first_pos - ctx + lax.broadcasted_iota(jnp.int32, (hd, blk), 1)
                fresh = (tok_h >= 0) & (tok_h < tree)
                for n in range(2):
                    put = mm(new_ref[n], pick)
                    for head in range(kv_heads):
                        old = buf[slot, n, i, j, head].astype(F32)
                        buf[slot, n, i, j, head] = jnp.where(fresh, put[head * hd:(head + 1) * hd], old).astype(BF16)

    for c in flush(step):
        c.start()

    early = EARLY_CHUNKS * CHUNK // per

    @pl.when(step == steps - early)
    def _():
        wq_copy.wait()

    @pl.when(step >= steps - early)
    def _():
        def out(i, head, value):
            q_ref[i, head] = value

        project_queries(h, wq_ref, cos, sin, out, hd, group, tree)

    @pl.when(step == steps - 1)
    def _():
        for back in range(slots):
            for c in flush(steps - 1 - back):
                c.wait()


def attend_kernel(ctx_ref, gain_ref, q_hbm, tab_hbm, mask_hbm, kc_hbm, vc_hbm, hid_hbm, wq_hbm, wo_hbm, out_ref,
                  y_ref, kbuf, vbuf, kext, qext, mbuf, scores, msg, rpart, xsend, xrecv, psend, precv, wout, resid, wq_ref, xbuf, tbuf, qbuf,
                  kv_sem, w_sem, hid_sem, q_sem, snd, rcv):
    cp, tp = lax.axis_index('cp'), lax.axis_index('tp')
    chip, core = cp // 2, cp % 2
    partner = {'cp': chip * 2 + 1 - core}
    across_x = {'cp': (1 - chip) * 2 + core}
    across_y = {'tp': 1 - tp}
    _, _, heads, hd, qcols = q_hbm.shape
    nreq = mask_hbm.shape[0]
    tree = mask_hbm.shape[1]
    group = qcols // tree
    num_blocks, blk = kbuf.shape[1], kbuf.shape[4]
    chunks = nreq // CHUNK
    width = wo_hbm.shape[1]
    wcols = width // 2
    coef = hd ** -0.5 * LOG2E
    own_cols = pl.ds(pl.multiple_of(tp * wcols, wcols), wcols)
    other_cols = pl.ds(pl.multiple_of((1 - tp) * wcols, wcols), wcols)

    def remote(src, dst, k, n, to):
        return pltpu.make_async_remote_copy(src_ref=src, dst_ref=dst, send_sem=snd.at[k, n], recv_sem=rcv.at[k, n], device_id=to, device_id_type=MESH)

    barrier = pltpu.get_barrier_semaphore()
    for to in (partner, across_x, across_y):
        pl.semaphore_signal(barrier, inc=1, device_id=to, device_id_type=MESH)

    def request_of(n):
        return (n // CHUNK) * CHUNK + (2 * (1 - chip) + n % CHUNK) % CHUNK

    def fetch(n):
        r, to = request_of(n), n % 2
        return [pltpu.make_async_copy(kc_hbm.at[r], kbuf.at[to], kv_sem.at[to, 0]),
                pltpu.make_async_copy(vc_hbm.at[r], vbuf.at[to, :, :, pl.ds(0, hd), :], kv_sem.at[to, 1]),
                pltpu.make_async_copy(mask_hbm.at[r], mbuf.at[to], kv_sem.at[to, 2])]

    def weight_copies():
        out = []
        for g in range(group):
            for h in range(heads):
                out.append(pltpu.make_async_copy(wo_hbm.at[pl.ds((h * group + g) * hd, hd)], wout.at[g, pl.ds(h * hd, hd)], w_sem.at[g, h]))
        return out

    def resid_copies():
        return [pltpu.make_async_copy(hid_hbm.at[k * CHUNK + cp, :, own_cols], resid.at[k], hid_sem.at[k]) for k in range(chunks)]

    first_queries = pltpu.make_async_copy(q_hbm, qbuf, q_sem.at[0])
    query_weight = pltpu.make_async_copy(wq_hbm, wq_ref, q_sem.at[1])

    def chunk_copies(k):
        pairs = tbuf.shape[0]
        return [pltpu.make_async_copy(hid_hbm.at[pl.ds(k * CHUNK, CHUNK)], xbuf, q_sem.at[2]),
                pltpu.make_async_copy(tab_hbm.at[pl.ds(k * pairs, pairs)], tbuf, q_sem.at[3])]

    for c in fetch(0) + [first_queries] + chunk_copies(EARLY_CHUNKS) + [query_weight] + weight_copies() + resid_copies():
        c.start()
    ones = jnp.ones((vbuf.shape[3] - hd, blk), BF16)
    for s in range(2):
        for j in range(num_blocks):
            for h in range(heads):
                vbuf[s, j, h, hd:, :] = ones
    pad = qext.shape[1] - hd - tree
    hide = jnp.where(lax.broadcasted_iota(jnp.int32, (pad, qcols), 0) == 0, MASKED, 0.0).astype(BF16)
    for h in range(heads):
        qext[h, hd + tree:, :] = hide
    pl.semaphore_wait(barrier, 3)
    first_queries.wait()

    def queries(k):
        for c in chunk_copies(k):
            c.wait()

        @pl.when(k == EARLY_CHUNKS)
        def _():
            query_weight.wait()

        h = normed_rows(xbuf[...].reshape(CHUNK * tree, width), gain_ref[...])
        cos = jnp.concatenate([tbuf[p, 0] for p in range(tbuf.shape[0])], axis=1)
        sin = jnp.concatenate([tbuf[p, 1] for p in range(tbuf.shape[0])], axis=1)

        def out(i, head, value):
            qbuf[k % EARLY_CHUNKS, i, head] = value

        project_queries(h, wq_ref, cos, sin, out, hd, group, tree)

        @pl.when(k + 1 < chunks)
        def _():
            for c in chunk_copies(k + 1):
                c.start()

    def attend(n):
        k, r, slot = n // CHUNK, request_of(n), n % 2
        i = r - k * CHUNK

        @pl.when(n + 1 < nreq)
        def _():
            for c in fetch(n + 1):
                c.start()

        ctx = ctx_ref[r]
        for c in fetch(n):
            c.wait()
        seen = jnp.concatenate([mbuf[slot].astype(F32)] * group, axis=0).T
        bias = jnp.where(seen > 0.0, 0.0, MASKED).astype(BF16)
        for h in range(heads):
            qext[h, :hd, :] = qbuf[k % EARLY_CHUNKS, i, h]
            qext[h, hd:hd + tree, :] = bias
        late = num_blocks // 2
        for j in range(late, num_blocks):
            off = (j * 4 + cp) * blk - ctx
            tok = off + lax.broadcasted_iota(jnp.int32, (tree, blk), 1)
            pick = jnp.where(tok == lax.broadcasted_iota(jnp.int32, (tree, blk), 0), 1.0, 0.0).astype(BF16)
            tok_p = off + lax.broadcasted_iota(jnp.int32, (pad, blk), 1)
            tail = jnp.where((tok_p >= tree) & (lax.broadcasted_iota(jnp.int32, (pad, blk), 0) == 0), 1.0, 0.0).astype(BF16)
            tok_h = off + lax.broadcasted_iota(jnp.int32, (hd, blk), 1)
            for h in range(heads):
                kext[j - late, h, :hd, :] = jnp.where(tok_h < tree, kbuf[slot, j, h].astype(F32), 0.0).astype(BF16)
                kext[j - late, h, hd:hd + tree, :] = pick
                kext[j - late, h, hd + tree:, :] = tail

        def score(h, j):
            if j < late:
                s = mm_tn(kbuf[slot, j, h], qext[h, :hd, :])
            else:
                s = mm_tn(kext[j - late, h], qext[h])
            scores[h % 2, j * blk:(j + 1) * blk, :] = s
            return jnp.max(s.reshape(blk // 8, 8, qcols), axis=0)

        tops = [None] * heads
        tops[0] = functools.reduce(jnp.maximum, [score(0, j) for j in range(num_blocks)])
        for h in range(heads):
            top = jnp.max(tops[h], axis=0, keepdims=True)
            shift = top * coef
            total, nxt = None, []
            for j in range(num_blocks):
                if h + 1 < heads:
                    nxt.append(score(h + 1, j))
                p = jnp.exp2(scores[h % 2, j * blk:(j + 1) * blk, :] * coef - shift).astype(BF16)
                o = mm(vbuf[slot, j, h], p)
                total = o if total is None else total + o
            if h + 1 < heads:
                tops[h + 1] = functools.reduce(jnp.maximum, nxt)
            msg[k, i, h * hd:(h + 1) * hd, :] = total[:hd]
            msg[k, i, heads * hd + h:heads * hd + h + 1, :] = top
            msg[k, i, heads * hd + heads + h:heads * hd + heads + h + 1, :] = total[hd:hd + 1]

        which = (n % CHUNK) // 2

        @pl.when(i % 2 != core)
        def _():
            remote(msg.at[k, i], rpart.at[k, which], k, which, partner).start()

    stat = heads * hd

    def scales(parts, h):
        tops = [p[stat + h:stat + h + 1, :] for p in parts]
        top = functools.reduce(jnp.maximum, tops)
        return top, [jnp.exp2((t - top) * coef) for t in tops]

    def merge_chip(k):
        remote(msg.at[k, 0], rpart.at[k, 0], k, 0, partner).wait_recv()
        parts = [msg.at[k, 2 * (1 - chip) + core], rpart.at[k, 0]]
        for h in range(heads):
            top, fac = scales(parts, h)
            rows = slice(h * hd, (h + 1) * hd)
            xsend[k, rows, :] = sum(p[rows, :] * f for p, f in zip(parts, fac))
            xsend[k, stat + h:stat + h + 1, :] = top
            srow = slice(stat + heads + h, stat + heads + h + 1)
            xsend[k, srow, :] = sum(p[srow, :] * f for p, f in zip(parts, fac))
        remote(xsend.at[k], xrecv.at[k], k, 2, across_x).start()

    def project(k):
        remote(msg.at[k, 0], rpart.at[k, 1], k, 1, partner).wait_recv()
        remote(xsend.at[k], xrecv.at[k], k, 2, across_x).wait_recv()
        parts = [msg.at[k, cp], rpart.at[k, 1], xrecv.at[k]]
        outs = []
        for h in range(heads):
            _, fac = scales(parts, h)
            rows = slice(h * hd, (h + 1) * hd)
            srow = slice(stat + heads + h, stat + heads + h + 1)
            inv = 1.0 / sum(p[srow, :] * f for p, f in zip(parts, fac))
            outs.append(sum(p[rows, :] * (f * inv) for p, f in zip(parts, fac)))
        attn = jnp.concatenate(outs, axis=0).T.astype(BF16)

        @pl.when(k == 0)
        def _():
            for c in weight_copies() + resid_copies():
                c.wait()

        def part(cols):
            acc = None
            for g in range(group):
                d = mm(attn[g * tree:(g + 1) * tree], wout[g, :, cols])
                acc = d if acc is None else acc + d
            return acc.astype(BF16).astype(F32)

        psend[k] = part(other_cols)
        remote(psend.at[k], precv.at[k], k, 3, across_y).start()
        y_ref[k * CHUNK + cp, tp] = resid[k].astype(F32) + part(own_cols)

    def piece(k, owner_cp, owner_tp, lo=0, n=None):
        rows = pl.ds(lo, tree if n is None else n)
        return y_ref.at[k * CHUNK + owner_cp, owner_tp, rows]

    hf = (tree * 3 // 8) // 8 * 8
    hb = tree - hf
    pcp, xcp, dcp = chip * 2 + 1 - core, (1 - chip) * 2 + core, (1 - chip) * 2 + 1 - core

    def gather_copy(k, n):
        if n == 4:
            return remote(piece(k, cp, tp), piece(k, cp, tp), k, n, across_x)
        if n == 5:
            return remote(piece(k, cp, tp), piece(k, cp, tp), k, n, across_y)
        if n == 6:
            return remote(piece(k, cp, tp), piece(k, cp, tp), k, n, partner)
        if n == 7:
            return remote(piece(k, xcp, tp, 0, hf), piece(k, xcp, tp, 0, hf), k, n, across_y)
        if n == 8:
            return remote(piece(k, xcp, tp), piece(k, xcp, tp), k, n, partner)
        if n == 9:
            return remote(piece(k, cp, 1 - tp, hf, hb), piece(k, cp, 1 - tp, hf, hb), k, n, across_x)
        if n == 10:
            return remote(piece(k, cp, 1 - tp), piece(k, cp, 1 - tp), k, n, partner)
        if n == 11:
            return remote(piece(k, xcp, 1 - tp, 0, hf), piece(k, xcp, 1 - tp, 0, hf), k, n, partner)
        return remote(piece(k, xcp, 1 - tp, hf, hb), piece(k, xcp, 1 - tp, hf, hb), k, n, partner)

    def landed(k, n):
        src = {4: (xcp, tp, 0, tree), 5: (cp, 1 - tp, 0, tree), 6: (pcp, tp, 0, tree), 7: (xcp, 1 - tp, 0, hf), 8: (dcp, tp, 0, tree),
               9: (xcp, 1 - tp, hf, hb), 10: (pcp, 1 - tp, 0, tree), 11: (dcp, 1 - tp, 0, hf), 12: (dcp, 1 - tp, hf, hb)}[n]
        ref = piece(k, *src)
        remote(ref, ref, k, n, partner).wait_recv()

    def finish(k):
        remote(psend.at[k], precv.at[k], k, 3, across_y).wait_recv()
        total = y_ref[k * CHUNK + cp, tp] + precv[k]
        y_ref[k * CHUNK + cp, tp] = total.astype(BF16).astype(F32)
        for n in (4, 5, 6):
            gather_copy(k, n).start()

    def forward(k):
        landed(k, 4)
        gather_copy(k, 7).start()
        gather_copy(k, 8).start()
        landed(k, 5)
        gather_copy(k, 9).start()
        gather_copy(k, 10).start()

    def forward_diagonal(k):
        landed(k, 7)
        gather_copy(k, 11).start()
        landed(k, 9)
        gather_copy(k, 12).start()

    def emit(k):
        for n in (6, 8, 10, 11, 12):
            landed(k, n)
        for i in range(CHUNK):
            for side in range(2):
                out_ref[k * CHUNK + i, :, side * wcols:(side + 1) * wcols] = y_ref[k * CHUNK + i, side].astype(BF16)

    work = {'merge': merge_chip, 'query': queries, 'project': project, 'finish': finish, 'forward': forward, 'diagonal': forward_diagonal, 'emit': emit}

    @pl.loop(0, 1 + max(max(turns) for _, _, turns in SCHEDULE))
    def _(n):
        @pl.when(n < nreq)
        def _():
            attend(n)

        for name, lowest, turns in SCHEDULE:
            @pl.when(functools.reduce(jnp.logical_or, [n == t for t in turns]))
            def _():
                work[name](sum([jnp.where(n > t, 1, 0) for t in turns]) + lowest)

    @pl.loop(0, chunks)
    def _(k):
        remote(msg.at[k, 0], rpart.at[k, 0], k, 0, partner).wait_send()
        remote(msg.at[k, 0], rpart.at[k, 1], k, 1, partner).wait_send()
        remote(xsend.at[k], xrecv.at[k], k, 2, across_x).wait_send()
        remote(psend.at[k], precv.at[k], k, 3, across_y).wait_send()
        for n in range(4, 13):
            gather_copy(k, n).wait_send()


def solution(mesh):
    cache_spec = P('dp', None, 'cp', 'tp')
    row_spec = P('dp')

    def local_step(hidden, attn_gain, w_query, w_key, w_value, w_out, cache_k, cache_v, ctx_len, positions, tree_mask):
        nreq, tree, width = hidden.shape
        num_blocks, kv_heads, blk, hd = cache_k.shape[1], cache_k.shape[3], cache_k.shape[4], cache_k.shape[5]
        qdim, kvdim = w_query.shape[1], w_key.shape[1]
        group = qdim // kvdim
        chunks = nreq // CHUNK
        keys = jnp.swapaxes(cache_k[:, :, 0], -1, -2)
        values = jnp.swapaxes(cache_v[:, :, 0], -1, -2)
        hbm = pl.BlockSpec(memory_space=pl.ANY)
        vmem = pl.BlockSpec(memory_space=pltpu.VMEM)
        smem = pl.BlockSpec(memory_space=pltpu.SMEM)
        cache_shape = jax.ShapeDtypeStruct(keys.shape, BF16)
        per, slots = CHUNK // 2, 8
        steps, early, rows = nreq // per, EARLY_CHUNKS * CHUNK // per, per * tree
        qcols = group * tree
        query, tables, new_keys, new_vals = pl.pallas_call(
            cache_kernel,
            grid=(steps,),
            in_specs=[smem, pl.BlockSpec((rows, width), lambda s: (steps - 1 - s, 0)), pl.BlockSpec((width,), lambda s: (0,)),
                      pl.BlockSpec((width, kvdim), lambda s: (0, 0)), pl.BlockSpec((width, kvdim), lambda s: (0, 0)),
                      pl.BlockSpec((nreq, tree), lambda s: (0, 0)), pl.BlockSpec((hd // 2,), lambda s: (0,)), hbm, hbm, hbm],
            out_specs=[pl.BlockSpec((pl.squeezed, per, kv_heads, hd, qcols), lambda s: (jnp.minimum(steps - 1 - s, early - 1) // (CHUNK // per), jnp.minimum(steps - 1 - s, early - 1) % (CHUNK // per), 0, 0, 0)),
                       pl.BlockSpec((1, 2, hd // 2, rows), lambda s: (steps - 1 - s, 0, 0, 0)), hbm, hbm],
            out_shape=[jax.ShapeDtypeStruct((EARLY_CHUNKS, CHUNK, kv_heads, hd, qcols), BF16), jax.ShapeDtypeStruct((steps, 2, hd // 2, rows), F32), cache_shape, cache_shape],
            scratch_shapes=[pltpu.VMEM((slots, 2, per, num_blocks, kv_heads, hd, blk), BF16), pltpu.VMEM((2, kvdim, rows), BF16), pltpu.VMEM((width, qdim), BF16),
                            pltpu.SemaphoreType.DMA((slots, 2)), pltpu.SemaphoreType.DMA((slots, 2)), pltpu.SemaphoreType.DMA],
            compiler_params=pltpu.CompilerParams(vmem_limit_bytes=62 * 2**20),
            name='fill_caches',
        )(ctx_len, hidden.reshape(nreq * tree, width), attn_gain, w_key, w_value, positions, jnp.asarray(rope_frequencies(hd)), w_query, keys, values)
        rows_msg = kv_heads * hd + 2 * kv_heads
        ext = hd + tree + 16
        wide_rows = (chunks, tree, width // 2)
        out_hidden = pl.pallas_call(
            attend_kernel,
            in_specs=[smem, vmem] + [hbm] * 8,
            out_specs=vmem,
            out_shape=pltpu.VMEM((nreq, tree, width), BF16),
            scratch_shapes=[
                pltpu.VMEM((nreq, 2, tree, width // 2), F32),
                pltpu.VMEM((2, num_blocks, kv_heads, hd, blk), BF16),
                pltpu.VMEM((2, num_blocks, kv_heads, hd + 16, blk), BF16),
                pltpu.VMEM((num_blocks - num_blocks // 2, kv_heads, ext, blk), BF16),
                pltpu.VMEM((kv_heads, ext, qcols), BF16),
                pltpu.VMEM((2, tree, tree), jnp.int32),
                pltpu.VMEM((2, num_blocks * blk, qcols), F32),
                pltpu.VMEM((chunks, CHUNK, rows_msg, qcols), F32),
                pltpu.VMEM((chunks, 2, rows_msg, qcols), F32),
                pltpu.VMEM((chunks, rows_msg, qcols), F32),
                pltpu.VMEM((chunks, rows_msg, qcols), F32),
                pltpu.VMEM(wide_rows, F32),
                pltpu.VMEM(wide_rows, F32),
                pltpu.VMEM((group, kv_heads * hd, width), BF16),
                pltpu.VMEM(wide_rows, BF16),
                pltpu.VMEM((width, qdim), BF16),
                pltpu.VMEM((CHUNK, tree, width), BF16),
                pltpu.VMEM((CHUNK // per, 2, hd // 2, rows), F32),
                pltpu.VMEM((EARLY_CHUNKS, CHUNK, kv_heads, hd, qcols), BF16),
                pltpu.SemaphoreType.DMA((2, 3)),
                pltpu.SemaphoreType.DMA((group, kv_heads)),
                pltpu.SemaphoreType.DMA((chunks,)),
                pltpu.SemaphoreType.DMA((4,)),
                pltpu.SemaphoreType.DMA((chunks, 13)),
                pltpu.SemaphoreType.DMA((chunks, 13)),
            ],
            compiler_params=pltpu.CompilerParams(collective_id=0, has_side_effects=True, vmem_limit_bytes=56 * 2**20),
            name='attend_and_combine',
        )(ctx_len, attn_gain, query, tables, tree_mask, new_keys, new_vals, hidden, w_query, w_out)
        return (out_hidden, jnp.swapaxes(new_keys, -1, -2)[:, :, None], jnp.swapaxes(new_vals, -1, -2)[:, :, None])

    return jax.shard_map(local_step, mesh=mesh, in_specs=(row_spec, P(), P(None, 'tp'), P(None, 'tp'), P(None, 'tp'), P('tp', None), cache_spec, cache_spec, row_spec, row_spec, row_spec), out_specs=(row_spec, cache_spec, cache_spec), check_vma=False)
```

```python
import functools
import math
import jax
import jax.numpy as jnp
import numpy as np
from jax import lax
from jax.experimental import pallas as pl
from jax.experimental.pallas import tpu as pltpu
from jax.sharding import PartitionSpec as P

ROPE_THETA = 500000.0
NORM_EPS = 1e-5
MASKED = -1e30
LOG2E = math.log2(math.e)
MESH = pl.DeviceIdType.MESH
F32 = jnp.float32
BF16 = jnp.bfloat16
CHUNK = 4
EARLY_CHUNKS = 3
HEAD_STEPS = 3

SCHEDULE = (
    ('emit', 0, (29, 31, 35, 36, 37, 38)),
    ('diagonal', 0, (22, 29, 30, 33, 34, 35)),
    ('forward', 0, (15, 17, 26, 30, 31, 32)),
    ('project', 0, (9, 10, 17, 19, 24, 25)),
    ('query', EARLY_CHUNKS, (9, 14, 16)),
    ('merge', 0, (4, 7, 9, 15, 19, 21)),
    ('finish', 0, (10, 13, 21, 24, 27, 28)),
)

def mm(a, b):
    return jnp.dot(a, b, preferred_element_type=F32)


def mm_tn(a, b):
    return lax.dot_general(a, b, (((0,), (0,)), ((), ())), preferred_element_type=F32)


def rope_frequencies(head_dim):
    freq_idx = np.arange(head_dim // 2, dtype=np.float32)
    inv_freq = np.float32(1.0) / (np.float32(ROPE_THETA) ** (np.float32(2.0) * freq_idx / np.float32(head_dim)))
    wavelen = np.float32(2.0 * math.pi) / inv_freq
    smooth = (np.float32(8192.0) / wavelen - np.float32(1.0)) / np.float32(3.0)
    blended = (np.float32(1.0) - smooth) * inv_freq / np.float32(8.0) + smooth * inv_freq
    return np.where(wavelen < 2048.0, inv_freq, np.where(wavelen > 8192.0, inv_freq / np.float32(8.0), blended)).astype(np.float32)


def cos_sin(angle):
    turns = jnp.floor(angle * (2.0 / math.pi) + 0.5)
    r = ((angle - turns * 1.5703125) - turns * 4.837512969970703125e-4) - turns * 7.549789954891882e-8
    z = r * r
    sin_r = r + r * z * (-1.6666654611e-1 + z * (8.3321608736e-3 + z * -1.9515295891e-4))
    cos_r = 1.0 - 0.5 * z + z * z * (4.166664568298827e-2 + z * (-1.388731625493765e-3 + z * 2.443315711809948e-5))
    quarter = turns.astype(jnp.int32) & 3
    odd = (quarter & 1) == 1
    cos, sin = jnp.where(odd, sin_r, cos_r), jnp.where(odd, cos_r, sin_r)
    return jnp.where((quarter == 1) | (quarter == 2), -cos, cos), jnp.where(quarter >= 2, -sin, sin)


def normed_rows(x, gain):
    wide = x.astype(F32)
    inv_rms = lax.rsqrt(jnp.mean(wide * wide, axis=-1, keepdims=True) + NORM_EPS)
    return (wide * inv_rms * gain.astype(F32)[None, :]).astype(BF16)


def rotate(rows, cos, sin):
    half = rows.shape[0] // 2
    first, second = rows[:half], rows[half:]
    return jnp.concatenate([first * cos - second * sin, second * cos + first * sin], axis=0)


def project_queries(h, wq_ref, cos, sin, out, hd, group, tree):
    reqs = h.shape[0] // tree
    for head in range(wq_ref.shape[1] // (group * hd)):
        q_t = mm(h, wq_ref[:, head * group * hd:(head + 1) * group * hd]).T
        parts = [rotate(q_t[g * hd:(g + 1) * hd], cos, sin) for g in range(group)]
        for i in range(reqs):
            out(i, head, jnp.concatenate([p[:, i * tree:(i + 1) * tree] for p in parts], axis=1).astype(BF16))


def prepare(vref, qext, hd, tree):
    num_blocks, heads, vrows, blk = vref.shape
    ones = jnp.ones((vrows - hd, blk), BF16)
    pad = qext.shape[1] - hd - tree
    hide = jnp.where(lax.broadcasted_iota(jnp.int32, (pad, qext.shape[2]), 0) == 0, MASKED, 0.0).astype(BF16)
    for h in range(heads):
        for j in range(num_blocks):
            vref[j, h, hd:, :] = ones
        qext[h, hd + tree:, :] = hide


def attention(ctx, tree_mask, qref, kref, vref, kext, qext, scores, out, cp):
    num_blocks, heads, hd, blk = kref.shape
    qcols, tree = qext.shape[2], tree_mask.shape[0]
    pad = qext.shape[1] - hd - tree
    late = num_blocks // 2
    coef = hd ** -0.5 * LOG2E
    seen = jnp.concatenate([tree_mask.astype(F32)] * (qcols // tree), axis=0).T
    bias = jnp.where(seen > 0.0, 0.0, MASKED).astype(BF16)
    for h in range(heads):
        qext[h, :hd, :] = qref[h]
        qext[h, hd:hd + tree, :] = bias
    for j in range(late, num_blocks):
        off = (j * 4 + cp) * blk - ctx
        tok = off + lax.broadcasted_iota(jnp.int32, (tree, blk), 1)
        pick = jnp.where(tok == lax.broadcasted_iota(jnp.int32, (tree, blk), 0), 1.0, 0.0).astype(BF16)
        tok_p = off + lax.broadcasted_iota(jnp.int32, (pad, blk), 1)
        tail = jnp.where((tok_p >= tree) & (lax.broadcasted_iota(jnp.int32, (pad, blk), 0) == 0), 1.0, 0.0).astype(BF16)
        tok_h = off + lax.broadcasted_iota(jnp.int32, (hd, blk), 1)
        for h in range(heads):
            kext[j - late, h, :hd, :] = jnp.where(tok_h < tree, kref[j, h].astype(F32), 0.0).astype(BF16)
            kext[j - late, h, hd:hd + tree, :] = pick
            kext[j - late, h, hd + tree:, :] = tail

    def score(h, j):
        if j < late:
            s = mm_tn(kref[j, h], qext[h, :hd, :])
        else:
            s = mm_tn(kext[j - late, h], qext[h])
        scores[h % 2, j * blk:(j + 1) * blk, :] = s
        return jnp.max(s.reshape(blk // 8, 8, qcols), axis=0)

    tops = [None] * heads
    tops[0] = functools.reduce(jnp.maximum, [score(0, j) for j in range(num_blocks)])
    for h in range(heads):
        top = jnp.max(tops[h], axis=0, keepdims=True)
        shift = top * coef
        total, nxt = None, []
        for j in range(num_blocks):
            if h + 1 < heads:
                nxt.append(score(h + 1, j))
            p = jnp.exp2(scores[h % 2, j * blk:(j + 1) * blk, :] * coef - shift).astype(BF16)
            o = mm(vref[j, h], p)
            total = o if total is None else total + o
        if h + 1 < heads:
            tops[h + 1] = functools.reduce(jnp.maximum, nxt)
        out[h * hd:(h + 1) * hd, :] = total[:hd]
        out[heads * hd + h:heads * hd + h + 1, :] = top
        out[heads * hd + heads + h:heads * hd + heads + h + 1, :] = total[hd:hd + 1]


def cache_kernel(ctx_ref, gain_ref, pos_ref, freq_ref, mask_ref, wk_hbm, wv_hbm, wq_hbm, x_hbm, kc_hbm, vc_hbm,
                 q_ref, tab_ref, msg_hbm, ko_hbm, vo_hbm,
                 buf, xbuf, new_ref, wk_ref, wv_ref, wq_ref, vbuf, kext, qext, scores, msg, in_sem, out_sem, w_sem, msg_sem):
    cp_rank, cp_size = lax.axis_index('cp'), lax.axis_size('cp')
    slots, _, per, num_blocks, kv_heads, hd, blk = buf.shape
    nreq, tree = pos_ref.shape
    steps = nreq // per
    group = q_ref.shape[4] // tree
    width = x_hbm.shape[2]
    half = hd // 2
    cols = per * tree

    def pair_of(idx):
        return (idx + steps - HEAD_STEPS) % steps

    def fetch(idx):
        rows, to = pl.ds(pair_of(idx) * per, per), idx % slots
        return [pltpu.make_async_copy(x_hbm.at[rows], xbuf.at[to], in_sem.at[to, 2])] + [
            pltpu.make_async_copy(src.at[rows], buf.at[to, n], in_sem.at[to, n]) for n, src in enumerate((kc_hbm, vc_hbm))]

    def flush(idx):
        rows, frm = pl.ds(pair_of(idx) * per, per), idx % slots
        return [pltpu.make_async_copy(buf.at[frm, n], dst.at[rows], out_sem.at[frm, n]) for n, dst in enumerate((ko_hbm, vo_hbm))]

    kv_weights = [pltpu.make_async_copy(src, dst, w_sem.at[n]) for n, (src, dst) in enumerate(((wk_hbm, wk_ref), (wv_hbm, wv_ref)))]
    q_weight = pltpu.make_async_copy(wq_hbm, wq_ref, w_sem.at[2])
    ahead = slots // 2
    for c in fetch(0) + kv_weights:
        c.start()
    for idx in range(1, ahead):
        for c in fetch(idx):
            c.start()
    q_weight.start()
    prepare(vbuf, qext, hd, tree)
    diag = lax.broadcasted_iota(jnp.int32, (half, half), 0) == lax.broadcasted_iota(jnp.int32, (half, half), 1)
    freq = jnp.sum(jnp.where(diag, freq_ref[...][None, :], 0.0), axis=1, keepdims=True)
    for c in kv_weights:
        c.wait()

    @pl.loop(0, steps)
    def _(step):
        slot, pair = step % slots, pair_of(step)
        later = step + ahead

        @pl.when(later < steps)
        def _():
            @pl.when(later >= slots)
            def _():
                for c in flush(later - slots):
                    c.wait()

            for c in fetch(later):
                c.start()

        for c in fetch(step):
            c.wait()
        h = normed_rows(xbuf[slot].reshape(cols, width), gain_ref[...])
        pos = jnp.concatenate([pos_ref[pl.ds(pair * per + i, 1), :] for i in range(per)], axis=1).astype(F32)
        cos, sin = cos_sin(pos * freq)
        tab_ref[pair, 0] = cos
        tab_ref[pair, 1] = sin
        key_t = mm(h, wk_ref[...]).T
        for n in range(kv_heads):
            new_ref[0, n * hd:(n + 1) * hd, :] = rotate(key_t[n * hd:(n + 1) * hd], cos, sin).astype(BF16)
        new_ref[1] = mm(h, wv_ref[...]).T.astype(BF16)
        for i in range(per):
            ctx = ctx_ref[pair * per + i]
            for j in range(num_blocks // 2, num_blocks):
                first_pos = (j * cp_size + cp_rank) * blk

                @pl.when((first_pos < ctx + tree) & (first_pos + blk > ctx))
                def _():
                    tok = first_pos - ctx + lax.broadcasted_iota(jnp.int32, (cols, blk), 1)
                    row = lax.broadcasted_iota(jnp.int32, (cols, blk), 0) - i * tree
                    pick = jnp.where((row == tok) & (row >= 0) & (row < tree), 1.0, 0.0).astype(BF16)
                    tok_h = first_pos - ctx + lax.broadcasted_iota(jnp.int32, (hd, blk), 1)
                    fresh = (tok_h >= 0) & (tok_h < tree)
                    for n in range(2):
                        put = mm(new_ref[n], pick)
                        for head in range(kv_heads):
                            old = buf[slot, n, i, j, head].astype(F32)
                            buf[slot, n, i, j, head] = jnp.where(fresh, put[head * hd:(head + 1) * hd], old).astype(BF16)

        for c in flush(step):
            c.start()

        @pl.when(step == HEAD_STEPS)
        def _():
            q_weight.wait()

        @pl.when(pair < EARLY_CHUNKS * CHUNK // per)
        def _():
            req = pair * per

            def out(i, head, value):
                q_ref[req // CHUNK, req % CHUNK + i, head] = value

            project_queries(h, wq_ref, cos, sin, out, hd, group, tree)

        @pl.when(pair < CHUNK // per)
        def _():
            @pl.loop(0, per)
            def _(i):
                req = pair * per + i
                for j in range(num_blocks):
                    for head in range(kv_heads):
                        vbuf[j, head, :hd, :] = buf[slot, 1, i, j, head]
                attention(ctx_ref[req], mask_ref[req], q_ref.at[0, req], buf.at[slot, 0, i], vbuf, kext, qext, scores, msg.at[req], cp_rank)
                pltpu.make_async_copy(msg.at[req], msg_hbm.at[req], msg_sem.at[req]).start()

    for idx in range(steps - slots, steps):
        for c in flush(idx):
            c.wait()
    for req in range(CHUNK):
        pltpu.make_async_copy(msg.at[req], msg_hbm.at[req], msg_sem.at[req]).wait()


def attend_kernel(ctx_ref, gain_ref, q_hbm, tab_hbm, msg_hbm, mask_hbm, kc_hbm, vc_hbm, hid_hbm, wq_hbm, wo_hbm, out_ref,
                  y_ref, kbuf, vbuf, kext, qext, mbuf, scores, msg, rpart, xsend, xrecv, psend, precv, wout, resid, wq_ref, xbuf, tbuf, qbuf,
                  kv_sem, w_sem, hid_sem, q_sem, snd, rcv):
    cp, tp = lax.axis_index('cp'), lax.axis_index('tp')
    chip, core = cp // 2, cp % 2
    partner = {'cp': chip * 2 + 1 - core}
    across_x = {'cp': (1 - chip) * 2 + core}
    across_y = {'tp': 1 - tp}
    _, _, heads, hd, qcols = q_hbm.shape
    nreq = mask_hbm.shape[0]
    tree = mask_hbm.shape[1]
    group = qcols // tree
    num_blocks, blk = kbuf.shape[1], kbuf.shape[4]
    chunks = nreq // CHUNK
    width = wo_hbm.shape[1]
    wcols = width // 2
    coef = hd ** -0.5 * LOG2E
    own_cols = pl.ds(pl.multiple_of(tp * wcols, wcols), wcols)
    other_cols = pl.ds(pl.multiple_of((1 - tp) * wcols, wcols), wcols)

    def remote(src, dst, k, n, to):
        return pltpu.make_async_remote_copy(src_ref=src, dst_ref=dst, send_sem=snd.at[k, n], recv_sem=rcv.at[k, n], device_id=to, device_id_type=MESH)

    barrier = pltpu.get_barrier_semaphore()
    for to in (partner, across_x, across_y):
        pl.semaphore_signal(barrier, inc=1, device_id=to, device_id_type=MESH)

    def request_of(n):
        return (n // CHUNK) * CHUNK + (2 * (1 - chip) + n % CHUNK) % CHUNK

    def fetch(n):
        r, to = request_of(n), n % 2
        return [pltpu.make_async_copy(kc_hbm.at[r], kbuf.at[to], kv_sem.at[to, 0]),
                pltpu.make_async_copy(vc_hbm.at[r], vbuf.at[to, :, :, pl.ds(0, hd), :], kv_sem.at[to, 1]),
                pltpu.make_async_copy(mask_hbm.at[r], mbuf.at[to], kv_sem.at[to, 2])]

    def weight_copies():
        out = []
        for g in range(group):
            for h in range(heads):
                out.append(pltpu.make_async_copy(wo_hbm.at[pl.ds((h * group + g) * hd, hd)], wout.at[g, pl.ds(h * hd, hd)], w_sem.at[g, h]))
        return out

    def resid_copies():
        return [pltpu.make_async_copy(hid_hbm.at[k * CHUNK + cp, :, own_cols], resid.at[k], hid_sem.at[k]) for k in range(chunks)]

    first_queries = pltpu.make_async_copy(q_hbm, qbuf, q_sem.at[0])
    query_weight = pltpu.make_async_copy(wq_hbm, wq_ref, q_sem.at[1])

    def chunk_copies(k):
        pairs = tbuf.shape[0]
        return [pltpu.make_async_copy(hid_hbm.at[pl.ds(k * CHUNK, CHUNK)], xbuf, q_sem.at[2]),
                pltpu.make_async_copy(tab_hbm.at[pl.ds(k * pairs, pairs)], tbuf, q_sem.at[3])]

    first_msgs = pltpu.make_async_copy(msg_hbm, msg.at[0], q_sem.at[4])
    for c in [first_msgs] + fetch(CHUNK) + [first_queries]:
        c.start()
    for to in range(2):
        prepare(vbuf.at[to], qext, hd, tree)
    pl.semaphore_wait(barrier, 3)
    first_msgs.wait()

    def share(k, i, which):
        @pl.when(i % 2 != core)
        def _():
            remote(msg.at[k, i], rpart.at[k, which], k, which, partner).start()

    for n in range(CHUNK):
        share(0, (2 * (1 - chip) + n) % CHUNK, n // 2)
    for c in weight_copies() + resid_copies() + chunk_copies(EARLY_CHUNKS) + [query_weight]:
        c.start()
    first_queries.wait()

    def queries(k):
        for c in chunk_copies(k):
            c.wait()

        @pl.when(k == EARLY_CHUNKS)
        def _():
            query_weight.wait()

        h = normed_rows(xbuf[...].reshape(CHUNK * tree, width), gain_ref[...])
        cos = jnp.concatenate([tbuf[p, 0] for p in range(tbuf.shape[0])], axis=1)
        sin = jnp.concatenate([tbuf[p, 1] for p in range(tbuf.shape[0])], axis=1)

        def out(i, head, value):
            qbuf[k % EARLY_CHUNKS, i, head] = value

        project_queries(h, wq_ref, cos, sin, out, hd, group, tree)

        @pl.when(k + 1 < chunks)
        def _():
            for c in chunk_copies(k + 1):
                c.start()

    def attend(n):
        k, r, slot = n // CHUNK, request_of(n), n % 2
        i = r - k * CHUNK

        @pl.when(n + 1 < nreq)
        def _():
            for c in fetch(n + 1):
                c.start()

        ctx = ctx_ref[r]
        for c in fetch(n):
            c.wait()
        attention(ctx, mbuf[slot], qbuf.at[k % EARLY_CHUNKS, i], kbuf.at[slot], vbuf.at[slot], kext, qext, scores, msg.at[k, i], cp)

        share(k, i, (n % CHUNK) // 2)

    stat = heads * hd

    def scales(parts, h):
        tops = [p[stat + h:stat + h + 1, :] for p in parts]
        top = functools.reduce(jnp.maximum, tops)
        return top, [jnp.exp2((t - top) * coef) for t in tops]

    def merge_chip(k):
        remote(msg.at[k, 0], rpart.at[k, 0], k, 0, partner).wait_recv()
        parts = [msg.at[k, 2 * (1 - chip) + core], rpart.at[k, 0]]
        for h in range(heads):
            top, fac = scales(parts, h)
            rows = slice(h * hd, (h + 1) * hd)
            xsend[k, rows, :] = sum(p[rows, :] * f for p, f in zip(parts, fac))
            xsend[k, stat + h:stat + h + 1, :] = top
            srow = slice(stat + heads + h, stat + heads + h + 1)
            xsend[k, srow, :] = sum(p[srow, :] * f for p, f in zip(parts, fac))
        remote(xsend.at[k], xrecv.at[k], k, 2, across_x).start()

    def project(k):
        remote(msg.at[k, 0], rpart.at[k, 1], k, 1, partner).wait_recv()
        remote(xsend.at[k], xrecv.at[k], k, 2, across_x).wait_recv()
        parts = [msg.at[k, cp], rpart.at[k, 1], xrecv.at[k]]
        outs = []
        for h in range(heads):
            _, fac = scales(parts, h)
            rows = slice(h * hd, (h + 1) * hd)
            srow = slice(stat + heads + h, stat + heads + h + 1)
            inv = 1.0 / sum(p[srow, :] * f for p, f in zip(parts, fac))
            outs.append(sum(p[rows, :] * (f * inv) for p, f in zip(parts, fac)))
        attn = jnp.concatenate(outs, axis=0).T.astype(BF16)

        @pl.when(k == 0)
        def _():
            for c in weight_copies() + resid_copies():
                c.wait()

        def part(cols):
            acc = None
            for g in range(group):
                d = mm(attn[g * tree:(g + 1) * tree], wout[g, :, cols])
                acc = d if acc is None else acc + d
            return acc.astype(BF16).astype(F32)

        psend[k] = part(other_cols)
        remote(psend.at[k], precv.at[k], k, 3, across_y).start()
        y_ref[k * CHUNK + cp, tp] = resid[k].astype(F32) + part(own_cols)

    def piece(k, owner_cp, owner_tp, lo=0, n=None):
        rows = pl.ds(lo, tree if n is None else n)
        return y_ref.at[k * CHUNK + owner_cp, owner_tp, rows]

    hf = (tree * 3 // 8) // 8 * 8
    hb = tree - hf
    pcp, xcp, dcp = chip * 2 + 1 - core, (1 - chip) * 2 + core, (1 - chip) * 2 + 1 - core

    def gather_copy(k, n):
        if n == 4:
            return remote(piece(k, cp, tp), piece(k, cp, tp), k, n, across_x)
        if n == 5:
            return remote(piece(k, cp, tp), piece(k, cp, tp), k, n, across_y)
        if n == 6:
            return remote(piece(k, cp, tp), piece(k, cp, tp), k, n, partner)
        if n == 7:
            return remote(piece(k, xcp, tp, 0, hf), piece(k, xcp, tp, 0, hf), k, n, across_y)
        if n == 8:
            return remote(piece(k, xcp, tp), piece(k, xcp, tp), k, n, partner)
        if n == 9:
            return remote(piece(k, cp, 1 - tp, hf, hb), piece(k, cp, 1 - tp, hf, hb), k, n, across_x)
        if n == 10:
            return remote(piece(k, cp, 1 - tp), piece(k, cp, 1 - tp), k, n, partner)
        if n == 11:
            return remote(piece(k, xcp, 1 - tp, 0, hf), piece(k, xcp, 1 - tp, 0, hf), k, n, partner)
        return remote(piece(k, xcp, 1 - tp, hf, hb), piece(k, xcp, 1 - tp, hf, hb), k, n, partner)

    def landed(k, n):
        src = {4: (xcp, tp, 0, tree), 5: (cp, 1 - tp, 0, tree), 6: (pcp, tp, 0, tree), 7: (xcp, 1 - tp, 0, hf), 8: (dcp, tp, 0, tree),
               9: (xcp, 1 - tp, hf, hb), 10: (pcp, 1 - tp, 0, tree), 11: (dcp, 1 - tp, 0, hf), 12: (dcp, 1 - tp, hf, hb)}[n]
        ref = piece(k, *src)
        remote(ref, ref, k, n, partner).wait_recv()

    def finish(k):
        remote(psend.at[k], precv.at[k], k, 3, across_y).wait_recv()
        total = y_ref[k * CHUNK + cp, tp] + precv[k]
        y_ref[k * CHUNK + cp, tp] = total.astype(BF16).astype(F32)
        for n in (4, 5, 6):
            gather_copy(k, n).start()

    def forward(k):
        landed(k, 4)
        gather_copy(k, 7).start()
        gather_copy(k, 8).start()
        landed(k, 5)
        gather_copy(k, 9).start()
        gather_copy(k, 10).start()

    def forward_diagonal(k):
        landed(k, 7)
        gather_copy(k, 11).start()
        landed(k, 9)
        gather_copy(k, 12).start()

    def emit(k):
        for n in (6, 8, 10, 11, 12):
            landed(k, n)
        for i in range(CHUNK):
            for side in range(2):
                out_ref[k * CHUNK + i, :, side * wcols:(side + 1) * wcols] = y_ref[k * CHUNK + i, side].astype(BF16)

    work = {'merge': merge_chip, 'query': queries, 'project': project, 'finish': finish, 'forward': forward, 'diagonal': forward_diagonal, 'emit': emit}

    @pl.loop(CHUNK, 1 + max(max(turns) for _, _, turns in SCHEDULE))
    def _(n):
        @pl.when(n < nreq)
        def _():
            attend(n)

        for name, lowest, turns in SCHEDULE:
            @pl.when(functools.reduce(jnp.logical_or, [n == t for t in turns]))
            def _():
                work[name](sum([jnp.where(n > t, 1, 0) for t in turns]) + lowest)

    @pl.loop(0, chunks)
    def _(k):
        remote(msg.at[k, 0], rpart.at[k, 0], k, 0, partner).wait_send()
        remote(msg.at[k, 0], rpart.at[k, 1], k, 1, partner).wait_send()
        remote(xsend.at[k], xrecv.at[k], k, 2, across_x).wait_send()
        remote(psend.at[k], precv.at[k], k, 3, across_y).wait_send()
        for n in range(4, 13):
            gather_copy(k, n).wait_send()


def solution(mesh):
    cache_spec = P('dp', None, 'cp', 'tp')
    row_spec = P('dp')

    def local_step(hidden, attn_gain, w_query, w_key, w_value, w_out, cache_k, cache_v, ctx_len, positions, tree_mask):
        nreq, tree, width = hidden.shape
        num_blocks, kv_heads, blk, hd = cache_k.shape[1], cache_k.shape[3], cache_k.shape[4], cache_k.shape[5]
        qdim, kvdim = w_query.shape[1], w_key.shape[1]
        group = qdim // kvdim
        chunks = nreq // CHUNK
        keys = jnp.swapaxes(cache_k[:, :, 0], -1, -2)
        values = jnp.swapaxes(cache_v[:, :, 0], -1, -2)
        hbm = pl.BlockSpec(memory_space=pl.ANY)
        vmem = pl.BlockSpec(memory_space=pltpu.VMEM)
        smem = pl.BlockSpec(memory_space=pltpu.SMEM)
        cache_shape = jax.ShapeDtypeStruct(keys.shape, BF16)
        per, slots = CHUNK // 2, 8
        steps, rows = nreq // per, per * tree
        qcols = group * tree
        rows_msg = kv_heads * hd + 2 * kv_heads
        ext = hd + tree + 16
        late_blocks = num_blocks - num_blocks // 2
        query, tables, first_msgs, new_keys, new_vals = pl.pallas_call(
            cache_kernel,
            in_specs=[smem] + [vmem] * 4 + [hbm] * 6,
            out_specs=[vmem, vmem, hbm, hbm, hbm],
            out_shape=[jax.ShapeDtypeStruct((EARLY_CHUNKS, CHUNK, kv_heads, hd, qcols), BF16), jax.ShapeDtypeStruct((steps, 2, hd // 2, rows), F32),
                       jax.ShapeDtypeStruct((CHUNK, rows_msg, qcols), F32), cache_shape, cache_shape],
            scratch_shapes=[
                pltpu.VMEM((slots, 2, per, num_blocks, kv_heads, hd, blk), BF16),
                pltpu.VMEM((slots, per, tree, width), BF16),
                pltpu.VMEM((2, kvdim, rows), BF16),
                pltpu.VMEM((width, kvdim), BF16),
                pltpu.VMEM((width, kvdim), BF16),
                pltpu.VMEM((width, qdim), BF16),
                pltpu.VMEM((num_blocks, kv_heads, hd + 16, blk), BF16),
                pltpu.VMEM((late_blocks, kv_heads, ext, blk), BF16),
                pltpu.VMEM((kv_heads, ext, qcols), BF16),
                pltpu.VMEM((2, num_blocks * blk, qcols), F32),
                pltpu.VMEM((CHUNK, rows_msg, qcols), F32),
                pltpu.SemaphoreType.DMA((slots, 3)),
                pltpu.SemaphoreType.DMA((slots, 2)),
                pltpu.SemaphoreType.DMA((3,)),
                pltpu.SemaphoreType.DMA((CHUNK,)),
            ],
            compiler_params=pltpu.CompilerParams(vmem_limit_bytes=62 * 2**20),
            name='fill_caches',
        )(ctx_len, attn_gain, positions, jnp.asarray(rope_frequencies(hd)), tree_mask, w_key, w_value, w_query, hidden, keys, values)
        wide_rows = (chunks, tree, width // 2)
        out_hidden = pl.pallas_call(
            attend_kernel,
            in_specs=[smem, vmem] + [hbm] * 9,
            out_specs=vmem,
            out_shape=pltpu.VMEM((nreq, tree, width), BF16),
            scratch_shapes=[
                pltpu.VMEM((nreq, 2, tree, width // 2), F32),
                pltpu.VMEM((2, num_blocks, kv_heads, hd, blk), BF16),
                pltpu.VMEM((2, num_blocks, kv_heads, hd + 16, blk), BF16),
                pltpu.VMEM((late_blocks, kv_heads, ext, blk), BF16),
                pltpu.VMEM((kv_heads, ext, qcols), BF16),
                pltpu.VMEM((2, tree, tree), jnp.int32),
                pltpu.VMEM((2, num_blocks * blk, qcols), F32),
                pltpu.VMEM((chunks, CHUNK, rows_msg, qcols), F32),
                pltpu.VMEM((chunks, 2, rows_msg, qcols), F32),
                pltpu.VMEM((chunks, rows_msg, qcols), F32),
                pltpu.VMEM((chunks, rows_msg, qcols), F32),
                pltpu.VMEM(wide_rows, F32),
                pltpu.VMEM(wide_rows, F32),
                pltpu.VMEM((group, kv_heads * hd, width), BF16),
                pltpu.VMEM(wide_rows, BF16),
                pltpu.VMEM((width, qdim), BF16),
                pltpu.VMEM((CHUNK, tree, width), BF16),
                pltpu.VMEM((CHUNK // per, 2, hd // 2, rows), F32),
                pltpu.VMEM((EARLY_CHUNKS, CHUNK, kv_heads, hd, qcols), BF16),
                pltpu.SemaphoreType.DMA((2, 3)),
                pltpu.SemaphoreType.DMA((group, kv_heads)),
                pltpu.SemaphoreType.DMA((chunks,)),
                pltpu.SemaphoreType.DMA((5,)),
                pltpu.SemaphoreType.DMA((chunks, 13)),
                pltpu.SemaphoreType.DMA((chunks, 13)),
            ],
            compiler_params=pltpu.CompilerParams(collective_id=0, has_side_effects=True, vmem_limit_bytes=56 * 2**20),
            name='attend_and_combine',
        )(ctx_len, attn_gain, query, tables, first_msgs, tree_mask, new_keys, new_vals, hidden, w_query, w_out)
        return (out_hidden, jnp.swapaxes(new_keys, -1, -2)[:, :, None], jnp.swapaxes(new_vals, -1, -2)[:, :, None])

    return jax.shard_map(local_step, mesh=mesh, in_specs=(row_spec, P(), P(None, 'tp'), P(None, 'tp'), P(None, 'tp'), P('tp', None), cache_spec, cache_spec, row_spec, row_spec, row_spec), out_specs=(row_spec, cache_spec, cache_spec), check_vma=False)
```

```python
import functools
import math
import jax
import jax.numpy as jnp
import numpy as np
from jax import lax
from jax.experimental import pallas as pl
from jax.experimental.pallas import tpu as pltpu
from jax.sharding import PartitionSpec as P

ROPE_THETA = 500000.0
NORM_EPS = 1e-5
MASKED = -1e30
LOG2E = math.log2(math.e)
MESH = pl.DeviceIdType.MESH
F32 = jnp.float32
BF16 = jnp.bfloat16
CHUNK = 4
EARLY_CHUNKS = 3

SCHEDULE = (
    ('emit', 0, (29, 31, 35, 36, 37, 38)),
    ('diagonal', 0, (22, 29, 30, 33, 34, 35)),
    ('forward', 0, (15, 17, 26, 30, 31, 32)),
    ('project', 0, (9, 10, 17, 19, 24, 25)),
    ('query', EARLY_CHUNKS, (9, 14, 16)),
    ('merge', 0, (4, 7, 9, 15, 19, 21)),
    ('finish', 0, (10, 13, 21, 24, 27, 28)),
)

def mm(a, b):
    return jnp.dot(a, b, preferred_element_type=F32)


def mm_tn(a, b):
    return lax.dot_general(a, b, (((0,), (0,)), ((), ())), preferred_element_type=F32)


def rope_frequencies(head_dim):
    freq_idx = np.arange(head_dim // 2, dtype=np.float32)
    inv_freq = np.float32(1.0) / (np.float32(ROPE_THETA) ** (np.float32(2.0) * freq_idx / np.float32(head_dim)))
    wavelen = np.float32(2.0 * math.pi) / inv_freq
    smooth = (np.float32(8192.0) / wavelen - np.float32(1.0)) / np.float32(3.0)
    blended = (np.float32(1.0) - smooth) * inv_freq / np.float32(8.0) + smooth * inv_freq
    return np.where(wavelen < 2048.0, inv_freq, np.where(wavelen > 8192.0, inv_freq / np.float32(8.0), blended)).astype(np.float32)


def cos_sin(angle):
    turns = jnp.floor(angle * (2.0 / math.pi) + 0.5)
    r = ((angle - turns * 1.5703125) - turns * 4.837512969970703125e-4) - turns * 7.549789954891882e-8
    z = r * r
    sin_r = r + r * z * (-1.6666654611e-1 + z * (8.3321608736e-3 + z * -1.9515295891e-4))
    cos_r = 1.0 - 0.5 * z + z * z * (4.166664568298827e-2 + z * (-1.388731625493765e-3 + z * 2.443315711809948e-5))
    quarter = turns.astype(jnp.int32) & 3
    odd = (quarter & 1) == 1
    cos, sin = jnp.where(odd, sin_r, cos_r), jnp.where(odd, cos_r, sin_r)
    return jnp.where((quarter == 1) | (quarter == 2), -cos, cos), jnp.where(quarter >= 2, -sin, sin)


def normed_rows(x, gain):
    wide = x.astype(F32)
    inv_rms = lax.rsqrt(jnp.mean(wide * wide, axis=-1, keepdims=True) + NORM_EPS)
    return (wide * inv_rms * gain.astype(F32)[None, :]).astype(BF16)


def rotate(rows, cos, sin):
    half = rows.shape[0] // 2
    first, second = rows[:half], rows[half:]
    return jnp.concatenate([first * cos - second * sin, second * cos + first * sin], axis=0)


def project_queries(h, wq_ref, cos, sin, out, hd, group, tree):
    reqs = h.shape[0] // tree
    for head in range(wq_ref.shape[1] // (group * hd)):
        q_t = mm(h, wq_ref[:, head * group * hd:(head + 1) * group * hd]).T
        parts = [rotate(q_t[g * hd:(g + 1) * hd], cos, sin) for g in range(group)]
        for i in range(reqs):
            out(i, head, jnp.concatenate([p[:, i * tree:(i + 1) * tree] for p in parts], axis=1).astype(BF16))


def prepare(vref, qext, hd, tree):
    num_blocks, heads, vrows, blk = vref.shape
    ones = jnp.ones((vrows - hd, blk), BF16)
    pad = qext.shape[1] - hd - tree
    hide = jnp.where(lax.broadcasted_iota(jnp.int32, (pad, qext.shape[2]), 0) == 0, MASKED, 0.0).astype(BF16)
    for h in range(heads):
        for j in range(num_blocks):
            vref[j, h, hd:, :] = ones
        qext[h, hd + tree:, :] = hide


def attention(ctx, tree_mask, qref, kref, vref, kext, qext, scores, out, cp):
    num_blocks, heads, hd, blk = kref.shape
    qcols, tree = qext.shape[2], tree_mask.shape[0]
    pad = qext.shape[1] - hd - tree
    late = num_blocks // 2
    coef = hd ** -0.5 * LOG2E
    seen = jnp.concatenate([tree_mask.astype(F32)] * (qcols // tree), axis=0).T
    bias = jnp.where(seen > 0.0, 0.0, MASKED).astype(BF16)
    for h in range(heads):
        qext[h, :hd, :] = qref[h]
        qext[h, hd:hd + tree, :] = bias
    for j in range(late, num_blocks):
        off = (j * 4 + cp) * blk - ctx
        tok = off + lax.broadcasted_iota(jnp.int32, (tree, blk), 1)
        pick = jnp.where(tok == lax.broadcasted_iota(jnp.int32, (tree, blk), 0), 1.0, 0.0).astype(BF16)
        tok_p = off + lax.broadcasted_iota(jnp.int32, (pad, blk), 1)
        tail = jnp.where((tok_p >= tree) & (lax.broadcasted_iota(jnp.int32, (pad, blk), 0) == 0), 1.0, 0.0).astype(BF16)
        tok_h = off + lax.broadcasted_iota(jnp.int32, (hd, blk), 1)
        for h in range(heads):
            kext[j - late, h, :hd, :] = jnp.where(tok_h < tree, kref[j, h].astype(F32), 0.0).astype(BF16)
            kext[j - late, h, hd:hd + tree, :] = pick
            kext[j - late, h, hd + tree:, :] = tail

    def score(h, j):
        if j < late:
            s = mm_tn(kref[j, h], qext[h, :hd, :])
        else:
            s = mm_tn(kext[j - late, h], qext[h])
        scores[h % 2, j * blk:(j + 1) * blk, :] = s
        return jnp.max(s.reshape(blk // 8, 8, qcols), axis=0)

    tops = [None] * heads
    tops[0] = functools.reduce(jnp.maximum, [score(0, j) for j in range(num_blocks)])
    for h in range(heads):
        top = jnp.max(tops[h], axis=0, keepdims=True)
        shift = top * coef
        total, nxt = None, []
        for j in range(num_blocks):
            if h + 1 < heads:
                nxt.append(score(h + 1, j))
            p = jnp.exp2(scores[h % 2, j * blk:(j + 1) * blk, :] * coef - shift).astype(BF16)
            o = mm(vref[j, h], p)
            total = o if total is None else total + o
        if h + 1 < heads:
            tops[h + 1] = functools.reduce(jnp.maximum, nxt)
        out[h * hd:(h + 1) * hd, :] = total[:hd]
        out[heads * hd + h:heads * hd + h + 1, :] = top
        out[heads * hd + heads + h:heads * hd + heads + h + 1, :] = total[hd:hd + 1]


def cache_kernel(ctx_ref, gain_ref, pos_ref, freq_ref, mask_ref, wk_hbm, wv_hbm, wq_hbm, x_hbm, kc_hbm, vc_hbm,
                 q_ref, tab_ref, msg_hbm, ko_hbm, vo_hbm,
                 buf, xbuf, new_ref, wk_ref, wv_ref, wq_ref, vbuf, kext, qext, scores, msg, in_sem, out_sem, w_sem, msg_sem):
    cp_rank, cp_size = lax.axis_index('cp'), lax.axis_size('cp')
    chunks, _, per, num_blocks, kv_heads, hd, blk = buf.shape
    tree = pos_ref.shape[1]
    group = q_ref.shape[4] // tree
    width = x_hbm.shape[2]
    half = hd // 2
    cols = per * tree

    def rows_of(c):
        return pl.ds(c * per, per)

    def fetch_rows(c):
        return pltpu.make_async_copy(x_hbm.at[rows_of(c)], xbuf.at[c], in_sem.at[c, 2])

    def fetch(c):
        return [pltpu.make_async_copy(src.at[rows_of(c)], buf.at[c, n], in_sem.at[c, n]) for n, src in enumerate((kc_hbm, vc_hbm))]

    def flush(c):
        return [pltpu.make_async_copy(buf.at[c, n], dst.at[rows_of(c)], out_sem.at[c, n]) for n, dst in enumerate((ko_hbm, vo_hbm))]

    kv_weights = [pltpu.make_async_copy(src, dst, w_sem.at[n]) for n, (src, dst) in enumerate(((wk_hbm, wk_ref), (wv_hbm, wv_ref)))]
    q_weight = pltpu.make_async_copy(wq_hbm, wq_ref, w_sem.at[2])
    for c in [fetch_rows(0)] + kv_weights + fetch(0) + [q_weight]:
        c.start()
    for n in range(1, chunks):
        for c in [fetch_rows(n)] + fetch(n):
            c.start()
    prepare(vbuf, qext, hd, tree)
    diag = lax.broadcasted_iota(jnp.int32, (half, half), 0) == lax.broadcasted_iota(jnp.int32, (half, half), 1)
    freq = jnp.sum(jnp.where(diag, freq_ref[...][None, :], 0.0), axis=1, keepdims=True)
    for c in kv_weights:
        c.wait()

    @pl.loop(0, chunks + EARLY_CHUNKS - 1)
    def _(turn):
        again = turn >= chunks
        k = turn - jnp.where(again, chunks - 1, 0)

        @pl.when(turn < chunks)
        def _():
            fetch_rows(k).wait()

        h = normed_rows(xbuf[k].reshape(cols, width), gain_ref[...])
        pos = jnp.concatenate([pos_ref[pl.ds(k * per + i, 1), :] for i in range(per)], axis=1).astype(F32)
        cos, sin = cos_sin(pos * freq)

        @pl.when(turn < chunks)
        def _():
            tab_ref[k, 0] = cos
            tab_ref[k, 1] = sin
            key_t = mm(h, wk_ref[...]).T
            for n in range(kv_heads):
                new_ref[0, n * hd:(n + 1) * hd, :] = rotate(key_t[n * hd:(n + 1) * hd], cos, sin).astype(BF16)
            new_ref[1] = mm(h, wv_ref[...]).T.astype(BF16)
            for c in fetch(k):
                c.wait()
            for i in range(per):
                ctx = ctx_ref[k * per + i]
                for j in range(num_blocks // 2, num_blocks):
                    first_pos = (j * cp_size + cp_rank) * blk

                    @pl.when((first_pos < ctx + tree) & (first_pos + blk > ctx))
                    def _():
                        tok = first_pos - ctx + lax.broadcasted_iota(jnp.int32, (cols, blk), 1)
                        row = lax.broadcasted_iota(jnp.int32, (cols, blk), 0) - i * tree
                        pick = jnp.where((row == tok) & (row >= 0) & (row < tree), 1.0, 0.0).astype(BF16)
                        tok_h = first_pos - ctx + lax.broadcasted_iota(jnp.int32, (hd, blk), 1)
                        fresh = (tok_h >= 0) & (tok_h < tree)
                        for n in range(2):
                            put = mm(new_ref[n], pick)
                            for head in range(kv_heads):
                                old = buf[k, n, i, j, head].astype(F32)
                                buf[k, n, i, j, head] = jnp.where(fresh, put[head * hd:(head + 1) * hd], old).astype(BF16)

            for c in flush(k):
                c.start()

        @pl.when(turn == 0)
        def _():
            q_weight.wait()

        @pl.when((turn == 0) | (turn >= chunks))
        def _():
            def out(i, head, value):
                q_ref[k, i, head] = value

            project_queries(h, wq_ref, cos, sin, out, hd, group, tree)

        @pl.when(turn == 0)
        def _():
            @pl.loop(0, per)
            def _(i):
                for j in range(num_blocks):
                    for head in range(kv_heads):
                        vbuf[j, head, :hd, :] = buf[0, 1, i, j, head]
                attention(ctx_ref[i], mask_ref[i], q_ref.at[0, i], buf.at[0, 0, i], vbuf, kext, qext, scores, msg.at[i], cp_rank)
                pltpu.make_async_copy(msg.at[i], msg_hbm.at[i], msg_sem.at[i]).start()

    for i in range(per):
        pltpu.make_async_copy(msg.at[i], msg_hbm.at[i], msg_sem.at[i]).wait()
    for n in range(chunks):
        for c in flush(n):
            c.wait()


def attend_kernel(ctx_ref, gain_ref, q_hbm, tab_hbm, msg_hbm, mask_hbm, kc_hbm, vc_hbm, hid_hbm, wq_hbm, wo_hbm, out_ref,
                  y_ref, kbuf, vbuf, kext, qext, mbuf, scores, msg, rpart, xsend, xrecv, psend, precv, wout, resid, wq_ref, xbuf, tbuf, qbuf,
                  kv_sem, w_sem, hid_sem, q_sem, snd, rcv):
    cp, tp = lax.axis_index('cp'), lax.axis_index('tp')
    chip, core = cp // 2, cp % 2
    partner = {'cp': chip * 2 + 1 - core}
    across_x = {'cp': (1 - chip) * 2 + core}
    across_y = {'tp': 1 - tp}
    _, _, heads, hd, qcols = q_hbm.shape
    nreq = mask_hbm.shape[0]
    tree = mask_hbm.shape[1]
    group = qcols // tree
    num_blocks, blk = kbuf.shape[1], kbuf.shape[4]
    chunks = nreq // CHUNK
    width = wo_hbm.shape[1]
    wcols = width // 2
    coef = hd ** -0.5 * LOG2E
    own_cols = pl.ds(pl.multiple_of(tp * wcols, wcols), wcols)
    other_cols = pl.ds(pl.multiple_of((1 - tp) * wcols, wcols), wcols)

    def remote(src, dst, k, n, to):
        return pltpu.make_async_remote_copy(src_ref=src, dst_ref=dst, send_sem=snd.at[k, n], recv_sem=rcv.at[k, n], device_id=to, device_id_type=MESH)

    barrier = pltpu.get_barrier_semaphore()
    for to in (partner, across_x, across_y):
        pl.semaphore_signal(barrier, inc=1, device_id=to, device_id_type=MESH)

    def request_of(n):
        return (n // CHUNK) * CHUNK + (2 * (1 - chip) + n % CHUNK) % CHUNK

    def fetch(n):
        r, to = request_of(n), n % 2
        return [pltpu.make_async_copy(kc_hbm.at[r], kbuf.at[to], kv_sem.at[to, 0]),
                pltpu.make_async_copy(vc_hbm.at[r], vbuf.at[to, :, :, pl.ds(0, hd), :], kv_sem.at[to, 1]),
                pltpu.make_async_copy(mask_hbm.at[r], mbuf.at[to], kv_sem.at[to, 2])]

    def weight_copies():
        out = []
        for g in range(group):
            for h in range(heads):
                out.append(pltpu.make_async_copy(wo_hbm.at[pl.ds((h * group + g) * hd, hd)], wout.at[g, pl.ds(h * hd, hd)], w_sem.at[g, h]))
        return out

    def resid_copies():
        return [pltpu.make_async_copy(hid_hbm.at[k * CHUNK + cp, :, own_cols], resid.at[k], hid_sem.at[k]) for k in range(chunks)]

    first_queries = pltpu.make_async_copy(q_hbm, qbuf, q_sem.at[0])
    query_weight = pltpu.make_async_copy(wq_hbm, wq_ref, q_sem.at[1])

    def chunk_copies(k):
        pairs = tbuf.shape[0]
        return [pltpu.make_async_copy(hid_hbm.at[pl.ds(k * CHUNK, CHUNK)], xbuf, q_sem.at[2]),
                pltpu.make_async_copy(tab_hbm.at[pl.ds(k * pairs, pairs)], tbuf, q_sem.at[3])]

    first_msgs = pltpu.make_async_copy(msg_hbm, msg.at[0], q_sem.at[4])
    for c in [first_msgs] + fetch(CHUNK) + [first_queries]:
        c.start()
    for to in range(2):
        prepare(vbuf.at[to], qext, hd, tree)
    pl.semaphore_wait(barrier, 3)
    first_msgs.wait()

    def share(k, i, which):
        @pl.when(i % 2 != core)
        def _():
            remote(msg.at[k, i], rpart.at[k, which], k, which, partner).start()

    for n in range(CHUNK):
        share(0, (2 * (1 - chip) + n) % CHUNK, n // 2)
    for c in weight_copies() + resid_copies() + chunk_copies(EARLY_CHUNKS) + [query_weight]:
        c.start()
    first_queries.wait()

    def queries(k):
        for c in chunk_copies(k):
            c.wait()

        @pl.when(k == EARLY_CHUNKS)
        def _():
            query_weight.wait()

        h = normed_rows(xbuf[...].reshape(CHUNK * tree, width), gain_ref[...])
        cos = jnp.concatenate([tbuf[p, 0] for p in range(tbuf.shape[0])], axis=1)
        sin = jnp.concatenate([tbuf[p, 1] for p in range(tbuf.shape[0])], axis=1)

        def out(i, head, value):
            qbuf[k % EARLY_CHUNKS, i, head] = value

        project_queries(h, wq_ref, cos, sin, out, hd, group, tree)

        @pl.when(k + 1 < chunks)
        def _():
            for c in chunk_copies(k + 1):
                c.start()

    def attend(n):
        k, r, slot = n // CHUNK, request_of(n), n % 2
        i = r - k * CHUNK

        @pl.when(n + 1 < nreq)
        def _():
            for c in fetch(n + 1):
                c.start()

        ctx = ctx_ref[r]
        for c in fetch(n):
            c.wait()
        attention(ctx, mbuf[slot], qbuf.at[k % EARLY_CHUNKS, i], kbuf.at[slot], vbuf.at[slot], kext, qext, scores, msg.at[k, i], cp)

        share(k, i, (n % CHUNK) // 2)

    stat = heads * hd

    def scales(parts, h):
        tops = [p[stat + h:stat + h + 1, :] for p in parts]
        top = functools.reduce(jnp.maximum, tops)
        return top, [jnp.exp2((t - top) * coef) for t in tops]

    def merge_chip(k):
        remote(msg.at[k, 0], rpart.at[k, 0], k, 0, partner).wait_recv()
        parts = [msg.at[k, 2 * (1 - chip) + core], rpart.at[k, 0]]
        for h in range(heads):
            top, fac = scales(parts, h)
            rows = slice(h * hd, (h + 1) * hd)
            xsend[k, rows, :] = sum(p[rows, :] * f for p, f in zip(parts, fac))
            xsend[k, stat + h:stat + h + 1, :] = top
            srow = slice(stat + heads + h, stat + heads + h + 1)
            xsend[k, srow, :] = sum(p[srow, :] * f for p, f in zip(parts, fac))
        remote(xsend.at[k], xrecv.at[k], k, 2, across_x).start()

    def project(k):
        remote(msg.at[k, 0], rpart.at[k, 1], k, 1, partner).wait_recv()
        remote(xsend.at[k], xrecv.at[k], k, 2, across_x).wait_recv()
        parts = [msg.at[k, cp], rpart.at[k, 1], xrecv.at[k]]
        outs = []
        for h in range(heads):
            _, fac = scales(parts, h)
            rows = slice(h * hd, (h + 1) * hd)
            srow = slice(stat + heads + h, stat + heads + h + 1)
            inv = 1.0 / sum(p[srow, :] * f for p, f in zip(parts, fac))
            outs.append(sum(p[rows, :] * (f * inv) for p, f in zip(parts, fac)))
        attn = jnp.concatenate(outs, axis=0).T.astype(BF16)

        @pl.when(k == 0)
        def _():
            for c in weight_copies() + resid_copies():
                c.wait()

        def part(cols):
            acc = None
            for g in range(group):
                d = mm(attn[g * tree:(g + 1) * tree], wout[g, :, cols])
                acc = d if acc is None else acc + d
            return acc.astype(BF16).astype(F32)

        psend[k] = part(other_cols)
        remote(psend.at[k], precv.at[k], k, 3, across_y).start()
        y_ref[k * CHUNK + cp, tp] = resid[k].astype(F32) + part(own_cols)

    def piece(k, owner_cp, owner_tp, lo=0, n=None):
        rows = pl.ds(lo, tree if n is None else n)
        return y_ref.at[k * CHUNK + owner_cp, owner_tp, rows]

    hf = (tree * 3 // 8) // 8 * 8
    hb = tree - hf
    pcp, xcp, dcp = chip * 2 + 1 - core, (1 - chip) * 2 + core, (1 - chip) * 2 + 1 - core

    def gather_copy(k, n):
        if n == 4:
            return remote(piece(k, cp, tp), piece(k, cp, tp), k, n, across_x)
        if n == 5:
            return remote(piece(k, cp, tp), piece(k, cp, tp), k, n, across_y)
        if n == 6:
            return remote(piece(k, cp, tp), piece(k, cp, tp), k, n, partner)
        if n == 7:
            return remote(piece(k, xcp, tp, 0, hf), piece(k, xcp, tp, 0, hf), k, n, across_y)
        if n == 8:
            return remote(piece(k, xcp, tp), piece(k, xcp, tp), k, n, partner)
        if n == 9:
            return remote(piece(k, cp, 1 - tp, hf, hb), piece(k, cp, 1 - tp, hf, hb), k, n, across_x)
        if n == 10:
            return remote(piece(k, cp, 1 - tp), piece(k, cp, 1 - tp), k, n, partner)
        if n == 11:
            return remote(piece(k, xcp, 1 - tp, 0, hf), piece(k, xcp, 1 - tp, 0, hf), k, n, partner)
        return remote(piece(k, xcp, 1 - tp, hf, hb), piece(k, xcp, 1 - tp, hf, hb), k, n, partner)

    def landed(k, n):
        src = {4: (xcp, tp, 0, tree), 5: (cp, 1 - tp, 0, tree), 6: (pcp, tp, 0, tree), 7: (xcp, 1 - tp, 0, hf), 8: (dcp, tp, 0, tree),
               9: (xcp, 1 - tp, hf, hb), 10: (pcp, 1 - tp, 0, tree), 11: (dcp, 1 - tp, 0, hf), 12: (dcp, 1 - tp, hf, hb)}[n]
        ref = piece(k, *src)
        remote(ref, ref, k, n, partner).wait_recv()

    def finish(k):
        remote(psend.at[k], precv.at[k], k, 3, across_y).wait_recv()
        total = y_ref[k * CHUNK + cp, tp] + precv[k]
        y_ref[k * CHUNK + cp, tp] = total.astype(BF16).astype(F32)
        for n in (4, 5, 6):
            gather_copy(k, n).start()

    def forward(k):
        landed(k, 4)
        gather_copy(k, 7).start()
        gather_copy(k, 8).start()
        landed(k, 5)
        gather_copy(k, 9).start()
        gather_copy(k, 10).start()

    def forward_diagonal(k):
        landed(k, 7)
        gather_copy(k, 11).start()
        landed(k, 9)
        gather_copy(k, 12).start()

    def emit(k):
        for n in (6, 8, 10, 11, 12):
            landed(k, n)
        for i in range(CHUNK):
            for side in range(2):
                out_ref[k * CHUNK + i, :, side * wcols:(side + 1) * wcols] = y_ref[k * CHUNK + i, side].astype(BF16)

    work = {'merge': merge_chip, 'query': queries, 'project': project, 'finish': finish, 'forward': forward, 'diagonal': forward_diagonal, 'emit': emit}

    @pl.loop(CHUNK, 1 + max(max(turns) for _, _, turns in SCHEDULE))
    def _(n):
        @pl.when(n < nreq)
        def _():
            attend(n)

        for name, lowest, turns in SCHEDULE:
            @pl.when(functools.reduce(jnp.logical_or, [n == t for t in turns]))
            def _():
                work[name](sum([jnp.where(n > t, 1, 0) for t in turns]) + lowest)

    @pl.loop(0, chunks)
    def _(k):
        remote(msg.at[k, 0], rpart.at[k, 0], k, 0, partner).wait_send()
        remote(msg.at[k, 0], rpart.at[k, 1], k, 1, partner).wait_send()
        remote(xsend.at[k], xrecv.at[k], k, 2, across_x).wait_send()
        remote(psend.at[k], precv.at[k], k, 3, across_y).wait_send()
        for n in range(4, 13):
            gather_copy(k, n).wait_send()


def solution(mesh):
    cache_spec = P('dp', None, 'cp', 'tp')
    row_spec = P('dp')

    def local_step(hidden, attn_gain, w_query, w_key, w_value, w_out, cache_k, cache_v, ctx_len, positions, tree_mask):
        nreq, tree, width = hidden.shape
        num_blocks, kv_heads, blk, hd = cache_k.shape[1], cache_k.shape[3], cache_k.shape[4], cache_k.shape[5]
        qdim, kvdim = w_query.shape[1], w_key.shape[1]
        group = qdim // kvdim
        chunks = nreq // CHUNK
        keys = jnp.swapaxes(cache_k[:, :, 0], -1, -2)
        values = jnp.swapaxes(cache_v[:, :, 0], -1, -2)
        hbm = pl.BlockSpec(memory_space=pl.ANY)
        vmem = pl.BlockSpec(memory_space=pltpu.VMEM)
        smem = pl.BlockSpec(memory_space=pltpu.SMEM)
        cache_shape = jax.ShapeDtypeStruct(keys.shape, BF16)
        rows = CHUNK * tree
        qcols = group * tree
        rows_msg = kv_heads * hd + 2 * kv_heads
        ext = hd + tree + 16
        late_blocks = num_blocks - num_blocks // 2
        query, tables, first_msgs, new_keys, new_vals = pl.pallas_call(
            cache_kernel,
            in_specs=[smem] + [vmem] * 4 + [hbm] * 6,
            out_specs=[vmem, vmem, hbm, hbm, hbm],
            out_shape=[jax.ShapeDtypeStruct((EARLY_CHUNKS, CHUNK, kv_heads, hd, qcols), BF16), jax.ShapeDtypeStruct((chunks, 2, hd // 2, rows), F32),
                       jax.ShapeDtypeStruct((CHUNK, rows_msg, qcols), F32), cache_shape, cache_shape],
            scratch_shapes=[
                pltpu.VMEM((chunks, 2, CHUNK, num_blocks, kv_heads, hd, blk), BF16),
                pltpu.VMEM((chunks, CHUNK, tree, width), BF16),
                pltpu.VMEM((2, kvdim, rows), BF16),
                pltpu.VMEM((width, kvdim), BF16),
                pltpu.VMEM((width, kvdim), BF16),
                pltpu.VMEM((width, qdim), BF16),
                pltpu.VMEM((num_blocks, kv_heads, hd + 16, blk), BF16),
                pltpu.VMEM((late_blocks, kv_heads, ext, blk), BF16),
                pltpu.VMEM((kv_heads, ext, qcols), BF16),
                pltpu.VMEM((2, num_blocks * blk, qcols), F32),
                pltpu.VMEM((CHUNK, rows_msg, qcols), F32),
                pltpu.SemaphoreType.DMA((chunks, 3)),
                pltpu.SemaphoreType.DMA((chunks, 2)),
                pltpu.SemaphoreType.DMA((3,)),
                pltpu.SemaphoreType.DMA((CHUNK,)),
            ],
            compiler_params=pltpu.CompilerParams(vmem_limit_bytes=62 * 2**20),
            name='fill_caches',
        )(ctx_len, attn_gain, positions, jnp.asarray(rope_frequencies(hd)), tree_mask, w_key, w_value, w_query, hidden, keys, values)
        wide_rows = (chunks, tree, width // 2)
        out_hidden = pl.pallas_call(
            attend_kernel,
            in_specs=[smem, vmem] + [hbm] * 9,
            out_specs=vmem,
            out_shape=pltpu.VMEM((nreq, tree, width), BF16),
            scratch_shapes=[
                pltpu.VMEM((nreq, 2, tree, width // 2), F32),
                pltpu.VMEM((2, num_blocks, kv_heads, hd, blk), BF16),
                pltpu.VMEM((2, num_blocks, kv_heads, hd + 16, blk), BF16),
                pltpu.VMEM((late_blocks, kv_heads, ext, blk), BF16),
                pltpu.VMEM((kv_heads, ext, qcols), BF16),
                pltpu.VMEM((2, tree, tree), jnp.int32),
                pltpu.VMEM((2, num_blocks * blk, qcols), F32),
                pltpu.VMEM((chunks, CHUNK, rows_msg, qcols), F32),
                pltpu.VMEM((chunks, 2, rows_msg, qcols), F32),
                pltpu.VMEM((chunks, rows_msg, qcols), F32),
                pltpu.VMEM((chunks, rows_msg, qcols), F32),
                pltpu.VMEM(wide_rows, F32),
                pltpu.VMEM(wide_rows, F32),
                pltpu.VMEM((group, kv_heads * hd, width), BF16),
                pltpu.VMEM(wide_rows, BF16),
                pltpu.VMEM((width, qdim), BF16),
                pltpu.VMEM((CHUNK, tree, width), BF16),
                pltpu.VMEM((1, 2, hd // 2, rows), F32),
                pltpu.VMEM((EARLY_CHUNKS, CHUNK, kv_heads, hd, qcols), BF16),
                pltpu.SemaphoreType.DMA((2, 3)),
                pltpu.SemaphoreType.DMA((group, kv_heads)),
                pltpu.SemaphoreType.DMA((chunks,)),
                pltpu.SemaphoreType.DMA((5,)),
                pltpu.SemaphoreType.DMA((chunks, 13)),
                pltpu.SemaphoreType.DMA((chunks, 13)),
            ],
            compiler_params=pltpu.CompilerParams(collective_id=0, has_side_effects=True, vmem_limit_bytes=56 * 2**20),
            name='attend_and_combine',
        )(ctx_len, attn_gain, query, tables, first_msgs, tree_mask, new_keys, new_vals, hidden, w_query, w_out)
        return (out_hidden, jnp.swapaxes(new_keys, -1, -2)[:, :, None], jnp.swapaxes(new_vals, -1, -2)[:, :, None])

    return jax.shard_map(local_step, mesh=mesh, in_specs=(row_spec, P(), P(None, 'tp'), P(None, 'tp'), P(None, 'tp'), P('tp', None), cache_spec, cache_spec, row_spec, row_spec, row_spec), out_specs=(row_spec, cache_spec, cache_spec), check_vma=False)
```

```python
import functools
import math
import jax
import jax.numpy as jnp
import numpy as np
from jax import lax
from jax.experimental import pallas as pl
from jax.experimental.pallas import tpu as pltpu
from jax.sharding import PartitionSpec as P

ROPE_THETA = 500000.0
NORM_EPS = 1e-5
MASKED = -1e30
LOG2E = math.log2(math.e)
MESH = pl.DeviceIdType.MESH
F32 = jnp.float32
BF16 = jnp.bfloat16
CHUNK = 4
EARLY_CHUNKS = 3

SCHEDULE = (
    ('emit', 0, (29, 31, 35, 36, 37, 38)),
    ('diagonal', 0, (22, 29, 30, 33, 34, 35)),
    ('forward', 0, (15, 17, 26, 30, 31, 32)),
    ('project', 0, (9, 10, 17, 19, 24, 25)),
    ('query', EARLY_CHUNKS, (9, 14, 16)),
    ('merge', 0, (4, 7, 9, 15, 19, 21)),
    ('finish', 0, (10, 13, 21, 24, 27, 28)),
)

def mm(a, b):
    return jnp.dot(a, b, preferred_element_type=F32)


def mm_tn(a, b):
    return lax.dot_general(a, b, (((0,), (0,)), ((), ())), preferred_element_type=F32)


def rope_frequencies(head_dim):
    freq_idx = np.arange(head_dim // 2, dtype=np.float32)
    inv_freq = np.float32(1.0) / (np.float32(ROPE_THETA) ** (np.float32(2.0) * freq_idx / np.float32(head_dim)))
    wavelen = np.float32(2.0 * math.pi) / inv_freq
    smooth = (np.float32(8192.0) / wavelen - np.float32(1.0)) / np.float32(3.0)
    blended = (np.float32(1.0) - smooth) * inv_freq / np.float32(8.0) + smooth * inv_freq
    return np.where(wavelen < 2048.0, inv_freq, np.where(wavelen > 8192.0, inv_freq / np.float32(8.0), blended)).astype(np.float32)


def cos_sin(angle):
    turns = jnp.floor(angle * (2.0 / math.pi) + 0.5)
    r = ((angle - turns * 1.5703125) - turns * 4.837512969970703125e-4) - turns * 7.549789954891882e-8
    z = r * r
    sin_r = r + r * z * (-1.6666654611e-1 + z * (8.3321608736e-3 + z * -1.9515295891e-4))
    cos_r = 1.0 - 0.5 * z + z * z * (4.166664568298827e-2 + z * (-1.388731625493765e-3 + z * 2.443315711809948e-5))
    quarter = turns.astype(jnp.int32) & 3
    odd = (quarter & 1) == 1
    cos, sin = jnp.where(odd, sin_r, cos_r), jnp.where(odd, cos_r, sin_r)
    return jnp.where((quarter == 1) | (quarter == 2), -cos, cos), jnp.where(quarter >= 2, -sin, sin)


def normed_rows(x, gain):
    wide = x.astype(F32)
    inv_rms = lax.rsqrt(jnp.mean(wide * wide, axis=-1, keepdims=True) + NORM_EPS)
    return (wide * inv_rms * gain.astype(F32)[None, :]).astype(BF16)


def rotate(rows, cos, sin):
    half = rows.shape[0] // 2
    first, second = rows[:half], rows[half:]
    return jnp.concatenate([first * cos - second * sin, second * cos + first * sin], axis=0)


def project_queries(h, wq_ref, cos, sin, out, hd, group, tree):
    reqs = h.shape[0] // tree
    for head in range(wq_ref.shape[1] // (group * hd)):
        q_t = mm(h, wq_ref[:, head * group * hd:(head + 1) * group * hd]).T
        parts = [rotate(q_t[g * hd:(g + 1) * hd], cos, sin) for g in range(group)]
        for i in range(reqs):
            out(i, head, jnp.concatenate([p[:, i * tree:(i + 1) * tree] for p in parts], axis=1).astype(BF16))


def prepare(vref, qext, hd, tree):
    num_blocks, heads, vrows, blk = vref.shape
    ones = jnp.ones((vrows - hd, blk), BF16)
    pad = qext.shape[1] - hd - tree
    hide = jnp.where(lax.broadcasted_iota(jnp.int32, (pad, qext.shape[2]), 0) == 0, MASKED, 0.0).astype(BF16)
    for h in range(heads):
        for j in range(num_blocks):
            vref[j, h, hd:, :] = ones
        qext[h, hd + tree:, :] = hide


def attention(ctx, tree_mask, qref, kref, vref, kext, qext, scores, out, cp):
    num_blocks, heads, hd, blk = kref.shape
    qcols, tree = qext.shape[2], tree_mask.shape[0]
    pad = qext.shape[1] - hd - tree
    late = num_blocks // 2
    coef = hd ** -0.5 * LOG2E
    seen = jnp.concatenate([tree_mask.astype(F32)] * (qcols // tree), axis=0).T
    bias = jnp.where(seen > 0.0, 0.0, MASKED).astype(BF16)
    for h in range(heads):
        qext[h, :hd, :] = qref[h]
        qext[h, hd:hd + tree, :] = bias
    for j in range(late, num_blocks):
        off = (j * 4 + cp) * blk - ctx
        tok = off + lax.broadcasted_iota(jnp.int32, (tree, blk), 1)
        pick = jnp.where(tok == lax.broadcasted_iota(jnp.int32, (tree, blk), 0), 1.0, 0.0).astype(BF16)
        tok_p = off + lax.broadcasted_iota(jnp.int32, (pad, blk), 1)
        tail = jnp.where((tok_p >= tree) & (lax.broadcasted_iota(jnp.int32, (pad, blk), 0) == 0), 1.0, 0.0).astype(BF16)
        tok_h = off + lax.broadcasted_iota(jnp.int32, (hd, blk), 1)
        for h in range(heads):
            kext[j - late, h, :hd, :] = jnp.where(tok_h < tree, kref[j, h].astype(F32), 0.0).astype(BF16)
            kext[j - late, h, hd:hd + tree, :] = pick
            kext[j - late, h, hd + tree:, :] = tail

    def score(h, j):
        if j < late:
            s = mm_tn(kref[j, h], qext[h, :hd, :])
        else:
            s = mm_tn(kext[j - late, h], qext[h])
        scores[h % 2, j * blk:(j + 1) * blk, :] = s
        return jnp.max(s.reshape(blk // 8, 8, qcols), axis=0)

    tops = [None] * heads
    tops[0] = functools.reduce(jnp.maximum, [score(0, j) for j in range(num_blocks)])
    for h in range(heads):
        top = jnp.max(tops[h], axis=0, keepdims=True)
        shift = top * coef
        total, nxt = None, []
        for j in range(num_blocks):
            if h + 1 < heads:
                nxt.append(score(h + 1, j))
            p = jnp.exp2(scores[h % 2, j * blk:(j + 1) * blk, :] * coef - shift).astype(BF16)
            o = mm(vref[j, h], p)
            total = o if total is None else total + o
        if h + 1 < heads:
            tops[h + 1] = functools.reduce(jnp.maximum, nxt)
        out[h * hd:(h + 1) * hd, :] = total[:hd]
        out[heads * hd + h:heads * hd + h + 1, :] = top
        out[heads * hd + heads + h:heads * hd + heads + h + 1, :] = total[hd:hd + 1]


def cache_kernel(ctx_ref, gain_ref, pos_ref, freq_ref, mask_ref, wk_hbm, wv_hbm, wq_hbm, x_hbm, kc_hbm, vc_hbm,
                 q_ref, tab_ref, msg_hbm, ko_hbm, vo_hbm,
                 buf, xbuf, new_ref, wk_ref, wv_ref, wq_ref, vbuf, kext, qext, scores, msg, in_sem, out_sem, w_sem, msg_sem):
    cp_rank, cp_size = lax.axis_index('cp'), lax.axis_size('cp')
    chunks, _, per, num_blocks, kv_heads, hd, blk = buf.shape
    tree = pos_ref.shape[1]
    group = q_ref.shape[4] // tree
    width = x_hbm.shape[2]
    half = hd // 2
    cols = per * tree

    def rows_of(c):
        return pl.ds(c * per, per)

    def fetch_rows(c):
        return pltpu.make_async_copy(x_hbm.at[rows_of(c)], xbuf.at[c], in_sem.at[c, 2])

    def fetch(c):
        return [pltpu.make_async_copy(src.at[rows_of(c)], buf.at[c, n], in_sem.at[c, n]) for n, src in enumerate((kc_hbm, vc_hbm))]

    def flush(c):
        return [pltpu.make_async_copy(buf.at[c, n], dst.at[rows_of(c)], out_sem.at[c, n]) for n, dst in enumerate((ko_hbm, vo_hbm))]

    kv_weights = [pltpu.make_async_copy(src, dst, w_sem.at[n]) for n, (src, dst) in enumerate(((wk_hbm, wk_ref), (wv_hbm, wv_ref)))]
    q_weight = pltpu.make_async_copy(wq_hbm, wq_ref, w_sem.at[2])
    for c in [fetch_rows(0)] + kv_weights:
        c.start()
    prepare(vbuf, qext, hd, tree)
    diag = lax.broadcasted_iota(jnp.int32, (half, half), 0) == lax.broadcasted_iota(jnp.int32, (half, half), 1)
    freq = jnp.sum(jnp.where(diag, freq_ref[...][None, :], 0.0), axis=1, keepdims=True)
    for c in kv_weights:
        c.wait()
    for c in fetch(0) + [q_weight]:
        c.start()

    @pl.loop(0, chunks + EARLY_CHUNKS - 1)
    def _(turn):
        again = turn >= chunks
        k = turn - jnp.where(again, chunks - 1, 0)

        @pl.when(turn < chunks)
        def _():
            fetch_rows(k).wait()

        h = normed_rows(xbuf[k].reshape(cols, width), gain_ref[...])
        pos = jnp.concatenate([pos_ref[pl.ds(k * per + i, 1), :] for i in range(per)], axis=1).astype(F32)
        cos, sin = cos_sin(pos * freq)

        @pl.when(turn < chunks)
        def _():
            tab_ref[k, 0] = cos
            tab_ref[k, 1] = sin
            key_t = mm(h, wk_ref[...]).T
            for n in range(kv_heads):
                new_ref[0, n * hd:(n + 1) * hd, :] = rotate(key_t[n * hd:(n + 1) * hd], cos, sin).astype(BF16)
            new_ref[1] = mm(h, wv_ref[...]).T.astype(BF16)
            for c in fetch(k):
                c.wait()
            for i in range(per):
                ctx = ctx_ref[k * per + i]
                for j in range(num_blocks // 2, num_blocks):
                    first_pos = (j * cp_size + cp_rank) * blk

                    @pl.when((first_pos < ctx + tree) & (first_pos + blk > ctx))
                    def _():
                        tok = first_pos - ctx + lax.broadcasted_iota(jnp.int32, (cols, blk), 1)
                        row = lax.broadcasted_iota(jnp.int32, (cols, blk), 0) - i * tree
                        pick = jnp.where((row == tok) & (row >= 0) & (row < tree), 1.0, 0.0).astype(BF16)
                        tok_h = first_pos - ctx + lax.broadcasted_iota(jnp.int32, (hd, blk), 1)
                        fresh = (tok_h >= 0) & (tok_h < tree)
                        for n in range(2):
                            put = mm(new_ref[n], pick)
                            for head in range(kv_heads):
                                old = buf[k, n, i, j, head].astype(F32)
                                buf[k, n, i, j, head] = jnp.where(fresh, put[head * hd:(head + 1) * hd], old).astype(BF16)

            for c in flush(k):
                c.start()

        @pl.when(turn == 0)
        def _():
            q_weight.wait()
            for n in range(1, chunks):
                for c in [fetch_rows(n)] + fetch(n):
                    c.start()

        @pl.when((turn == 0) | (turn >= chunks))
        def _():
            def out(i, head, value):
                q_ref[k, i, head] = value

            project_queries(h, wq_ref, cos, sin, out, hd, group, tree)

        @pl.when(turn == 0)
        def _():
            @pl.loop(0, per)
            def _(i):
                for j in range(num_blocks):
                    for head in range(kv_heads):
                        vbuf[j, head, :hd, :] = buf[0, 1, i, j, head]
                attention(ctx_ref[i], mask_ref[i], q_ref.at[0, i], buf.at[0, 0, i], vbuf, kext, qext, scores, msg.at[i], cp_rank)
                pltpu.make_async_copy(msg.at[i], msg_hbm.at[i], msg_sem.at[i]).start()

    for i in range(per):
        pltpu.make_async_copy(msg.at[i], msg_hbm.at[i], msg_sem.at[i]).wait()
    for n in range(chunks):
        for c in flush(n):
            c.wait()


def attend_kernel(ctx_ref, gain_ref, q_hbm, tab_hbm, msg_hbm, mask_hbm, kc_hbm, vc_hbm, hid_hbm, wq_hbm, wo_hbm, out_ref,
                  y_ref, kbuf, vbuf, kext, qext, mbuf, scores, msg, rpart, xsend, xrecv, psend, precv, wout, resid, wq_ref, xbuf, tbuf, qbuf,
                  kv_sem, w_sem, hid_sem, q_sem, snd, rcv):
    cp, tp = lax.axis_index('cp'), lax.axis_index('tp')
    chip, core = cp // 2, cp % 2
    partner = {'cp': chip * 2 + 1 - core}
    across_x = {'cp': (1 - chip) * 2 + core}
    across_y = {'tp': 1 - tp}
    _, _, heads, hd, qcols = q_hbm.shape
    nreq = mask_hbm.shape[0]
    tree = mask_hbm.shape[1]
    group = qcols // tree
    num_blocks, blk = kbuf.shape[1], kbuf.shape[4]
    chunks = nreq // CHUNK
    width = wo_hbm.shape[1]
    wcols = width // 2
    coef = hd ** -0.5 * LOG2E
    own_cols = pl.ds(pl.multiple_of(tp * wcols, wcols), wcols)
    other_cols = pl.ds(pl.multiple_of((1 - tp) * wcols, wcols), wcols)

    def remote(src, dst, k, n, to):
        return pltpu.make_async_remote_copy(src_ref=src, dst_ref=dst, send_sem=snd.at[k, n], recv_sem=rcv.at[k, n], device_id=to, device_id_type=MESH)

    barrier = pltpu.get_barrier_semaphore()
    for to in (partner, across_x, across_y):
        pl.semaphore_signal(barrier, inc=1, device_id=to, device_id_type=MESH)

    def request_of(n):
        return (n // CHUNK) * CHUNK + (2 * (1 - chip) + n % CHUNK) % CHUNK

    def fetch(n):
        r, to = request_of(n), n % 2
        return [pltpu.make_async_copy(kc_hbm.at[r], kbuf.at[to], kv_sem.at[to, 0]),
                pltpu.make_async_copy(vc_hbm.at[r], vbuf.at[to, :, :, pl.ds(0, hd), :], kv_sem.at[to, 1]),
                pltpu.make_async_copy(mask_hbm.at[r], mbuf.at[to], kv_sem.at[to, 2])]

    def weight_copies():
        out = []
        for g in range(group):
            for h in range(heads):
                out.append(pltpu.make_async_copy(wo_hbm.at[pl.ds((h * group + g) * hd, hd)], wout.at[g, pl.ds(h * hd, hd)], w_sem.at[g, h]))
        return out

    def resid_copies():
        return [pltpu.make_async_copy(hid_hbm.at[k * CHUNK + cp, :, own_cols], resid.at[k], hid_sem.at[k]) for k in range(chunks)]

    first_queries = pltpu.make_async_copy(q_hbm, qbuf, q_sem.at[0])
    query_weight = pltpu.make_async_copy(wq_hbm, wq_ref, q_sem.at[1])

    def chunk_copies(k):
        pairs = tbuf.shape[0]
        return [pltpu.make_async_copy(hid_hbm.at[pl.ds(k * CHUNK, CHUNK)], xbuf, q_sem.at[2]),
                pltpu.make_async_copy(tab_hbm.at[pl.ds(k * pairs, pairs)], tbuf, q_sem.at[3])]

    first_msgs = pltpu.make_async_copy(msg_hbm, msg.at[0], q_sem.at[4])
    for c in [first_msgs] + fetch(CHUNK) + [first_queries]:
        c.start()
    for to in range(2):
        prepare(vbuf.at[to], qext, hd, tree)
    pl.semaphore_wait(barrier, 3)
    first_msgs.wait()

    def share(k, i, which):
        @pl.when(i % 2 != core)
        def _():
            remote(msg.at[k, i], rpart.at[k, which], k, which, partner).start()

    for n in range(CHUNK):
        share(0, (2 * (1 - chip) + n) % CHUNK, n // 2)
    first_queries.wait()

    def queries(k):
        for c in chunk_copies(k):
            c.wait()

        @pl.when(k == EARLY_CHUNKS)
        def _():
            query_weight.wait()

        h = normed_rows(xbuf[...].reshape(CHUNK * tree, width), gain_ref[...])
        cos = jnp.concatenate([tbuf[p, 0] for p in range(tbuf.shape[0])], axis=1)
        sin = jnp.concatenate([tbuf[p, 1] for p in range(tbuf.shape[0])], axis=1)

        def out(i, head, value):
            qbuf[k % EARLY_CHUNKS, i, head] = value

        project_queries(h, wq_ref, cos, sin, out, hd, group, tree)

        @pl.when(k + 1 < chunks)
        def _():
            for c in chunk_copies(k + 1):
                c.start()

    def attend(n):
        k, r, slot = n // CHUNK, request_of(n), n % 2
        i = r - k * CHUNK

        @pl.when(n + 1 < nreq)
        def _():
            for c in fetch(n + 1):
                c.start()

        ctx = ctx_ref[r]
        for c in fetch(n):
            c.wait()
        attention(ctx, mbuf[slot], qbuf.at[k % EARLY_CHUNKS, i], kbuf.at[slot], vbuf.at[slot], kext, qext, scores, msg.at[k, i], cp)

        share(k, i, (n % CHUNK) // 2)

    stat = heads * hd

    def scales(parts, h):
        tops = [p[stat + h:stat + h + 1, :] for p in parts]
        top = functools.reduce(jnp.maximum, tops)
        return top, [jnp.exp2((t - top) * coef) for t in tops]

    def merge_chip(k):
        remote(msg.at[k, 0], rpart.at[k, 0], k, 0, partner).wait_recv()
        parts = [msg.at[k, 2 * (1 - chip) + core], rpart.at[k, 0]]
        for h in range(heads):
            top, fac = scales(parts, h)
            rows = slice(h * hd, (h + 1) * hd)
            xsend[k, rows, :] = sum(p[rows, :] * f for p, f in zip(parts, fac))
            xsend[k, stat + h:stat + h + 1, :] = top
            srow = slice(stat + heads + h, stat + heads + h + 1)
            xsend[k, srow, :] = sum(p[srow, :] * f for p, f in zip(parts, fac))
        remote(xsend.at[k], xrecv.at[k], k, 2, across_x).start()

    def project(k):
        remote(msg.at[k, 0], rpart.at[k, 1], k, 1, partner).wait_recv()
        remote(xsend.at[k], xrecv.at[k], k, 2, across_x).wait_recv()
        parts = [msg.at[k, cp], rpart.at[k, 1], xrecv.at[k]]
        outs = []
        for h in range(heads):
            _, fac = scales(parts, h)
            rows = slice(h * hd, (h + 1) * hd)
            srow = slice(stat + heads + h, stat + heads + h + 1)
            inv = 1.0 / sum(p[srow, :] * f for p, f in zip(parts, fac))
            outs.append(sum(p[rows, :] * (f * inv) for p, f in zip(parts, fac)))
        attn = jnp.concatenate(outs, axis=0).T.astype(BF16)

        @pl.when(k == 0)
        def _():
            for c in weight_copies() + resid_copies():
                c.wait()

        def part(cols):
            acc = None
            for g in range(group):
                d = mm(attn[g * tree:(g + 1) * tree], wout[g, :, cols])
                acc = d if acc is None else acc + d
            return acc.astype(BF16).astype(F32)

        psend[k] = part(other_cols)
        remote(psend.at[k], precv.at[k], k, 3, across_y).start()
        y_ref[k * CHUNK + cp, tp] = resid[k].astype(F32) + part(own_cols)

    def piece(k, owner_cp, owner_tp, lo=0, n=None):
        rows = pl.ds(lo, tree if n is None else n)
        return y_ref.at[k * CHUNK + owner_cp, owner_tp, rows]

    hf = (tree * 3 // 8) // 8 * 8
    hb = tree - hf
    pcp, xcp, dcp = chip * 2 + 1 - core, (1 - chip) * 2 + core, (1 - chip) * 2 + 1 - core

    def gather_copy(k, n):
        if n == 4:
            return remote(piece(k, cp, tp), piece(k, cp, tp), k, n, across_x)
        if n == 5:
            return remote(piece(k, cp, tp), piece(k, cp, tp), k, n, across_y)
        if n == 6:
            return remote(piece(k, cp, tp), piece(k, cp, tp), k, n, partner)
        if n == 7:
            return remote(piece(k, xcp, tp, 0, hf), piece(k, xcp, tp, 0, hf), k, n, across_y)
        if n == 8:
            return remote(piece(k, xcp, tp), piece(k, xcp, tp), k, n, partner)
        if n == 9:
            return remote(piece(k, cp, 1 - tp, hf, hb), piece(k, cp, 1 - tp, hf, hb), k, n, across_x)
        if n == 10:
            return remote(piece(k, cp, 1 - tp), piece(k, cp, 1 - tp), k, n, partner)
        if n == 11:
            return remote(piece(k, xcp, 1 - tp, 0, hf), piece(k, xcp, 1 - tp, 0, hf), k, n, partner)
        return remote(piece(k, xcp, 1 - tp, hf, hb), piece(k, xcp, 1 - tp, hf, hb), k, n, partner)

    def landed(k, n):
        src = {4: (xcp, tp, 0, tree), 5: (cp, 1 - tp, 0, tree), 6: (pcp, tp, 0, tree), 7: (xcp, 1 - tp, 0, hf), 8: (dcp, tp, 0, tree),
               9: (xcp, 1 - tp, hf, hb), 10: (pcp, 1 - tp, 0, tree), 11: (dcp, 1 - tp, 0, hf), 12: (dcp, 1 - tp, hf, hb)}[n]
        ref = piece(k, *src)
        remote(ref, ref, k, n, partner).wait_recv()

    def finish(k):
        remote(psend.at[k], precv.at[k], k, 3, across_y).wait_recv()
        total = y_ref[k * CHUNK + cp, tp] + precv[k]
        y_ref[k * CHUNK + cp, tp] = total.astype(BF16).astype(F32)
        for n in (4, 5, 6):
            gather_copy(k, n).start()

    def forward(k):
        landed(k, 4)
        gather_copy(k, 7).start()
        gather_copy(k, 8).start()
        landed(k, 5)
        gather_copy(k, 9).start()
        gather_copy(k, 10).start()

    def forward_diagonal(k):
        landed(k, 7)
        gather_copy(k, 11).start()
        landed(k, 9)
        gather_copy(k, 12).start()

    def emit(k):
        for n in (6, 8, 10, 11, 12):
            landed(k, n)
        for i in range(CHUNK):
            for side in range(2):
                out_ref[k * CHUNK + i, :, side * wcols:(side + 1) * wcols] = y_ref[k * CHUNK + i, side].astype(BF16)

    work = {'merge': merge_chip, 'query': queries, 'project': project, 'finish': finish, 'forward': forward, 'diagonal': forward_diagonal, 'emit': emit}

    @pl.loop(CHUNK, 1 + max(max(turns) for _, _, turns in SCHEDULE))
    def _(n):
        @pl.when(n < nreq)
        def _():
            attend(n)

        @pl.when(n == CHUNK)
        def _():
            for c in weight_copies() + resid_copies():
                c.start()

        @pl.when(n == CHUNK + 1)
        def _():
            for c in chunk_copies(EARLY_CHUNKS) + [query_weight]:
                c.start()

        for name, lowest, turns in SCHEDULE:
            @pl.when(functools.reduce(jnp.logical_or, [n == t for t in turns]))
            def _():
                work[name](sum([jnp.where(n > t, 1, 0) for t in turns]) + lowest)

    @pl.loop(0, chunks)
    def _(k):
        remote(msg.at[k, 0], rpart.at[k, 0], k, 0, partner).wait_send()
        remote(msg.at[k, 0], rpart.at[k, 1], k, 1, partner).wait_send()
        remote(xsend.at[k], xrecv.at[k], k, 2, across_x).wait_send()
        remote(psend.at[k], precv.at[k], k, 3, across_y).wait_send()
        for n in range(4, 13):
            gather_copy(k, n).wait_send()


def solution(mesh):
    cache_spec = P('dp', None, 'cp', 'tp')
    row_spec = P('dp')

    def local_step(hidden, attn_gain, w_query, w_key, w_value, w_out, cache_k, cache_v, ctx_len, positions, tree_mask):
        nreq, tree, width = hidden.shape
        num_blocks, kv_heads, blk, hd = cache_k.shape[1], cache_k.shape[3], cache_k.shape[4], cache_k.shape[5]
        qdim, kvdim = w_query.shape[1], w_key.shape[1]
        group = qdim // kvdim
        chunks = nreq // CHUNK
        keys = jnp.swapaxes(cache_k[:, :, 0], -1, -2)
        values = jnp.swapaxes(cache_v[:, :, 0], -1, -2)
        hbm = pl.BlockSpec(memory_space=pl.ANY)
        vmem = pl.BlockSpec(memory_space=pltpu.VMEM)
        smem = pl.BlockSpec(memory_space=pltpu.SMEM)
        cache_shape = jax.ShapeDtypeStruct(keys.shape, BF16)
        rows = CHUNK * tree
        qcols = group * tree
        rows_msg = kv_heads * hd + 2 * kv_heads
        ext = hd + tree + 16
        late_blocks = num_blocks - num_blocks // 2
        query, tables, first_msgs, new_keys, new_vals = pl.pallas_call(
            cache_kernel,
            in_specs=[smem] + [vmem] * 4 + [hbm] * 6,
            out_specs=[vmem, vmem, hbm, hbm, hbm],
            out_shape=[jax.ShapeDtypeStruct((EARLY_CHUNKS, CHUNK, kv_heads, hd, qcols), BF16), jax.ShapeDtypeStruct((chunks, 2, hd // 2, rows), F32),
                       jax.ShapeDtypeStruct((CHUNK, rows_msg, qcols), F32), cache_shape, cache_shape],
            scratch_shapes=[
                pltpu.VMEM((chunks, 2, CHUNK, num_blocks, kv_heads, hd, blk), BF16),
                pltpu.VMEM((chunks, CHUNK, tree, width), BF16),
                pltpu.VMEM((2, kvdim, rows), BF16),
                pltpu.VMEM((width, kvdim), BF16),
                pltpu.VMEM((width, kvdim), BF16),
                pltpu.VMEM((width, qdim), BF16),
                pltpu.VMEM((num_blocks, kv_heads, hd + 16, blk), BF16),
                pltpu.VMEM((late_blocks, kv_heads, ext, blk), BF16),
                pltpu.VMEM((kv_heads, ext, qcols), BF16),
                pltpu.VMEM((2, num_blocks * blk, qcols), F32),
                pltpu.VMEM((CHUNK, rows_msg, qcols), F32),
                pltpu.SemaphoreType.DMA((chunks, 3)),
                pltpu.SemaphoreType.DMA((chunks, 2)),
                pltpu.SemaphoreType.DMA((3,)),
                pltpu.SemaphoreType.DMA((CHUNK,)),
            ],
            compiler_params=pltpu.CompilerParams(vmem_limit_bytes=62 * 2**20),
            name='fill_caches',
        )(ctx_len, attn_gain, positions, jnp.asarray(rope_frequencies(hd)), tree_mask, w_key, w_value, w_query, hidden, keys, values)
        wide_rows = (chunks, tree, width // 2)
        out_hidden = pl.pallas_call(
            attend_kernel,
            in_specs=[smem, vmem] + [hbm] * 9,
            out_specs=vmem,
            out_shape=pltpu.VMEM((nreq, tree, width), BF16),
            scratch_shapes=[
                pltpu.VMEM((nreq, 2, tree, width // 2), F32),
                pltpu.VMEM((2, num_blocks, kv_heads, hd, blk), BF16),
                pltpu.VMEM((2, num_blocks, kv_heads, hd + 16, blk), BF16),
                pltpu.VMEM((late_blocks, kv_heads, ext, blk), BF16),
                pltpu.VMEM((kv_heads, ext, qcols), BF16),
                pltpu.VMEM((2, tree, tree), jnp.int32),
                pltpu.VMEM((2, num_blocks * blk, qcols), F32),
                pltpu.VMEM((chunks, CHUNK, rows_msg, qcols), F32),
                pltpu.VMEM((chunks, 2, rows_msg, qcols), F32),
                pltpu.VMEM((chunks, rows_msg, qcols), F32),
                pltpu.VMEM((chunks, rows_msg, qcols), F32),
                pltpu.VMEM(wide_rows, F32),
                pltpu.VMEM(wide_rows, F32),
                pltpu.VMEM((group, kv_heads * hd, width), BF16),
                pltpu.VMEM(wide_rows, BF16),
                pltpu.VMEM((width, qdim), BF16),
                pltpu.VMEM((CHUNK, tree, width), BF16),
                pltpu.VMEM((1, 2, hd // 2, rows), F32),
                pltpu.VMEM((EARLY_CHUNKS, CHUNK, kv_heads, hd, qcols), BF16),
                pltpu.SemaphoreType.DMA((2, 3)),
                pltpu.SemaphoreType.DMA((group, kv_heads)),
                pltpu.SemaphoreType.DMA((chunks,)),
                pltpu.SemaphoreType.DMA((5,)),
                pltpu.SemaphoreType.DMA((chunks, 13)),
                pltpu.SemaphoreType.DMA((chunks, 13)),
            ],
            compiler_params=pltpu.CompilerParams(collective_id=0, has_side_effects=True, vmem_limit_bytes=56 * 2**20),
            name='attend_and_combine',
        )(ctx_len, attn_gain, query, tables, first_msgs, tree_mask, new_keys, new_vals, hidden, w_query, w_out)
        return (out_hidden, jnp.swapaxes(new_keys, -1, -2)[:, :, None], jnp.swapaxes(new_vals, -1, -2)[:, :, None])

    return jax.shard_map(local_step, mesh=mesh, in_specs=(row_spec, P(), P(None, 'tp'), P(None, 'tp'), P(None, 'tp'), P('tp', None), cache_spec, cache_spec, row_spec, row_spec, row_spec), out_specs=(row_spec, cache_spec, cache_spec), check_vma=False)
```

```python
import functools
import math
import jax
import jax.numpy as jnp
import numpy as np
from jax import lax
from jax.experimental import pallas as pl
from jax.experimental.pallas import tpu as pltpu
from jax.sharding import PartitionSpec as P

ROPE_THETA = 500000.0
NORM_EPS = 1e-5
MASKED = -1e30
LOG2E = math.log2(math.e)
MESH = pl.DeviceIdType.MESH
F32 = jnp.float32
BF16 = jnp.bfloat16
CHUNK = 4

SCHEDULE = (
    ('finish', 0, (7, 14, 17, 25, 26, 27)),
    ('query', 2, (3, 7, 11, 15)),
    ('forward', 0, (11, 22, 23, 27, 28, 29)),
    ('merge', 1, (3, 6, 10, 15, 18)),
    ('project', 0, (3, 7, 11, 15, 20, 24)),
    ('diagonal', 0, (18, 25, 26, 29, 31, 32)),
    ('emit', 0, (23, 28, 29, 30, 32, 33)),
)

def mm(a, b):
    return jnp.dot(a, b, preferred_element_type=F32)


def mm_tn(a, b):
    return lax.dot_general(a, b, (((0,), (0,)), ((), ())), preferred_element_type=F32)


def rope_frequencies(head_dim):
    freq_idx = np.arange(head_dim // 2, dtype=np.float32)
    inv_freq = np.float32(1.0) / (np.float32(ROPE_THETA) ** (np.float32(2.0) * freq_idx / np.float32(head_dim)))
    wavelen = np.float32(2.0 * math.pi) / inv_freq
    smooth = (np.float32(8192.0) / wavelen - np.float32(1.0)) / np.float32(3.0)
    blended = (np.float32(1.0) - smooth) * inv_freq / np.float32(8.0) + smooth * inv_freq
    return np.where(wavelen < 2048.0, inv_freq, np.where(wavelen > 8192.0, inv_freq / np.float32(8.0), blended)).astype(np.float32)


def cos_sin(angle):
    turns = jnp.floor(angle * (2.0 / math.pi) + 0.5)
    r = ((angle - turns * 1.5703125) - turns * 4.837512969970703125e-4) - turns * 7.549789954891882e-8
    z = r * r
    sin_r = r + r * z * (-1.6666654611e-1 + z * (8.3321608736e-3 + z * -1.9515295891e-4))
    cos_r = 1.0 - 0.5 * z + z * z * (4.166664568298827e-2 + z * (-1.388731625493765e-3 + z * 2.443315711809948e-5))
    quarter = turns.astype(jnp.int32) & 3
    odd = (quarter & 1) == 1
    cos, sin = jnp.where(odd, sin_r, cos_r), jnp.where(odd, cos_r, sin_r)
    return jnp.where((quarter == 1) | (quarter == 2), -cos, cos), jnp.where(quarter >= 2, -sin, sin)


def normed_rows(x, gain):
    wide = x.astype(F32)
    inv_rms = lax.rsqrt(jnp.mean(wide * wide, axis=-1, keepdims=True) + NORM_EPS)
    return (wide * inv_rms * gain.astype(F32)[None, :]).astype(BF16)


def rotate(rows, cos, sin):
    half = rows.shape[0] // 2
    first, second = rows[:half], rows[half:]
    return jnp.concatenate([first * cos - second * sin, second * cos + first * sin], axis=0)


def project_queries(h, wq_ref, cos, sin, out, hd, group, tree):
    reqs = h.shape[0] // tree
    for head in range(wq_ref.shape[1] // (group * hd)):
        q_t = mm(h, wq_ref[:, head * group * hd:(head + 1) * group * hd]).T
        parts = [rotate(q_t[g * hd:(g + 1) * hd], cos, sin) for g in range(group)]
        for i in range(reqs):
            out(i, head, jnp.concatenate([p[:, i * tree:(i + 1) * tree] for p in parts], axis=1).astype(BF16))


def prepare(vref, qext, hd, tree):
    num_blocks, heads, vrows, blk = vref.shape
    ones = jnp.ones((vrows - hd, blk), BF16)
    pad = qext.shape[1] - hd - tree
    hide = jnp.where(lax.broadcasted_iota(jnp.int32, (pad, qext.shape[2]), 0) == 0, MASKED, 0.0).astype(BF16)
    for h in range(heads):
        for j in range(num_blocks):
            vref[j, h, hd:, :] = ones
        qext[h, hd + tree:, :] = hide


def attention(ctx, tree_mask, qref, kref, vref, kext, qext, scores, out, cp):
    num_blocks, heads, hd, blk = kref.shape
    qcols, tree = qext.shape[2], tree_mask.shape[0]
    pad = qext.shape[1] - hd - tree
    late = num_blocks // 2
    coef = hd ** -0.5 * LOG2E
    seen = jnp.concatenate([tree_mask.astype(F32)] * (qcols // tree), axis=0).T
    bias = jnp.where(seen > 0.0, 0.0, MASKED).astype(BF16)
    for h in range(heads):
        qext[h, :hd, :] = qref[h]
        qext[h, hd:hd + tree, :] = bias
    for j in range(late, num_blocks):
        off = (j * 4 + cp) * blk - ctx
        tok = off + lax.broadcasted_iota(jnp.int32, (tree, blk), 1)
        pick = jnp.where(tok == lax.broadcasted_iota(jnp.int32, (tree, blk), 0), 1.0, 0.0).astype(BF16)
        tok_p = off + lax.broadcasted_iota(jnp.int32, (pad, blk), 1)
        tail = jnp.where((tok_p >= tree) & (lax.broadcasted_iota(jnp.int32, (pad, blk), 0) == 0), 1.0, 0.0).astype(BF16)
        tok_h = off + lax.broadcasted_iota(jnp.int32, (hd, blk), 1)
        for h in range(heads):
            kext[j - late, h, :hd, :] = jnp.where(tok_h < tree, kref[j, h].astype(F32), 0.0).astype(BF16)
            kext[j - late, h, hd:hd + tree, :] = pick
            kext[j - late, h, hd + tree:, :] = tail

    def score(h, j):
        if j < late:
            s = mm_tn(kref[j, h], qext[h, :hd, :])
        else:
            s = mm_tn(kext[j - late, h], qext[h])
        scores[h % 2, j * blk:(j + 1) * blk, :] = s
        return jnp.max(s.reshape(blk // 8, 8, qcols), axis=0)

    tops = [None] * heads
    tops[0] = functools.reduce(jnp.maximum, [score(0, j) for j in range(num_blocks)])
    for h in range(heads):
        top = jnp.max(tops[h], axis=0, keepdims=True)
        shift = top * coef
        total, nxt = None, []
        for j in range(num_blocks):
            if h + 1 < heads:
                nxt.append(score(h + 1, j))
            p = jnp.exp2(scores[h % 2, j * blk:(j + 1) * blk, :] * coef - shift).astype(BF16)
            o = mm(vref[j, h], p)
            total = o if total is None else total + o
        if h + 1 < heads:
            tops[h + 1] = functools.reduce(jnp.maximum, nxt)
        out[h * hd:(h + 1) * hd, :] = total[:hd]
        out[heads * hd + h:heads * hd + h + 1, :] = top
        out[heads * hd + heads + h:heads * hd + heads + h + 1, :] = total[hd:hd + 1]


def cache_kernel(ctx_ref, gain_ref, pos_ref, freq_ref, mask_ref, wk_hbm, wv_hbm, wq_hbm, x_hbm, kc_hbm, vc_hbm,
                 q_ref, tab_ref, msg_hbm, ko_hbm, vo_hbm,
                 buf, xbuf, new_ref, wk_ref, wv_ref, wq_ref, vbuf, kext, qext, scores, msg, in_sem, out_sem, w_sem, msg_sem):
    cp_rank, cp_size = lax.axis_index('cp'), lax.axis_size('cp')
    chunks, _, per, num_blocks, kv_heads, hd, blk = buf.shape
    tree = pos_ref.shape[1]
    group = q_ref.shape[3] // tree
    width = x_hbm.shape[2]
    half = hd // 2
    cols = per * tree

    def rows_of(c):
        return pl.ds(c * per, per)

    def fetch_rows(c):
        return pltpu.make_async_copy(x_hbm.at[rows_of(c)], xbuf.at[c], in_sem.at[c, 2])

    def fetch(c):
        return [pltpu.make_async_copy(src.at[rows_of(c)], buf.at[c, n], in_sem.at[c, n]) for n, src in enumerate((kc_hbm, vc_hbm))]

    def flush(c):
        return [pltpu.make_async_copy(buf.at[c, n], dst.at[rows_of(c)], out_sem.at[c, n]) for n, dst in enumerate((ko_hbm, vo_hbm))]

    kv_weights = [pltpu.make_async_copy(src, dst, w_sem.at[n]) for n, (src, dst) in enumerate(((wk_hbm, wk_ref), (wv_hbm, wv_ref)))]
    q_weight = pltpu.make_async_copy(wq_hbm, wq_ref, w_sem.at[2])
    for c in [fetch_rows(0)] + kv_weights:
        c.start()
    prepare(vbuf, qext, hd, tree)
    diag = lax.broadcasted_iota(jnp.int32, (half, half), 0) == lax.broadcasted_iota(jnp.int32, (half, half), 1)
    freq = jnp.sum(jnp.where(diag, freq_ref[...][None, :], 0.0), axis=1, keepdims=True)
    for c in kv_weights:
        c.wait()
    for c in fetch(0) + [q_weight]:
        c.start()

    @pl.loop(0, chunks)
    def _(k):
        fetch_rows(k).wait()
        h = normed_rows(xbuf[k].reshape(cols, width), gain_ref[...])
        pos = jnp.concatenate([pos_ref[pl.ds(k * per + i, 1), :] for i in range(per)], axis=1).astype(F32)
        cos, sin = cos_sin(pos * freq)

        tab_ref[k, 0] = cos
        tab_ref[k, 1] = sin
        key_t = mm(h, wk_ref[...]).T
        for n in range(kv_heads):
            new_ref[0, n * hd:(n + 1) * hd, :] = rotate(key_t[n * hd:(n + 1) * hd], cos, sin).astype(BF16)
        new_ref[1] = mm(h, wv_ref[...]).T.astype(BF16)
        for c in fetch(k):
            c.wait()
        for i in range(per):
            ctx = ctx_ref[k * per + i]
            for j in range(num_blocks // 2, num_blocks):
                first_pos = (j * cp_size + cp_rank) * blk

                @pl.when((first_pos < ctx + tree) & (first_pos + blk > ctx))
                def _():
                    tok = first_pos - ctx + lax.broadcasted_iota(jnp.int32, (cols, blk), 1)
                    row = lax.broadcasted_iota(jnp.int32, (cols, blk), 0) - i * tree
                    pick = jnp.where((row == tok) & (row >= 0) & (row < tree), 1.0, 0.0).astype(BF16)
                    tok_h = first_pos - ctx + lax.broadcasted_iota(jnp.int32, (hd, blk), 1)
                    fresh = (tok_h >= 0) & (tok_h < tree)
                    for n in range(2):
                        put = mm(new_ref[n], pick)
                        for head in range(kv_heads):
                            old = buf[k, n, i, j, head].astype(F32)
                            buf[k, n, i, j, head] = jnp.where(fresh, put[head * hd:(head + 1) * hd], old).astype(BF16)

        for c in flush(k):
            c.start()

        @pl.when(k == 0)
        def _():
            q_weight.wait()
            for n in range(1, chunks):
                for c in [fetch_rows(n)] + fetch(n):
                    c.start()

            def out(i, head, value):
                q_ref[i, head] = value

            project_queries(h, wq_ref, cos, sin, out, hd, group, tree)

            @pl.loop(0, per // 2)
            def _(i):
                req = (1 - cp_rank // 2) * (per // 2) + i
                for j in range(num_blocks):
                    for head in range(kv_heads):
                        vbuf[j, head, :hd, :] = buf[0, 1, req, j, head]
                attention(ctx_ref[req], mask_ref[req], q_ref.at[req], buf.at[0, 0, req], vbuf, kext, qext, scores, msg.at[i], cp_rank)
                pltpu.make_async_copy(msg.at[i], msg_hbm.at[i], msg_sem.at[i]).start()

    for i in range(per // 2):
        pltpu.make_async_copy(msg.at[i], msg_hbm.at[i], msg_sem.at[i]).wait()
    for n in range(chunks):
        for c in flush(n):
            c.wait()


def attend_kernel(ctx_ref, gain_ref, q_hbm, tab_hbm, msg_hbm, mask_hbm, kc_hbm, vc_hbm, hid_hbm, wq_hbm, wo_hbm, out_ref,
                  y_ref, kbuf, vbuf, kext, qext, mbuf, scores, msg, rpart, xsend, xrecv, psend, precv, wout, resid, wq_ref, xbuf, tbuf, qbuf,
                  kv_sem, w_sem, hid_sem, q_sem, snd, rcv):
    cp, tp = lax.axis_index('cp'), lax.axis_index('tp')
    chip, core = cp // 2, cp % 2
    partner = {'cp': chip * 2 + 1 - core}
    across_x = {'cp': (1 - chip) * 2 + core}
    across_y = {'tp': 1 - tp}
    _, heads, hd, qcols = q_hbm.shape
    nreq = mask_hbm.shape[0]
    tree = mask_hbm.shape[1]
    group = qcols // tree
    num_blocks, blk = kbuf.shape[1], kbuf.shape[4]
    chunks = nreq // CHUNK
    width = wo_hbm.shape[1]
    wcols = width // 2
    coef = hd ** -0.5 * LOG2E
    own_cols = pl.ds(pl.multiple_of(tp * wcols, wcols), wcols)
    other_cols = pl.ds(pl.multiple_of((1 - tp) * wcols, wcols), wcols)

    def remote(src, dst, k, n, to):
        return pltpu.make_async_remote_copy(src_ref=src, dst_ref=dst, send_sem=snd.at[k, n], recv_sem=rcv.at[k, n], device_id=to, device_id_type=MESH)

    barrier = pltpu.get_barrier_semaphore()
    for to in (partner, across_x, across_y):
        pl.semaphore_signal(barrier, inc=1, device_id=to, device_id_type=MESH)

    turns = nreq - CHUNK // 2

    def turn_of(n):
        pair = n // 2
        foreign = jnp.where((pair % 2 == 0) & (n < turns - 2), 1, 0)
        return pair // 2 + foreign, 2 * (chip + foreign - 2 * chip * foreign) + n % 2, foreign

    def fetch(n):
        k, i, _ = turn_of(n)
        r, to = k * CHUNK + i, n % 2
        return [pltpu.make_async_copy(kc_hbm.at[r], kbuf.at[to], kv_sem.at[to, 0]),
                pltpu.make_async_copy(vc_hbm.at[r], vbuf.at[to, :, :, pl.ds(0, hd), :], kv_sem.at[to, 1]),
                pltpu.make_async_copy(mask_hbm.at[r], mbuf.at[to], kv_sem.at[to, 2])]

    def weight_copies():
        out = []
        for g in range(group):
            for h in range(heads):
                out.append(pltpu.make_async_copy(wo_hbm.at[pl.ds((h * group + g) * hd, hd)], wout.at[g, pl.ds(h * hd, hd)], w_sem.at[g, h]))
        return out

    def resid_copies():
        return [pltpu.make_async_copy(hid_hbm.at[k * CHUNK + cp, :, own_cols], resid.at[k], hid_sem.at[k]) for k in range(chunks)]

    first_queries = pltpu.make_async_copy(q_hbm, qbuf.at[0], q_sem.at[0])
    query_weight = pltpu.make_async_copy(wq_hbm, wq_ref, q_sem.at[1])

    def chunk_copies(k):
        pairs = tbuf.shape[0]
        return [pltpu.make_async_copy(hid_hbm.at[pl.ds(k * CHUNK, CHUNK)], xbuf, q_sem.at[2]),
                pltpu.make_async_copy(tab_hbm.at[pl.ds(k * pairs, pairs)], tbuf, q_sem.at[3])]

    first_msgs = pltpu.make_async_copy(msg_hbm, msg.at[0, pl.ds(2 * (1 - chip), 2)], q_sem.at[4])
    for c in [first_msgs] + chunk_copies(1) + [query_weight] + fetch(0) + [first_queries]:
        c.start()
    for to in range(2):
        prepare(vbuf.at[to], qext, hd, tree)
    pl.semaphore_wait(barrier, 3)
    first_msgs.wait()

    def share(k, i, which):
        @pl.when(i % 2 != core)
        def _():
            remote(msg.at[k, i], rpart.at[k, which], k, which, partner).start()

    for n in range(2):
        share(0, 2 * (1 - chip) + n, 0)

    def queries(k):
        for c in chunk_copies(k):
            c.wait()

        @pl.when(k == 1)
        def _():
            query_weight.wait()

        h = normed_rows(xbuf[...].reshape(CHUNK * tree, width), gain_ref[...])
        cos = jnp.concatenate([tbuf[p, 0] for p in range(tbuf.shape[0])], axis=1)
        sin = jnp.concatenate([tbuf[p, 1] for p in range(tbuf.shape[0])], axis=1)

        def out(i, head, value):
            qbuf[k % 2, i, head] = value

        project_queries(h, wq_ref, cos, sin, out, hd, group, tree)

        @pl.when(k + 1 < chunks)
        def _():
            for c in chunk_copies(k + 1):
                c.start()

    def attend(n):
        k, i, foreign = turn_of(n)
        r, slot = k * CHUNK + i, n % 2

        @pl.when(n + 1 < turns)
        def _():
            for c in fetch(n + 1):
                c.start()

        ctx = ctx_ref[r]
        for c in fetch(n):
            c.wait()
        attention(ctx, mbuf[slot], qbuf.at[k % 2, i], kbuf.at[slot], vbuf.at[slot], kext, qext, scores, msg.at[k, i], cp)

        share(k, i, 1 - foreign)

    stat = heads * hd

    def scales(parts, h):
        tops = [p[stat + h:stat + h + 1, :] for p in parts]
        top = functools.reduce(jnp.maximum, tops)
        return top, [jnp.exp2((t - top) * coef) for t in tops]

    def merge_chip(k):
        remote(msg.at[k, 0], rpart.at[k, 0], k, 0, partner).wait_recv()
        parts = [msg.at[k, 2 * (1 - chip) + core], rpart.at[k, 0]]
        for h in range(heads):
            top, fac = scales(parts, h)
            rows = slice(h * hd, (h + 1) * hd)
            xsend[k, rows, :] = sum(p[rows, :] * f for p, f in zip(parts, fac))
            xsend[k, stat + h:stat + h + 1, :] = top
            srow = slice(stat + heads + h, stat + heads + h + 1)
            xsend[k, srow, :] = sum(p[srow, :] * f for p, f in zip(parts, fac))
        remote(xsend.at[k], xrecv.at[k], k, 2, across_x).start()

    def project(k):
        remote(msg.at[k, 0], rpart.at[k, 1], k, 1, partner).wait_recv()
        remote(xsend.at[k], xrecv.at[k], k, 2, across_x).wait_recv()
        parts = [msg.at[k, cp], rpart.at[k, 1], xrecv.at[k]]
        outs = []
        for h in range(heads):
            _, fac = scales(parts, h)
            rows = slice(h * hd, (h + 1) * hd)
            srow = slice(stat + heads + h, stat + heads + h + 1)
            inv = 1.0 / sum(p[srow, :] * f for p, f in zip(parts, fac))
            outs.append(sum(p[rows, :] * (f * inv) for p, f in zip(parts, fac)))
        attn = jnp.concatenate(outs, axis=0).T.astype(BF16)

        @pl.when(k == 0)
        def _():
            for c in weight_copies() + resid_copies():
                c.wait()

        def part(cols):
            acc = None
            for g in range(group):
                d = mm(attn[g * tree:(g + 1) * tree], wout[g, :, cols])
                acc = d if acc is None else acc + d
            return acc.astype(BF16).astype(F32)

        psend[k] = part(other_cols)
        remote(psend.at[k], precv.at[k], k, 3, across_y).start()
        y_ref[k * CHUNK + cp, tp] = resid[k].astype(F32) + part(own_cols)

    def piece(k, owner_cp, owner_tp, lo=0, n=None):
        rows = pl.ds(lo, tree if n is None else n)
        return y_ref.at[k * CHUNK + owner_cp, owner_tp, rows]

    hf = (tree * 3 // 8) // 8 * 8
    hb = tree - hf
    pcp, xcp, dcp = chip * 2 + 1 - core, (1 - chip) * 2 + core, (1 - chip) * 2 + 1 - core

    def gather_copy(k, n):
        if n == 4:
            return remote(piece(k, cp, tp), piece(k, cp, tp), k, n, across_x)
        if n == 5:
            return remote(piece(k, cp, tp), piece(k, cp, tp), k, n, across_y)
        if n == 6:
            return remote(piece(k, cp, tp), piece(k, cp, tp), k, n, partner)
        if n == 7:
            return remote(piece(k, xcp, tp, 0, hf), piece(k, xcp, tp, 0, hf), k, n, across_y)
        if n == 8:
            return remote(piece(k, xcp, tp), piece(k, xcp, tp), k, n, partner)
        if n == 9:
            return remote(piece(k, cp, 1 - tp, hf, hb), piece(k, cp, 1 - tp, hf, hb), k, n, across_x)
        if n == 10:
            return remote(piece(k, cp, 1 - tp), piece(k, cp, 1 - tp), k, n, partner)
        if n == 11:
            return remote(piece(k, xcp, 1 - tp, 0, hf), piece(k, xcp, 1 - tp, 0, hf), k, n, partner)
        return remote(piece(k, xcp, 1 - tp, hf, hb), piece(k, xcp, 1 - tp, hf, hb), k, n, partner)

    def landed(k, n):
        src = {4: (xcp, tp, 0, tree), 5: (cp, 1 - tp, 0, tree), 6: (pcp, tp, 0, tree), 7: (xcp, 1 - tp, 0, hf), 8: (dcp, tp, 0, tree),
               9: (xcp, 1 - tp, hf, hb), 10: (pcp, 1 - tp, 0, tree), 11: (dcp, 1 - tp, 0, hf), 12: (dcp, 1 - tp, hf, hb)}[n]
        ref = piece(k, *src)
        remote(ref, ref, k, n, partner).wait_recv()

    def finish(k):
        remote(psend.at[k], precv.at[k], k, 3, across_y).wait_recv()
        total = y_ref[k * CHUNK + cp, tp] + precv[k]
        y_ref[k * CHUNK + cp, tp] = total.astype(BF16).astype(F32)
        for n in (4, 5, 6):
            gather_copy(k, n).start()

    def forward(k):
        landed(k, 4)
        gather_copy(k, 7).start()
        gather_copy(k, 8).start()
        landed(k, 5)
        gather_copy(k, 9).start()
        gather_copy(k, 10).start()

    def forward_diagonal(k):
        landed(k, 7)
        gather_copy(k, 11).start()
        landed(k, 9)
        gather_copy(k, 12).start()

    def emit(k):
        for n in (6, 8, 10, 11, 12):
            landed(k, n)
        for i in range(CHUNK):
            for side in range(2):
                out_ref[k * CHUNK + i, :, side * wcols:(side + 1) * wcols] = y_ref[k * CHUNK + i, side].astype(BF16)

    work = {'merge': merge_chip, 'query': queries, 'project': project, 'finish': finish, 'forward': forward, 'diagonal': forward_diagonal, 'emit': emit}

    merge_chip(0)
    queries(1)
    first_queries.wait()

    @pl.loop(0, 1 + max(max(when) for _, _, when in SCHEDULE))
    def _(n):
        @pl.when(n < turns)
        def _():
            attend(n)

        @pl.when(n == 0)
        def _():
            for c in weight_copies() + resid_copies():
                c.start()

        for name, lowest, when in SCHEDULE:
            @pl.when(functools.reduce(jnp.logical_or, [n == t for t in when]))
            def _():
                work[name](sum([jnp.where(n > t, 1, 0) for t in when]) + lowest)

    @pl.loop(0, chunks)
    def _(k):
        remote(msg.at[k, 0], rpart.at[k, 0], k, 0, partner).wait_send()
        remote(msg.at[k, 0], rpart.at[k, 1], k, 1, partner).wait_send()
        remote(xsend.at[k], xrecv.at[k], k, 2, across_x).wait_send()
        remote(psend.at[k], precv.at[k], k, 3, across_y).wait_send()
        for n in range(4, 13):
            gather_copy(k, n).wait_send()


def solution(mesh):
    cache_spec = P('dp', None, 'cp', 'tp')
    row_spec = P('dp')

    def local_step(hidden, attn_gain, w_query, w_key, w_value, w_out, cache_k, cache_v, ctx_len, positions, tree_mask):
        nreq, tree, width = hidden.shape
        num_blocks, kv_heads, blk, hd = cache_k.shape[1], cache_k.shape[3], cache_k.shape[4], cache_k.shape[5]
        qdim, kvdim = w_query.shape[1], w_key.shape[1]
        group = qdim // kvdim
        chunks = nreq // CHUNK
        keys = jnp.swapaxes(cache_k[:, :, 0], -1, -2)
        values = jnp.swapaxes(cache_v[:, :, 0], -1, -2)
        hbm = pl.BlockSpec(memory_space=pl.ANY)
        vmem = pl.BlockSpec(memory_space=pltpu.VMEM)
        smem = pl.BlockSpec(memory_space=pltpu.SMEM)
        cache_shape = jax.ShapeDtypeStruct(keys.shape, BF16)
        rows = CHUNK * tree
        qcols = group * tree
        rows_msg = kv_heads * hd + 2 * kv_heads
        ext = hd + tree + 16
        late_blocks = num_blocks - num_blocks // 2
        query, tables, first_msgs, new_keys, new_vals = pl.pallas_call(
            cache_kernel,
            in_specs=[smem] + [vmem] * 4 + [hbm] * 6,
            out_specs=[vmem, vmem, hbm, hbm, hbm],
            out_shape=[jax.ShapeDtypeStruct((CHUNK, kv_heads, hd, qcols), BF16), jax.ShapeDtypeStruct((chunks, 2, hd // 2, rows), F32),
                       jax.ShapeDtypeStruct((CHUNK // 2, rows_msg, qcols), F32), cache_shape, cache_shape],
            scratch_shapes=[
                pltpu.VMEM((chunks, 2, CHUNK, num_blocks, kv_heads, hd, blk), BF16),
                pltpu.VMEM((chunks, CHUNK, tree, width), BF16),
                pltpu.VMEM((2, kvdim, rows), BF16),
                pltpu.VMEM((width, kvdim), BF16),
                pltpu.VMEM((width, kvdim), BF16),
                pltpu.VMEM((width, qdim), BF16),
                pltpu.VMEM((num_blocks, kv_heads, hd + 16, blk), BF16),
                pltpu.VMEM((late_blocks, kv_heads, ext, blk), BF16),
                pltpu.VMEM((kv_heads, ext, qcols), BF16),
                pltpu.VMEM((2, num_blocks * blk, qcols), F32),
                pltpu.VMEM((CHUNK // 2, rows_msg, qcols), F32),
                pltpu.SemaphoreType.DMA((chunks, 3)),
                pltpu.SemaphoreType.DMA((chunks, 2)),
                pltpu.SemaphoreType.DMA((3,)),
                pltpu.SemaphoreType.DMA((CHUNK // 2,)),
            ],
            compiler_params=pltpu.CompilerParams(vmem_limit_bytes=62 * 2**20),
            name='fill_caches',
        )(ctx_len, attn_gain, positions, jnp.asarray(rope_frequencies(hd)), tree_mask, w_key, w_value, w_query, hidden, keys, values)
        wide_rows = (chunks, tree, width // 2)
        out_hidden = pl.pallas_call(
            attend_kernel,
            in_specs=[smem, vmem] + [hbm] * 9,
            out_specs=vmem,
            out_shape=pltpu.VMEM((nreq, tree, width), BF16),
            scratch_shapes=[
                pltpu.VMEM((nreq, 2, tree, width // 2), F32),
                pltpu.VMEM((2, num_blocks, kv_heads, hd, blk), BF16),
                pltpu.VMEM((2, num_blocks, kv_heads, hd + 16, blk), BF16),
                pltpu.VMEM((late_blocks, kv_heads, ext, blk), BF16),
                pltpu.VMEM((kv_heads, ext, qcols), BF16),
                pltpu.VMEM((2, tree, tree), jnp.int32),
                pltpu.VMEM((2, num_blocks * blk, qcols), F32),
                pltpu.VMEM((chunks, CHUNK, rows_msg, qcols), F32),
                pltpu.VMEM((chunks, 2, rows_msg, qcols), F32),
                pltpu.VMEM((chunks, rows_msg, qcols), F32),
                pltpu.VMEM((chunks, rows_msg, qcols), F32),
                pltpu.VMEM(wide_rows, F32),
                pltpu.VMEM(wide_rows, F32),
                pltpu.VMEM((group, kv_heads * hd, width), BF16),
                pltpu.VMEM(wide_rows, BF16),
                pltpu.VMEM((width, qdim), BF16),
                pltpu.VMEM((CHUNK, tree, width), BF16),
                pltpu.VMEM((1, 2, hd // 2, rows), F32),
                pltpu.VMEM((2, CHUNK, kv_heads, hd, qcols), BF16),
                pltpu.SemaphoreType.DMA((2, 3)),
                pltpu.SemaphoreType.DMA((group, kv_heads)),
                pltpu.SemaphoreType.DMA((chunks,)),
                pltpu.SemaphoreType.DMA((5,)),
                pltpu.SemaphoreType.DMA((chunks, 13)),
                pltpu.SemaphoreType.DMA((chunks, 13)),
            ],
            compiler_params=pltpu.CompilerParams(collective_id=0, has_side_effects=True, vmem_limit_bytes=56 * 2**20),
            name='attend_and_combine',
        )(ctx_len, attn_gain, query, tables, first_msgs, tree_mask, new_keys, new_vals, hidden, w_query, w_out)
        return (out_hidden, jnp.swapaxes(new_keys, -1, -2)[:, :, None], jnp.swapaxes(new_vals, -1, -2)[:, :, None])

    return jax.shard_map(local_step, mesh=mesh, in_specs=(row_spec, P(), P(None, 'tp'), P(None, 'tp'), P(None, 'tp'), P('tp', None), cache_spec, cache_spec, row_spec, row_spec, row_spec), out_specs=(row_spec, cache_spec, cache_spec), check_vma=False)
```

```python
import functools
import math
import jax
import jax.numpy as jnp
import numpy as np
from jax import lax
from jax.experimental import pallas as pl
from jax.experimental.pallas import tpu as pltpu
from jax.sharding import PartitionSpec as P

ROPE_THETA = 500000.0
NORM_EPS = 1e-5
MASKED = -1e30
LOG2E = math.log2(math.e)
MESH = pl.DeviceIdType.MESH
F32 = jnp.float32
BF16 = jnp.bfloat16
CHUNK = 4

SCHEDULE = (
    ('finish', 0, (7, 14, 17, 25, 26, 27)),
    ('query', 2, (3, 7, 11, 15)),
    ('forward', 0, (11, 22, 23, 27, 28, 29)),
    ('merge', 1, (3, 6, 10, 15, 18)),
    ('project', 0, (3, 7, 11, 15, 20, 24)),
    ('diagonal', 0, (18, 25, 26, 29, 31, 32)),
    ('emit', 0, (23, 28, 29, 30, 32, 33)),
)

def mm(a, b):
    return jnp.dot(a, b, preferred_element_type=F32)


def mm_tn(a, b):
    return lax.dot_general(a, b, (((0,), (0,)), ((), ())), preferred_element_type=F32)


def rope_frequencies(head_dim):
    freq_idx = np.arange(head_dim // 2, dtype=np.float32)
    inv_freq = np.float32(1.0) / (np.float32(ROPE_THETA) ** (np.float32(2.0) * freq_idx / np.float32(head_dim)))
    wavelen = np.float32(2.0 * math.pi) / inv_freq
    smooth = (np.float32(8192.0) / wavelen - np.float32(1.0)) / np.float32(3.0)
    blended = (np.float32(1.0) - smooth) * inv_freq / np.float32(8.0) + smooth * inv_freq
    return np.where(wavelen < 2048.0, inv_freq, np.where(wavelen > 8192.0, inv_freq / np.float32(8.0), blended)).astype(np.float32)


def cos_sin(angle):
    turns = jnp.floor(angle * (2.0 / math.pi) + 0.5)
    r = ((angle - turns * 1.5703125) - turns * 4.837512969970703125e-4) - turns * 7.549789954891882e-8
    z = r * r
    sin_r = r + r * z * (-1.6666654611e-1 + z * (8.3321608736e-3 + z * -1.9515295891e-4))
    cos_r = 1.0 - 0.5 * z + z * z * (4.166664568298827e-2 + z * (-1.388731625493765e-3 + z * 2.443315711809948e-5))
    quarter = turns.astype(jnp.int32) & 3
    odd = (quarter & 1) == 1
    cos, sin = jnp.where(odd, sin_r, cos_r), jnp.where(odd, cos_r, sin_r)
    return jnp.where((quarter == 1) | (quarter == 2), -cos, cos), jnp.where(quarter >= 2, -sin, sin)


def normed_rows(x, gain):
    wide = x.astype(F32)
    inv_rms = lax.rsqrt(jnp.mean(wide * wide, axis=-1, keepdims=True) + NORM_EPS)
    return (wide * inv_rms * gain.astype(F32)[None, :]).astype(BF16)


def rotate(rows, cos, sin):
    half = rows.shape[0] // 2
    first, second = rows[:half], rows[half:]
    return jnp.concatenate([first * cos - second * sin, second * cos + first * sin], axis=0)


def project_queries(h, wq_ref, cos, sin, out, hd, group, tree):
    reqs = h.shape[0] // tree
    for head in range(wq_ref.shape[1] // (group * hd)):
        q_t = mm(h, wq_ref[:, head * group * hd:(head + 1) * group * hd]).T
        parts = [rotate(q_t[g * hd:(g + 1) * hd], cos, sin) for g in range(group)]
        for i in range(reqs):
            out(i, head, jnp.concatenate([p[:, i * tree:(i + 1) * tree] for p in parts], axis=1).astype(BF16))


def prepare(vref, qext, hd, tree):
    num_blocks, heads, vrows, blk = vref.shape
    ones = jnp.ones((vrows - hd, blk), BF16)
    pad = qext.shape[1] - hd - tree
    hide = jnp.where(lax.broadcasted_iota(jnp.int32, (pad, qext.shape[2]), 0) == 0, MASKED, 0.0).astype(BF16)
    for h in range(heads):
        for j in range(num_blocks):
            vref[j, h, hd:, :] = ones
        qext[h, hd + tree:, :] = hide


def attention(ctx, tree_mask, qref, kref, vref, kext, qext, scores, out, cp):
    num_blocks, heads, hd, blk = kref.shape
    qcols, tree = qext.shape[2], tree_mask.shape[0]
    pad = qext.shape[1] - hd - tree
    late = num_blocks // 2
    coef = hd ** -0.5 * LOG2E
    seen = jnp.concatenate([tree_mask.astype(F32)] * (qcols // tree), axis=0).T
    bias = jnp.where(seen > 0.0, 0.0, MASKED).astype(BF16)
    for h in range(heads):
        qext[h, :hd, :] = qref[h]
        qext[h, hd:hd + tree, :] = bias
    for j in range(late, num_blocks):
        off = (j * 4 + cp) * blk - ctx
        tok = off + lax.broadcasted_iota(jnp.int32, (tree, blk), 1)
        pick = jnp.where(tok == lax.broadcasted_iota(jnp.int32, (tree, blk), 0), 1.0, 0.0).astype(BF16)
        tok_p = off + lax.broadcasted_iota(jnp.int32, (pad, blk), 1)
        tail = jnp.where((tok_p >= tree) & (lax.broadcasted_iota(jnp.int32, (pad, blk), 0) == 0), 1.0, 0.0).astype(BF16)
        tok_h = off + lax.broadcasted_iota(jnp.int32, (hd, blk), 1)
        for h in range(heads):
            kext[j - late, h, :hd, :] = jnp.where(tok_h < tree, kref[j, h].astype(F32), 0.0).astype(BF16)
            kext[j - late, h, hd:hd + tree, :] = pick
            kext[j - late, h, hd + tree:, :] = tail

    def score(h, j):
        if j < late:
            s = mm_tn(kref[j, h], qext[h, :hd, :])
        else:
            s = mm_tn(kext[j - late, h], qext[h])
        scores[h % 2, j * blk:(j + 1) * blk, :] = s
        return jnp.max(s.reshape(blk // 8, 8, qcols), axis=0)

    tops = [None] * heads
    tops[0] = functools.reduce(jnp.maximum, [score(0, j) for j in range(num_blocks)])
    for h in range(heads):
        top = jnp.max(tops[h], axis=0, keepdims=True)
        shift = top * coef
        total, nxt = None, []
        for j in range(num_blocks):
            if h + 1 < heads:
                nxt.append(score(h + 1, j))
            p = jnp.exp2(scores[h % 2, j * blk:(j + 1) * blk, :] * coef - shift).astype(BF16)
            o = mm(vref[j, h], p)
            total = o if total is None else total + o
        if h + 1 < heads:
            tops[h + 1] = functools.reduce(jnp.maximum, nxt)
        out[h * hd:(h + 1) * hd, :] = total[:hd]
        out[heads * hd + h:heads * hd + h + 1, :] = top
        out[heads * hd + heads + h:heads * hd + heads + h + 1, :] = total[hd:hd + 1]


def cache_kernel(ctx_ref, gain_ref, pos_ref, freq_ref, mask_ref, wk_hbm, wv_hbm, wq_hbm, x_hbm, kc_hbm, vc_hbm,
                 q_ref, tab_ref, msg_hbm, ko_hbm, vo_hbm,
                 buf, xbuf, new_ref, wk_ref, wv_ref, wq_ref, vbuf, kext, qext, scores, msg, in_sem, out_sem, w_sem, msg_sem):
    cp_rank, cp_size = lax.axis_index('cp'), lax.axis_size('cp')
    chunks, _, per, num_blocks, kv_heads, hd, blk = buf.shape
    tree = pos_ref.shape[1]
    group = q_ref.shape[3] // tree
    width = x_hbm.shape[2]
    half = hd // 2
    cols = per * tree

    def rows_of(c):
        return pl.ds(c * per, per)

    def fetch_rows(c):
        return pltpu.make_async_copy(x_hbm.at[rows_of(c)], xbuf.at[c], in_sem.at[c, 2])

    def fetch(c):
        return [pltpu.make_async_copy(src.at[rows_of(c)], buf.at[c, n], in_sem.at[c, n]) for n, src in enumerate((kc_hbm, vc_hbm))]

    def flush(c):
        return [pltpu.make_async_copy(buf.at[c, n], dst.at[rows_of(c)], out_sem.at[c, n]) for n, dst in enumerate((ko_hbm, vo_hbm))]

    kv_weights = [pltpu.make_async_copy(src, dst, w_sem.at[n]) for n, (src, dst) in enumerate(((wk_hbm, wk_ref), (wv_hbm, wv_ref)))]
    q_weight = pltpu.make_async_copy(wq_hbm, wq_ref, w_sem.at[2])
    for c in [fetch_rows(0)] + kv_weights:
        c.start()
    prepare(vbuf, qext, hd, tree)
    diag = lax.broadcasted_iota(jnp.int32, (half, half), 0) == lax.broadcasted_iota(jnp.int32, (half, half), 1)
    freq = jnp.sum(jnp.where(diag, freq_ref[...][None, :], 0.0), axis=1, keepdims=True)
    for c in kv_weights:
        c.wait()
    for c in fetch(0) + [q_weight]:
        c.start()

    @pl.loop(0, chunks)
    def _(k):
        fetch_rows(k).wait()
        h = normed_rows(xbuf[k].reshape(cols, width), gain_ref[...])
        pos = jnp.concatenate([pos_ref[pl.ds(k * per + i, 1), :] for i in range(per)], axis=1).astype(F32)
        cos, sin = cos_sin(pos * freq)

        tab_ref[k, 0] = cos
        tab_ref[k, 1] = sin
        key_t = mm(h, wk_ref[...]).T
        for n in range(kv_heads):
            new_ref[0, n * hd:(n + 1) * hd, :] = rotate(key_t[n * hd:(n + 1) * hd], cos, sin).astype(BF16)
        new_ref[1] = mm(h, wv_ref[...]).T.astype(BF16)
        for c in fetch(k):
            c.wait()
        for i in range(per):
            ctx = ctx_ref[k * per + i]
            for j in range(num_blocks // 2, num_blocks):
                first_pos = (j * cp_size + cp_rank) * blk

                @pl.when((first_pos < ctx + tree) & (first_pos + blk > ctx))
                def _():
                    tok = first_pos - ctx + lax.broadcasted_iota(jnp.int32, (cols, blk), 1)
                    row = lax.broadcasted_iota(jnp.int32, (cols, blk), 0) - i * tree
                    pick = jnp.where((row == tok) & (row >= 0) & (row < tree), 1.0, 0.0).astype(BF16)
                    tok_h = first_pos - ctx + lax.broadcasted_iota(jnp.int32, (hd, blk), 1)
                    fresh = (tok_h >= 0) & (tok_h < tree)
                    for n in range(2):
                        put = mm(new_ref[n], pick)
                        for head in range(kv_heads):
                            old = buf[k, n, i, j, head].astype(F32)
                            buf[k, n, i, j, head] = jnp.where(fresh, put[head * hd:(head + 1) * hd], old).astype(BF16)

        for c in flush(k):
            c.start()

        @pl.when(k == 0)
        def _():
            q_weight.wait()
            for n in range(1, chunks):
                for c in [fetch_rows(n)] + fetch(n):
                    c.start()

            def out(i, head, value):
                q_ref[i, head] = value

            project_queries(h, wq_ref, cos, sin, out, hd, group, tree)

            @pl.loop(0, per // 2)
            def _(i):
                req = (1 - cp_rank // 2) * (per // 2) + i
                for j in range(num_blocks):
                    for head in range(kv_heads):
                        vbuf[j, head, :hd, :] = buf[0, 1, req, j, head]
                attention(ctx_ref[req], mask_ref[req], q_ref.at[req], buf.at[0, 0, req], vbuf, kext, qext, scores, msg.at[i], cp_rank)
                pltpu.make_async_copy(msg.at[i], msg_hbm.at[i], msg_sem.at[i]).start()

    for i in range(per // 2):
        pltpu.make_async_copy(msg.at[i], msg_hbm.at[i], msg_sem.at[i]).wait()
    for n in range(chunks):
        for c in flush(n):
            c.wait()


def attend_kernel(ctx_ref, gain_ref, q_hbm, tab_hbm, msg_hbm, mask_hbm, kc_hbm, vc_hbm, hid_hbm, wq_hbm, wo_hbm, out_ref,
                  y_ref, kbuf, vbuf, kext, qext, mbuf, scores, msg, rpart, xsend, xrecv, psend, precv, wout, resid, wq_ref, xbuf, tbuf, qbuf,
                  kv_sem, w_sem, hid_sem, q_sem, snd, rcv):
    cp, tp = lax.axis_index('cp'), lax.axis_index('tp')
    chip, core = cp // 2, cp % 2
    partner = {'cp': chip * 2 + 1 - core}
    across_x = {'cp': (1 - chip) * 2 + core}
    across_y = {'tp': 1 - tp}
    _, heads, hd, qcols = q_hbm.shape
    nreq = mask_hbm.shape[0]
    tree = mask_hbm.shape[1]
    group = qcols // tree
    num_blocks, blk = kbuf.shape[1], kbuf.shape[4]
    chunks = nreq // CHUNK
    width = wo_hbm.shape[1]
    wcols = width // 2
    coef = hd ** -0.5 * LOG2E
    own_cols = pl.ds(pl.multiple_of(tp * wcols, wcols), wcols)
    other_cols = pl.ds(pl.multiple_of((1 - tp) * wcols, wcols), wcols)

    def remote(src, dst, k, n, to):
        return pltpu.make_async_remote_copy(src_ref=src, dst_ref=dst, send_sem=snd.at[k, n], recv_sem=rcv.at[k, n], device_id=to, device_id_type=MESH)

    barrier = pltpu.get_barrier_semaphore()
    for to in (partner, across_x, across_y):
        pl.semaphore_signal(barrier, inc=1, device_id=to, device_id_type=MESH)

    turns = nreq - CHUNK // 2

    def turn_of(n):
        pair = n // 2
        foreign = jnp.where((pair % 2 == 0) & (n < turns - 2), 1, 0)
        return pair // 2 + foreign, 2 * (chip + foreign - 2 * chip * foreign) + n % 2, foreign

    def fetch(n):
        k, i, _ = turn_of(n)
        r, to = k * CHUNK + i, n % 2
        return [pltpu.make_async_copy(kc_hbm.at[r], kbuf.at[to], kv_sem.at[to, 0]),
                pltpu.make_async_copy(vc_hbm.at[r], vbuf.at[to, :, :, pl.ds(0, hd), :], kv_sem.at[to, 1]),
                pltpu.make_async_copy(mask_hbm.at[r], mbuf.at[to], kv_sem.at[to, 2])]

    def weight_copies():
        out = []
        for g in range(group):
            for h in range(heads):
                out.append(pltpu.make_async_copy(wo_hbm.at[pl.ds((h * group + g) * hd, hd)], wout.at[g, pl.ds(h * hd, hd)], w_sem.at[g, h]))
        return out

    def resid_copies():
        return [pltpu.make_async_copy(hid_hbm.at[k * CHUNK + cp, :, own_cols], resid.at[k], hid_sem.at[k]) for k in range(chunks)]

    first_queries = pltpu.make_async_copy(q_hbm, qbuf.at[0], q_sem.at[0])
    query_weight = pltpu.make_async_copy(wq_hbm, wq_ref, q_sem.at[1])

    def chunk_copies(k):
        pairs = tbuf.shape[0]
        return [pltpu.make_async_copy(hid_hbm.at[pl.ds(k * CHUNK, CHUNK)], xbuf, q_sem.at[2]),
                pltpu.make_async_copy(tab_hbm.at[pl.ds(k * pairs, pairs)], tbuf, q_sem.at[3])]

    first_msgs = pltpu.make_async_copy(msg_hbm, msg.at[0, pl.ds(2 * (1 - chip), 2)], q_sem.at[4])
    first_msgs.start()
    for to in range(2):
        prepare(vbuf.at[to], qext, hd, tree)
    pl.semaphore_wait(barrier, 3)
    first_msgs.wait()

    def share(k, i, which):
        @pl.when(i % 2 != core)
        def _():
            remote(msg.at[k, i], rpart.at[k, which], k, which, partner).start()

    for n in range(2):
        share(0, 2 * (1 - chip) + n, 0)
    for c in chunk_copies(1) + [query_weight] + fetch(0) + [first_queries]:
        c.start()

    def queries(k):
        for c in chunk_copies(k):
            c.wait()

        @pl.when(k == 1)
        def _():
            query_weight.wait()

        h = normed_rows(xbuf[...].reshape(CHUNK * tree, width), gain_ref[...])
        cos = jnp.concatenate([tbuf[p, 0] for p in range(tbuf.shape[0])], axis=1)
        sin = jnp.concatenate([tbuf[p, 1] for p in range(tbuf.shape[0])], axis=1)

        def out(i, head, value):
            qbuf[k % 2, i, head] = value

        project_queries(h, wq_ref, cos, sin, out, hd, group, tree)

        @pl.when(k + 1 < chunks)
        def _():
            for c in chunk_copies(k + 1):
                c.start()

    def attend(n):
        k, i, foreign = turn_of(n)
        r, slot = k * CHUNK + i, n % 2

        @pl.when(n + 1 < turns)
        def _():
            for c in fetch(n + 1):
                c.start()

        ctx = ctx_ref[r]
        for c in fetch(n):
            c.wait()
        attention(ctx, mbuf[slot], qbuf.at[k % 2, i], kbuf.at[slot], vbuf.at[slot], kext, qext, scores, msg.at[k, i], cp)

        share(k, i, 1 - foreign)

    stat = heads * hd

    def scales(parts, h):
        tops = [p[stat + h:stat + h + 1, :] for p in parts]
        top = functools.reduce(jnp.maximum, tops)
        return top, [jnp.exp2((t - top) * coef) for t in tops]

    def merge_chip(k):
        remote(msg.at[k, 0], rpart.at[k, 0], k, 0, partner).wait_recv()
        parts = [msg.at[k, 2 * (1 - chip) + core], rpart.at[k, 0]]
        for h in range(heads):
            top, fac = scales(parts, h)
            rows = slice(h * hd, (h + 1) * hd)
            xsend[k, rows, :] = sum(p[rows, :] * f for p, f in zip(parts, fac))
            xsend[k, stat + h:stat + h + 1, :] = top
            srow = slice(stat + heads + h, stat + heads + h + 1)
            xsend[k, srow, :] = sum(p[srow, :] * f for p, f in zip(parts, fac))
        remote(xsend.at[k], xrecv.at[k], k, 2, across_x).start()

    def project(k):
        remote(msg.at[k, 0], rpart.at[k, 1], k, 1, partner).wait_recv()
        remote(xsend.at[k], xrecv.at[k], k, 2, across_x).wait_recv()
        parts = [msg.at[k, cp], rpart.at[k, 1], xrecv.at[k]]
        outs = []
        for h in range(heads):
            _, fac = scales(parts, h)
            rows = slice(h * hd, (h + 1) * hd)
            srow = slice(stat + heads + h, stat + heads + h + 1)
            inv = 1.0 / sum(p[srow, :] * f for p, f in zip(parts, fac))
            outs.append(sum(p[rows, :] * (f * inv) for p, f in zip(parts, fac)))
        attn = jnp.concatenate(outs, axis=0).T.astype(BF16)

        @pl.when(k == 0)
        def _():
            for c in weight_copies() + resid_copies():
                c.wait()

        def part(cols):
            acc = None
            for g in range(group):
                d = mm(attn[g * tree:(g + 1) * tree], wout[g, :, cols])
                acc = d if acc is None else acc + d
            return acc.astype(BF16).astype(F32)

        psend[k] = part(other_cols)
        remote(psend.at[k], precv.at[k], k, 3, across_y).start()
        y_ref[k * CHUNK + cp, tp] = resid[k].astype(F32) + part(own_cols)

    def piece(k, owner_cp, owner_tp, lo=0, n=None):
        rows = pl.ds(lo, tree if n is None else n)
        return y_ref.at[k * CHUNK + owner_cp, owner_tp, rows]

    hf = (tree * 3 // 8) // 8 * 8
    hb = tree - hf
    pcp, xcp, dcp = chip * 2 + 1 - core, (1 - chip) * 2 + core, (1 - chip) * 2 + 1 - core

    def gather_copy(k, n):
        if n == 4:
            return remote(piece(k, cp, tp), piece(k, cp, tp), k, n, across_x)
        if n == 5:
            return remote(piece(k, cp, tp), piece(k, cp, tp), k, n, across_y)
        if n == 6:
            return remote(piece(k, cp, tp), piece(k, cp, tp), k, n, partner)
        if n == 7:
            return remote(piece(k, xcp, tp, 0, hf), piece(k, xcp, tp, 0, hf), k, n, across_y)
        if n == 8:
            return remote(piece(k, xcp, tp), piece(k, xcp, tp), k, n, partner)
        if n == 9:
            return remote(piece(k, cp, 1 - tp, hf, hb), piece(k, cp, 1 - tp, hf, hb), k, n, across_x)
        if n == 10:
            return remote(piece(k, cp, 1 - tp), piece(k, cp, 1 - tp), k, n, partner)
        if n == 11:
            return remote(piece(k, xcp, 1 - tp, 0, hf), piece(k, xcp, 1 - tp, 0, hf), k, n, partner)
        return remote(piece(k, xcp, 1 - tp, hf, hb), piece(k, xcp, 1 - tp, hf, hb), k, n, partner)

    def landed(k, n):
        src = {4: (xcp, tp, 0, tree), 5: (cp, 1 - tp, 0, tree), 6: (pcp, tp, 0, tree), 7: (xcp, 1 - tp, 0, hf), 8: (dcp, tp, 0, tree),
               9: (xcp, 1 - tp, hf, hb), 10: (pcp, 1 - tp, 0, tree), 11: (dcp, 1 - tp, 0, hf), 12: (dcp, 1 - tp, hf, hb)}[n]
        ref = piece(k, *src)
        remote(ref, ref, k, n, partner).wait_recv()

    def finish(k):
        remote(psend.at[k], precv.at[k], k, 3, across_y).wait_recv()
        total = y_ref[k * CHUNK + cp, tp] + precv[k]
        y_ref[k * CHUNK + cp, tp] = total.astype(BF16).astype(F32)
        for n in (4, 5, 6):
            gather_copy(k, n).start()

    def forward(k):
        landed(k, 4)
        gather_copy(k, 7).start()
        gather_copy(k, 8).start()
        landed(k, 5)
        gather_copy(k, 9).start()
        gather_copy(k, 10).start()

    def forward_diagonal(k):
        landed(k, 7)
        gather_copy(k, 11).start()
        landed(k, 9)
        gather_copy(k, 12).start()

    def emit(k):
        for n in (6, 8, 10, 11, 12):
            landed(k, n)
        for i in range(CHUNK):
            for side in range(2):
                out_ref[k * CHUNK + i, :, side * wcols:(side + 1) * wcols] = y_ref[k * CHUNK + i, side].astype(BF16)

    work = {'merge': merge_chip, 'query': queries, 'project': project, 'finish': finish, 'forward': forward, 'diagonal': forward_diagonal, 'emit': emit}

    merge_chip(0)
    queries(1)
    first_queries.wait()

    @pl.loop(0, 1 + max(max(when) for _, _, when in SCHEDULE))
    def _(n):
        @pl.when(n < turns)
        def _():
            attend(n)

        @pl.when(n == 0)
        def _():
            for c in weight_copies() + resid_copies():
                c.start()

        for name, lowest, when in SCHEDULE:
            now = n + 1 - core if name == 'merge' else n

            @pl.when(functools.reduce(jnp.logical_or, [now == t for t in when]))
            def _():
                work[name](sum([jnp.where(now > t, 1, 0) for t in when]) + lowest)

    @pl.loop(0, chunks)
    def _(k):
        remote(msg.at[k, 0], rpart.at[k, 0], k, 0, partner).wait_send()
        remote(msg.at[k, 0], rpart.at[k, 1], k, 1, partner).wait_send()
        remote(xsend.at[k], xrecv.at[k], k, 2, across_x).wait_send()
        remote(psend.at[k], precv.at[k], k, 3, across_y).wait_send()
        for n in range(4, 13):
            gather_copy(k, n).wait_send()


def solution(mesh):
    cache_spec = P('dp', None, 'cp', 'tp')
    row_spec = P('dp')

    def local_step(hidden, attn_gain, w_query, w_key, w_value, w_out, cache_k, cache_v, ctx_len, positions, tree_mask):
        nreq, tree, width = hidden.shape
        num_blocks, kv_heads, blk, hd = cache_k.shape[1], cache_k.shape[3], cache_k.shape[4], cache_k.shape[5]
        qdim, kvdim = w_query.shape[1], w_key.shape[1]
        group = qdim // kvdim
        chunks = nreq // CHUNK
        keys = jnp.swapaxes(cache_k[:, :, 0], -1, -2)
        values = jnp.swapaxes(cache_v[:, :, 0], -1, -2)
        hbm = pl.BlockSpec(memory_space=pl.ANY)
        vmem = pl.BlockSpec(memory_space=pltpu.VMEM)
        smem = pl.BlockSpec(memory_space=pltpu.SMEM)
        cache_shape = jax.ShapeDtypeStruct(keys.shape, BF16)
        rows = CHUNK * tree
        qcols = group * tree
        rows_msg = kv_heads * hd + 2 * kv_heads
        ext = hd + tree + 16
        late_blocks = num_blocks - num_blocks // 2
        query, tables, first_msgs, new_keys, new_vals = pl.pallas_call(
            cache_kernel,
            in_specs=[smem] + [vmem] * 4 + [hbm] * 6,
            out_specs=[vmem, vmem, hbm, hbm, hbm],
            out_shape=[jax.ShapeDtypeStruct((CHUNK, kv_heads, hd, qcols), BF16), jax.ShapeDtypeStruct((chunks, 2, hd // 2, rows), F32),
                       jax.ShapeDtypeStruct((CHUNK // 2, rows_msg, qcols), F32), cache_shape, cache_shape],
            scratch_shapes=[
                pltpu.VMEM((chunks, 2, CHUNK, num_blocks, kv_heads, hd, blk), BF16),
                pltpu.VMEM((chunks, CHUNK, tree, width), BF16),
                pltpu.VMEM((2, kvdim, rows), BF16),
                pltpu.VMEM((width, kvdim), BF16),
                pltpu.VMEM((width, kvdim), BF16),
                pltpu.VMEM((width, qdim), BF16),
                pltpu.VMEM((num_blocks, kv_heads, hd + 16, blk), BF16),
                pltpu.VMEM((late_blocks, kv_heads, ext, blk), BF16),
                pltpu.VMEM((kv_heads, ext, qcols), BF16),
                pltpu.VMEM((2, num_blocks * blk, qcols), F32),
                pltpu.VMEM((CHUNK // 2, rows_msg, qcols), F32),
                pltpu.SemaphoreType.DMA((chunks, 3)),
                pltpu.SemaphoreType.DMA((chunks, 2)),
                pltpu.SemaphoreType.DMA((3,)),
                pltpu.SemaphoreType.DMA((CHUNK // 2,)),
            ],
            compiler_params=pltpu.CompilerParams(vmem_limit_bytes=62 * 2**20),
            name='fill_caches',
        )(ctx_len, attn_gain, positions, jnp.asarray(rope_frequencies(hd)), tree_mask, w_key, w_value, w_query, hidden, keys, values)
        wide_rows = (chunks, tree, width // 2)
        out_hidden = pl.pallas_call(
            attend_kernel,
            in_specs=[smem, vmem] + [hbm] * 9,
            out_specs=vmem,
            out_shape=pltpu.VMEM((nreq, tree, width), BF16),
            scratch_shapes=[
                pltpu.VMEM((nreq, 2, tree, width // 2), F32),
                pltpu.VMEM((2, num_blocks, kv_heads, hd, blk), BF16),
                pltpu.VMEM((2, num_blocks, kv_heads, hd + 16, blk), BF16),
                pltpu.VMEM((late_blocks, kv_heads, ext, blk), BF16),
                pltpu.VMEM((kv_heads, ext, qcols), BF16),
                pltpu.VMEM((2, tree, tree), jnp.int32),
                pltpu.VMEM((2, num_blocks * blk, qcols), F32),
                pltpu.VMEM((chunks, CHUNK, rows_msg, qcols), F32),
                pltpu.VMEM((chunks, 2, rows_msg, qcols), F32),
                pltpu.VMEM((chunks, rows_msg, qcols), F32),
                pltpu.VMEM((chunks, rows_msg, qcols), F32),
                pltpu.VMEM(wide_rows, F32),
                pltpu.VMEM(wide_rows, F32),
                pltpu.VMEM((group, kv_heads * hd, width), BF16),
                pltpu.VMEM(wide_rows, BF16),
                pltpu.VMEM((width, qdim), BF16),
                pltpu.VMEM((CHUNK, tree, width), BF16),
                pltpu.VMEM((1, 2, hd // 2, rows), F32),
                pltpu.VMEM((2, CHUNK, kv_heads, hd, qcols), BF16),
                pltpu.SemaphoreType.DMA((2, 3)),
                pltpu.SemaphoreType.DMA((group, kv_heads)),
                pltpu.SemaphoreType.DMA((chunks,)),
                pltpu.SemaphoreType.DMA((5,)),
                pltpu.SemaphoreType.DMA((chunks, 13)),
                pltpu.SemaphoreType.DMA((chunks, 13)),
            ],
            compiler_params=pltpu.CompilerParams(collective_id=0, has_side_effects=True, vmem_limit_bytes=56 * 2**20),
            name='attend_and_combine',
        )(ctx_len, attn_gain, query, tables, first_msgs, tree_mask, new_keys, new_vals, hidden, w_query, w_out)
        return (out_hidden, jnp.swapaxes(new_keys, -1, -2)[:, :, None], jnp.swapaxes(new_vals, -1, -2)[:, :, None])

    return jax.shard_map(local_step, mesh=mesh, in_specs=(row_spec, P(), P(None, 'tp'), P(None, 'tp'), P(None, 'tp'), P('tp', None), cache_spec, cache_spec, row_spec, row_spec, row_spec), out_specs=(row_spec, cache_spec, cache_spec), check_vma=False)
```

```python
import functools
import math
import jax
import jax.numpy as jnp
import numpy as np
from jax import lax
from jax.experimental import pallas as pl
from jax.experimental.pallas import tpu as pltpu
from jax.sharding import PartitionSpec as P

ROPE_THETA = 500000.0
NORM_EPS = 1e-5
MASKED = -1e30
LOG2E = math.log2(math.e)
MESH = pl.DeviceIdType.MESH
F32 = jnp.float32
BF16 = jnp.bfloat16
CHUNK = 4

SCHEDULE = (
    ('finish', 0, (7, 14, 17, 25, 26, 27)),
    ('query', 2, (3, 7, 11, 15)),
    ('forward', 0, (11, 22, 23, 27, 28, 29)),
    ('merge', 1, (3, 6, 10, 15, 18)),
    ('project', 0, (3, 7, 11, 15, 20, 24)),
    ('diagonal', 0, (18, 25, 26, 29, 31, 32)),
    ('emit', 0, (23, 28, 29, 30, 32, 33)),
)

def mm(a, b):
    return jnp.dot(a, b, preferred_element_type=F32)


def mm_tn(a, b):
    return lax.dot_general(a, b, (((0,), (0,)), ((), ())), preferred_element_type=F32)


def rope_frequencies(head_dim):
    freq_idx = np.arange(head_dim // 2, dtype=np.float32)
    inv_freq = np.float32(1.0) / (np.float32(ROPE_THETA) ** (np.float32(2.0) * freq_idx / np.float32(head_dim)))
    wavelen = np.float32(2.0 * math.pi) / inv_freq
    smooth = (np.float32(8192.0) / wavelen - np.float32(1.0)) / np.float32(3.0)
    blended = (np.float32(1.0) - smooth) * inv_freq / np.float32(8.0) + smooth * inv_freq
    return np.where(wavelen < 2048.0, inv_freq, np.where(wavelen > 8192.0, inv_freq / np.float32(8.0), blended)).astype(np.float32)


def cos_sin(angle):
    turns = jnp.floor(angle * (2.0 / math.pi) + 0.5)
    r = ((angle - turns * 1.5703125) - turns * 4.837512969970703125e-4) - turns * 7.549789954891882e-8
    z = r * r
    sin_r = r + r * z * (-1.6666654611e-1 + z * (8.3321608736e-3 + z * -1.9515295891e-4))
    cos_r = 1.0 - 0.5 * z + z * z * (4.166664568298827e-2 + z * (-1.388731625493765e-3 + z * 2.443315711809948e-5))
    quarter = turns.astype(jnp.int32) & 3
    odd = (quarter & 1) == 1
    cos, sin = jnp.where(odd, sin_r, cos_r), jnp.where(odd, cos_r, sin_r)
    return jnp.where((quarter == 1) | (quarter == 2), -cos, cos), jnp.where(quarter >= 2, -sin, sin)


def normed_rows(x, gain):
    wide = x.astype(F32)
    inv_rms = lax.rsqrt(jnp.mean(wide * wide, axis=-1, keepdims=True) + NORM_EPS)
    return (wide * inv_rms * gain.astype(F32)[None, :]).astype(BF16)


def rotate(rows, cos, sin):
    half = rows.shape[0] // 2
    first, second = rows[:half], rows[half:]
    return jnp.concatenate([first * cos - second * sin, second * cos + first * sin], axis=0)


def project_queries(h, wq_ref, cos, sin, out, hd, group, tree):
    reqs = h.shape[0] // tree
    for head in range(wq_ref.shape[1] // (group * hd)):
        q_t = mm(h, wq_ref[:, head * group * hd:(head + 1) * group * hd]).T
        parts = [rotate(q_t[g * hd:(g + 1) * hd], cos, sin) for g in range(group)]
        for i in range(reqs):
            out(i, head, jnp.concatenate([p[:, i * tree:(i + 1) * tree] for p in parts], axis=1).astype(BF16))


def prepare(vref, qext, hd, tree):
    num_blocks, heads, vrows, blk = vref.shape
    ones = jnp.ones((vrows - hd, blk), BF16)
    pad = qext.shape[1] - hd - tree
    hide = jnp.where(lax.broadcasted_iota(jnp.int32, (pad, qext.shape[2]), 0) == 0, MASKED, 0.0).astype(BF16)
    for h in range(heads):
        for j in range(num_blocks):
            vref[j, h, hd:, :] = ones
        qext[h, hd + tree:, :] = hide


def attention(ctx, tree_mask, qref, kref, vref, kext, qext, scores, out, cp):
    num_blocks, heads, hd, blk = kref.shape
    qcols, tree = qext.shape[2], tree_mask.shape[0]
    pad = qext.shape[1] - hd - tree
    late = num_blocks // 2
    coef = hd ** -0.5 * LOG2E
    seen = jnp.concatenate([tree_mask.astype(F32)] * (qcols // tree), axis=0).T
    bias = jnp.where(seen > 0.0, 0.0, MASKED).astype(BF16)
    for h in range(heads):
        qext[h, :hd, :] = qref[h]
        qext[h, hd:hd + tree, :] = bias
    for j in range(late, num_blocks):
        off = (j * 4 + cp) * blk - ctx
        tok = off + lax.broadcasted_iota(jnp.int32, (tree, blk), 1)
        pick = jnp.where(tok == lax.broadcasted_iota(jnp.int32, (tree, blk), 0), 1.0, 0.0).astype(BF16)
        tok_p = off + lax.broadcasted_iota(jnp.int32, (pad, blk), 1)
        tail = jnp.where((tok_p >= tree) & (lax.broadcasted_iota(jnp.int32, (pad, blk), 0) == 0), 1.0, 0.0).astype(BF16)
        tok_h = off + lax.broadcasted_iota(jnp.int32, (hd, blk), 1)
        for h in range(heads):
            kext[j - late, h, :hd, :] = jnp.where(tok_h < tree, kref[j, h].astype(F32), 0.0).astype(BF16)
            kext[j - late, h, hd:hd + tree, :] = pick
            kext[j - late, h, hd + tree:, :] = tail

    def score(h, j):
        if j < late:
            s = mm_tn(kref[j, h], qext[h, :hd, :])
        else:
            s = mm_tn(kext[j - late, h], qext[h])
        scores[h % 2, j * blk:(j + 1) * blk, :] = s
        return jnp.max(s.reshape(blk // 8, 8, qcols), axis=0)

    tops = [None] * heads
    tops[0] = functools.reduce(jnp.maximum, [score(0, j) for j in range(num_blocks)])
    for h in range(heads):
        top = jnp.max(tops[h], axis=0, keepdims=True)
        shift = top * coef
        total, nxt = None, []
        for j in range(num_blocks):
            if h + 1 < heads:
                nxt.append(score(h + 1, j))
            p = jnp.exp2(scores[h % 2, j * blk:(j + 1) * blk, :] * coef - shift).astype(BF16)
            o = mm(vref[j, h], p)
            total = o if total is None else total + o
        if h + 1 < heads:
            tops[h + 1] = functools.reduce(jnp.maximum, nxt)
        out[h * hd:(h + 1) * hd, :] = total[:hd]
        out[heads * hd + h:heads * hd + h + 1, :] = top
        out[heads * hd + heads + h:heads * hd + heads + h + 1, :] = total[hd:hd + 1]


def cache_kernel(ctx_ref, gain_ref, pos_ref, freq_ref, mask_ref, wk_hbm, wv_hbm, wq_hbm, x_hbm, kc_hbm, vc_hbm,
                 q_ref, tab_ref, msg_hbm, ko_hbm, vo_hbm,
                 buf, xbuf, new_ref, wk_ref, wv_ref, wq_ref, vbuf, kext, qext, scores, msg, in_sem, out_sem, w_sem, msg_sem):
    cp_rank, cp_size = lax.axis_index('cp'), lax.axis_size('cp')
    chunks, _, per, num_blocks, kv_heads, hd, blk = buf.shape
    tree = pos_ref.shape[1]
    group = q_ref.shape[3] // tree
    width = x_hbm.shape[2]
    half = hd // 2
    cols = per * tree

    def rows_of(c):
        return pl.ds(c * per, per)

    def fetch_rows(c):
        return pltpu.make_async_copy(x_hbm.at[rows_of(c)], xbuf.at[c], in_sem.at[c, 2])

    def fetch(c):
        return [pltpu.make_async_copy(src.at[rows_of(c)], buf.at[c, n], in_sem.at[c, n]) for n, src in enumerate((kc_hbm, vc_hbm))]

    def flush(c):
        return [pltpu.make_async_copy(buf.at[c, n], dst.at[rows_of(c)], out_sem.at[c, n]) for n, dst in enumerate((ko_hbm, vo_hbm))]

    kv_weights = [pltpu.make_async_copy(src, dst, w_sem.at[n]) for n, (src, dst) in enumerate(((wk_hbm, wk_ref), (wv_hbm, wv_ref)))]
    q_weight = pltpu.make_async_copy(wq_hbm, wq_ref, w_sem.at[2])
    for c in [fetch_rows(0)] + kv_weights:
        c.start()
    prepare(vbuf, qext, hd, tree)
    diag = lax.broadcasted_iota(jnp.int32, (half, half), 0) == lax.broadcasted_iota(jnp.int32, (half, half), 1)
    freq = jnp.sum(jnp.where(diag, freq_ref[...][None, :], 0.0), axis=1, keepdims=True)
    for c in kv_weights:
        c.wait()
    for c in fetch(0) + [q_weight]:
        c.start()

    @pl.loop(0, chunks)
    def _(k):
        fetch_rows(k).wait()
        h = normed_rows(xbuf[k].reshape(cols, width), gain_ref[...])
        pos = jnp.concatenate([pos_ref[pl.ds(k * per + i, 1), :] for i in range(per)], axis=1).astype(F32)
        cos, sin = cos_sin(pos * freq)

        tab_ref[k, 0] = cos
        tab_ref[k, 1] = sin
        key_t = mm(h, wk_ref[...]).T
        for n in range(kv_heads):
            new_ref[0, n * hd:(n + 1) * hd, :] = rotate(key_t[n * hd:(n + 1) * hd], cos, sin).astype(BF16)
        new_ref[1] = mm(h, wv_ref[...]).T.astype(BF16)
        for c in fetch(k):
            c.wait()
        for i in range(per):
            ctx = ctx_ref[k * per + i]
            for j in range(num_blocks // 2, num_blocks):
                first_pos = (j * cp_size + cp_rank) * blk

                @pl.when((first_pos < ctx + tree) & (first_pos + blk > ctx))
                def _():
                    tok = first_pos - ctx + lax.broadcasted_iota(jnp.int32, (cols, blk), 1)
                    row = lax.broadcasted_iota(jnp.int32, (cols, blk), 0) - i * tree
                    pick = jnp.where((row == tok) & (row >= 0) & (row < tree), 1.0, 0.0).astype(BF16)
                    tok_h = first_pos - ctx + lax.broadcasted_iota(jnp.int32, (hd, blk), 1)
                    fresh = (tok_h >= 0) & (tok_h < tree)
                    for n in range(2):
                        put = mm(new_ref[n], pick)
                        for head in range(kv_heads):
                            old = buf[k, n, i, j, head].astype(F32)
                            buf[k, n, i, j, head] = jnp.where(fresh, put[head * hd:(head + 1) * hd], old).astype(BF16)

        for c in flush(k):
            c.start()

        @pl.when(k == 0)
        def _():
            q_weight.wait()
            for n in range(1, chunks - 1 - per // 2):
                for c in [fetch_rows(n)] + fetch(n):
                    c.start()

            def out(i, head, value):
                q_ref[i, head] = value

            project_queries(h, wq_ref, cos, sin, out, hd, group, tree)

            @pl.loop(0, per // 2)
            def _(i):
                later = chunks - 1 - per // 2 + i
                for c in [fetch_rows(later)] + fetch(later):
                    c.start()
                req = (1 - cp_rank // 2) * (per // 2) + i
                for j in range(num_blocks):
                    for head in range(kv_heads):
                        vbuf[j, head, :hd, :] = buf[0, 1, req, j, head]
                attention(ctx_ref[req], mask_ref[req], q_ref.at[req], buf.at[0, 0, req], vbuf, kext, qext, scores, msg.at[i], cp_rank)
                pltpu.make_async_copy(msg.at[i], msg_hbm.at[i], msg_sem.at[i]).start()

            for c in [fetch_rows(chunks - 1)] + fetch(chunks - 1):
                c.start()

    for i in range(per // 2):
        pltpu.make_async_copy(msg.at[i], msg_hbm.at[i], msg_sem.at[i]).wait()
    for n in range(chunks):
        for c in flush(n):
            c.wait()


def attend_kernel(ctx_ref, gain_ref, q_hbm, tab_hbm, msg_hbm, mask_hbm, kc_hbm, vc_hbm, hid_hbm, wq_hbm, wo_hbm, out_ref,
                  y_ref, kbuf, vbuf, kext, qext, mbuf, scores, msg, rpart, xsend, xrecv, psend, precv, wout, resid, wq_ref, xbuf, tbuf, qbuf,
                  kv_sem, w_sem, hid_sem, q_sem, snd, rcv):
    cp, tp = lax.axis_index('cp'), lax.axis_index('tp')
    chip, core = cp // 2, cp % 2
    partner = {'cp': chip * 2 + 1 - core}
    across_x = {'cp': (1 - chip) * 2 + core}
    across_y = {'tp': 1 - tp}
    _, heads, hd, qcols = q_hbm.shape
    nreq = mask_hbm.shape[0]
    tree = mask_hbm.shape[1]
    group = qcols // tree
    num_blocks, blk = kbuf.shape[1], kbuf.shape[4]
    chunks = nreq // CHUNK
    width = wo_hbm.shape[1]
    wcols = width // 2
    coef = hd ** -0.5 * LOG2E
    own_cols = pl.ds(pl.multiple_of(tp * wcols, wcols), wcols)
    other_cols = pl.ds(pl.multiple_of((1 - tp) * wcols, wcols), wcols)

    def remote(src, dst, k, n, to):
        return pltpu.make_async_remote_copy(src_ref=src, dst_ref=dst, send_sem=snd.at[k, n], recv_sem=rcv.at[k, n], device_id=to, device_id_type=MESH)

    barrier = pltpu.get_barrier_semaphore()
    for to in (partner, across_x, across_y):
        pl.semaphore_signal(barrier, inc=1, device_id=to, device_id_type=MESH)

    turns = nreq - CHUNK // 2

    def turn_of(n):
        pair = n // 2
        foreign = jnp.where((pair % 2 == 0) & (n < turns - 2), 1, 0)
        return pair // 2 + foreign, 2 * (chip + foreign - 2 * chip * foreign) + n % 2, foreign

    def fetch(n):
        k, i, _ = turn_of(n)
        r, to = k * CHUNK + i, n % 2
        return [pltpu.make_async_copy(kc_hbm.at[r], kbuf.at[to], kv_sem.at[to, 0]),
                pltpu.make_async_copy(vc_hbm.at[r], vbuf.at[to, :, :, pl.ds(0, hd), :], kv_sem.at[to, 1]),
                pltpu.make_async_copy(mask_hbm.at[r], mbuf.at[to], kv_sem.at[to, 2])]

    def weight_copies():
        out = []
        for g in range(group):
            for h in range(heads):
                out.append(pltpu.make_async_copy(wo_hbm.at[pl.ds((h * group + g) * hd, hd)], wout.at[g, pl.ds(h * hd, hd)], w_sem.at[g, h]))
        return out

    def resid_copies():
        return [pltpu.make_async_copy(hid_hbm.at[k * CHUNK + cp, :, own_cols], resid.at[k], hid_sem.at[k]) for k in range(chunks)]

    first_queries = pltpu.make_async_copy(q_hbm, qbuf.at[0], q_sem.at[0])
    query_weight = pltpu.make_async_copy(wq_hbm, wq_ref, q_sem.at[1])

    def chunk_copies(k):
        pairs = tbuf.shape[0]
        return [pltpu.make_async_copy(hid_hbm.at[pl.ds(k * CHUNK, CHUNK)], xbuf, q_sem.at[2]),
                pltpu.make_async_copy(tab_hbm.at[pl.ds(k * pairs, pairs)], tbuf, q_sem.at[3])]

    first_msgs = pltpu.make_async_copy(msg_hbm, msg.at[0, pl.ds(2 * (1 - chip), 2)], q_sem.at[4])
    first_msgs.start()
    for to in range(2):
        prepare(vbuf.at[to], qext, hd, tree)
    pl.semaphore_wait(barrier, 3)
    first_msgs.wait()

    def share(k, i, which):
        @pl.when(i % 2 != core)
        def _():
            remote(msg.at[k, i], rpart.at[k, which], k, which, partner).start()

    for n in range(2):
        share(0, 2 * (1 - chip) + n, 0)
    for c in chunk_copies(1) + [query_weight] + fetch(0) + [first_queries]:
        c.start()

    def queries(k):
        for c in chunk_copies(k):
            c.wait()

        @pl.when(k == 1)
        def _():
            query_weight.wait()

        h = normed_rows(xbuf[...].reshape(CHUNK * tree, width), gain_ref[...])
        cos = jnp.concatenate([tbuf[p, 0] for p in range(tbuf.shape[0])], axis=1)
        sin = jnp.concatenate([tbuf[p, 1] for p in range(tbuf.shape[0])], axis=1)

        def out(i, head, value):
            qbuf[k % 2, i, head] = value

        project_queries(h, wq_ref, cos, sin, out, hd, group, tree)

        @pl.when(k + 1 < chunks)
        def _():
            for c in chunk_copies(k + 1):
                c.start()

    def attend(n):
        k, i, foreign = turn_of(n)
        r, slot = k * CHUNK + i, n % 2

        @pl.when(n + 1 < turns)
        def _():
            for c in fetch(n + 1):
                c.start()

        ctx = ctx_ref[r]
        for c in fetch(n):
            c.wait()
        attention(ctx, mbuf[slot], qbuf.at[k % 2, i], kbuf.at[slot], vbuf.at[slot], kext, qext, scores, msg.at[k, i], cp)

        share(k, i, 1 - foreign)

    stat = heads * hd

    def scales(parts, h):
        tops = [p[stat + h:stat + h + 1, :] for p in parts]
        top = functools.reduce(jnp.maximum, tops)
        return top, [jnp.exp2((t - top) * coef) for t in tops]

    def merge_chip(k):
        remote(msg.at[k, 0], rpart.at[k, 0], k, 0, partner).wait_recv()
        parts = [msg.at[k, 2 * (1 - chip) + core], rpart.at[k, 0]]
        for h in range(heads):
            top, fac = scales(parts, h)
            rows = slice(h * hd, (h + 1) * hd)
            xsend[k, rows, :] = sum(p[rows, :] * f for p, f in zip(parts, fac))
            xsend[k, stat + h:stat + h + 1, :] = top
            srow = slice(stat + heads + h, stat + heads + h + 1)
            xsend[k, srow, :] = sum(p[srow, :] * f for p, f in zip(parts, fac))
        remote(xsend.at[k], xrecv.at[k], k, 2, across_x).start()

    def project(k):
        remote(msg.at[k, 0], rpart.at[k, 1], k, 1, partner).wait_recv()
        remote(xsend.at[k], xrecv.at[k], k, 2, across_x).wait_recv()
        parts = [msg.at[k, cp], rpart.at[k, 1], xrecv.at[k]]
        outs = []
        for h in range(heads):
            _, fac = scales(parts, h)
            rows = slice(h * hd, (h + 1) * hd)
            srow = slice(stat + heads + h, stat + heads + h + 1)
            inv = 1.0 / sum(p[srow, :] * f for p, f in zip(parts, fac))
            outs.append(sum(p[rows, :] * (f * inv) for p, f in zip(parts, fac)))
        attn = jnp.concatenate(outs, axis=0).T.astype(BF16)

        @pl.when(k == 0)
        def _():
            for c in weight_copies() + resid_copies():
                c.wait()

        def part(cols):
            acc = None
            for g in range(group):
                d = mm(attn[g * tree:(g + 1) * tree], wout[g, :, cols])
                acc = d if acc is None else acc + d
            return acc.astype(BF16).astype(F32)

        psend[k] = part(other_cols)
        remote(psend.at[k], precv.at[k], k, 3, across_y).start()
        y_ref[k * CHUNK + cp, tp] = resid[k].astype(F32) + part(own_cols)

    def piece(k, owner_cp, owner_tp, lo=0, n=None):
        rows = pl.ds(lo, tree if n is None else n)
        return y_ref.at[k * CHUNK + owner_cp, owner_tp, rows]

    hf = (tree * 3 // 8) // 8 * 8
    hb = tree - hf
    pcp, xcp, dcp = chip * 2 + 1 - core, (1 - chip) * 2 + core, (1 - chip) * 2 + 1 - core

    def gather_copy(k, n):
        if n == 4:
            return remote(piece(k, cp, tp), piece(k, cp, tp), k, n, across_x)
        if n == 5:
            return remote(piece(k, cp, tp), piece(k, cp, tp), k, n, across_y)
        if n == 6:
            return remote(piece(k, cp, tp), piece(k, cp, tp), k, n, partner)
        if n == 7:
            return remote(piece(k, xcp, tp, 0, hf), piece(k, xcp, tp, 0, hf), k, n, across_y)
        if n == 8:
            return remote(piece(k, xcp, tp), piece(k, xcp, tp), k, n, partner)
        if n == 9:
            return remote(piece(k, cp, 1 - tp, hf, hb), piece(k, cp, 1 - tp, hf, hb), k, n, across_x)
        if n == 10:
            return remote(piece(k, cp, 1 - tp), piece(k, cp, 1 - tp), k, n, partner)
        if n == 11:
            return remote(piece(k, xcp, 1 - tp, 0, hf), piece(k, xcp, 1 - tp, 0, hf), k, n, partner)
        return remote(piece(k, xcp, 1 - tp, hf, hb), piece(k, xcp, 1 - tp, hf, hb), k, n, partner)

    def landed(k, n):
        src = {4: (xcp, tp, 0, tree), 5: (cp, 1 - tp, 0, tree), 6: (pcp, tp, 0, tree), 7: (xcp, 1 - tp, 0, hf), 8: (dcp, tp, 0, tree),
               9: (xcp, 1 - tp, hf, hb), 10: (pcp, 1 - tp, 0, tree), 11: (dcp, 1 - tp, 0, hf), 12: (dcp, 1 - tp, hf, hb)}[n]
        ref = piece(k, *src)
        remote(ref, ref, k, n, partner).wait_recv()

    def finish(k):
        remote(psend.at[k], precv.at[k], k, 3, across_y).wait_recv()
        total = y_ref[k * CHUNK + cp, tp] + precv[k]
        y_ref[k * CHUNK + cp, tp] = total.astype(BF16).astype(F32)
        for n in (4, 5, 6):
            gather_copy(k, n).start()

    def forward(k):
        landed(k, 4)
        gather_copy(k, 7).start()
        gather_copy(k, 8).start()
        landed(k, 5)
        gather_copy(k, 9).start()
        gather_copy(k, 10).start()

    def forward_diagonal(k):
        landed(k, 7)
        gather_copy(k, 11).start()
        landed(k, 9)
        gather_copy(k, 12).start()

    def emit(k):
        for n in (6, 8, 10, 11, 12):
            landed(k, n)
        for i in range(CHUNK):
            for side in range(2):
                out_ref[k * CHUNK + i, :, side * wcols:(side + 1) * wcols] = y_ref[k * CHUNK + i, side].astype(BF16)

    work = {'merge': merge_chip, 'query': queries, 'project': project, 'finish': finish, 'forward': forward, 'diagonal': forward_diagonal, 'emit': emit}

    merge_chip(0)
    queries(1)
    first_queries.wait()

    @pl.loop(0, 1 + max(max(when) for _, _, when in SCHEDULE))
    def _(n):
        @pl.when(n < turns)
        def _():
            attend(n)

        @pl.when(n == 0)
        def _():
            for c in weight_copies() + resid_copies():
                c.start()

        for name, lowest, when in SCHEDULE:
            now = n + 1 - core if name == 'merge' else n

            @pl.when(functools.reduce(jnp.logical_or, [now == t for t in when]))
            def _():
                work[name](sum([jnp.where(now > t, 1, 0) for t in when]) + lowest)

    @pl.loop(0, chunks)
    def _(k):
        remote(msg.at[k, 0], rpart.at[k, 0], k, 0, partner).wait_send()
        remote(msg.at[k, 0], rpart.at[k, 1], k, 1, partner).wait_send()
        remote(xsend.at[k], xrecv.at[k], k, 2, across_x).wait_send()
        remote(psend.at[k], precv.at[k], k, 3, across_y).wait_send()
        for n in range(4, 13):
            gather_copy(k, n).wait_send()


def solution(mesh):
    cache_spec = P('dp', None, 'cp', 'tp')
    row_spec = P('dp')

    def local_step(hidden, attn_gain, w_query, w_key, w_value, w_out, cache_k, cache_v, ctx_len, positions, tree_mask):
        nreq, tree, width = hidden.shape
        num_blocks, kv_heads, blk, hd = cache_k.shape[1], cache_k.shape[3], cache_k.shape[4], cache_k.shape[5]
        qdim, kvdim = w_query.shape[1], w_key.shape[1]
        group = qdim // kvdim
        chunks = nreq // CHUNK
        keys = jnp.swapaxes(cache_k[:, :, 0], -1, -2)
        values = jnp.swapaxes(cache_v[:, :, 0], -1, -2)
        hbm = pl.BlockSpec(memory_space=pl.ANY)
        vmem = pl.BlockSpec(memory_space=pltpu.VMEM)
        smem = pl.BlockSpec(memory_space=pltpu.SMEM)
        cache_shape = jax.ShapeDtypeStruct(keys.shape, BF16)
        rows = CHUNK * tree
        qcols = group * tree
        rows_msg = kv_heads * hd + 2 * kv_heads
        ext = hd + tree + 16
        late_blocks = num_blocks - num_blocks // 2
        query, tables, first_msgs, new_keys, new_vals = pl.pallas_call(
            cache_kernel,
            in_specs=[smem] + [vmem] * 4 + [hbm] * 6,
            out_specs=[vmem, vmem, hbm, hbm, hbm],
            out_shape=[jax.ShapeDtypeStruct((CHUNK, kv_heads, hd, qcols), BF16), jax.ShapeDtypeStruct((chunks, 2, hd // 2, rows), F32),
                       jax.ShapeDtypeStruct((CHUNK // 2, rows_msg, qcols), F32), cache_shape, cache_shape],
            scratch_shapes=[
                pltpu.VMEM((chunks, 2, CHUNK, num_blocks, kv_heads, hd, blk), BF16),
                pltpu.VMEM((chunks, CHUNK, tree, width), BF16),
                pltpu.VMEM((2, kvdim, rows), BF16),
                pltpu.VMEM((width, kvdim), BF16),
                pltpu.VMEM((width, kvdim), BF16),
                pltpu.VMEM((width, qdim), BF16),
                pltpu.VMEM((num_blocks, kv_heads, hd + 16, blk), BF16),
                pltpu.VMEM((late_blocks, kv_heads, ext, blk), BF16),
                pltpu.VMEM((kv_heads, ext, qcols), BF16),
                pltpu.VMEM((2, num_blocks * blk, qcols), F32),
                pltpu.VMEM((CHUNK // 2, rows_msg, qcols), F32),
                pltpu.SemaphoreType.DMA((chunks, 3)),
                pltpu.SemaphoreType.DMA((chunks, 2)),
                pltpu.SemaphoreType.DMA((3,)),
                pltpu.SemaphoreType.DMA((CHUNK // 2,)),
            ],
            compiler_params=pltpu.CompilerParams(vmem_limit_bytes=62 * 2**20),
            name='fill_caches',
        )(ctx_len, attn_gain, positions, jnp.asarray(rope_frequencies(hd)), tree_mask, w_key, w_value, w_query, hidden, keys, values)
        wide_rows = (chunks, tree, width // 2)
        out_hidden = pl.pallas_call(
            attend_kernel,
            in_specs=[smem, vmem] + [hbm] * 9,
            out_specs=vmem,
            out_shape=pltpu.VMEM((nreq, tree, width), BF16),
            scratch_shapes=[
                pltpu.VMEM((nreq, 2, tree, width // 2), F32),
                pltpu.VMEM((2, num_blocks, kv_heads, hd, blk), BF16),
                pltpu.VMEM((2, num_blocks, kv_heads, hd + 16, blk), BF16),
                pltpu.VMEM((late_blocks, kv_heads, ext, blk), BF16),
                pltpu.VMEM((kv_heads, ext, qcols), BF16),
                pltpu.VMEM((2, tree, tree), jnp.int32),
                pltpu.VMEM((2, num_blocks * blk, qcols), F32),
                pltpu.VMEM((chunks, CHUNK, rows_msg, qcols), F32),
                pltpu.VMEM((chunks, 2, rows_msg, qcols), F32),
                pltpu.VMEM((chunks, rows_msg, qcols), F32),
                pltpu.VMEM((chunks, rows_msg, qcols), F32),
                pltpu.VMEM(wide_rows, F32),
                pltpu.VMEM(wide_rows, F32),
                pltpu.VMEM((group, kv_heads * hd, width), BF16),
                pltpu.VMEM(wide_rows, BF16),
                pltpu.VMEM((width, qdim), BF16),
                pltpu.VMEM((CHUNK, tree, width), BF16),
                pltpu.VMEM((1, 2, hd // 2, rows), F32),
                pltpu.VMEM((2, CHUNK, kv_heads, hd, qcols), BF16),
                pltpu.SemaphoreType.DMA((2, 3)),
                pltpu.SemaphoreType.DMA((group, kv_heads)),
                pltpu.SemaphoreType.DMA((chunks,)),
                pltpu.SemaphoreType.DMA((5,)),
                pltpu.SemaphoreType.DMA((chunks, 13)),
                pltpu.SemaphoreType.DMA((chunks, 13)),
            ],
            compiler_params=pltpu.CompilerParams(collective_id=0, has_side_effects=True, vmem_limit_bytes=56 * 2**20),
            name='attend_and_combine',
        )(ctx_len, attn_gain, query, tables, first_msgs, tree_mask, new_keys, new_vals, hidden, w_query, w_out)
        return (out_hidden, jnp.swapaxes(new_keys, -1, -2)[:, :, None], jnp.swapaxes(new_vals, -1, -2)[:, :, None])

    return jax.shard_map(local_step, mesh=mesh, in_specs=(row_spec, P(), P(None, 'tp'), P(None, 'tp'), P(None, 'tp'), P('tp', None), cache_spec, cache_spec, row_spec, row_spec, row_spec), out_specs=(row_spec, cache_spec, cache_spec), check_vma=False)
```
